128 devices in a mesh: lat: 8 (over x, core), lon: 16 (over y, z).
Axes of the slice: x: 4, y: 4, z: 4, core: 2. Of those that a mesh axis runs over, the one named last changes fastest.
Arguments:
- zonal_wind: float32 [16, 64, 4096], P(None, 'lat', 'lon'), may hold values from -0.45 to 0.45
- merid_wind: float32 [16, 64, 4096], P(None, 'lat', 'lon'), may hold values from -0.45 to 0.45
- operator_rows: float32 [8, 64], replicated, may hold values from -1.5 to 1.5
- innovation: float32 [524288], P(('lat', 'lon')), may hold values from -6 to 6
- error_weight: float32 [524288], P(('lat', 'lon')), may hold values from 0.25 to 4
- interp_weight: float32 [4, 524288], P(None, ('lat', 'lon')), may hold values from 0.05 to 1
- obs_slot: int32 [4, 524288], P(None, ('lat', 'lon')), may hold values from 0 to 2047
- block_count: int32 [4096], P(('lat', 'lon')), may hold values from 1 to 128
- block_type: int32 [4096], P(('lat', 'lon')), may hold values from 0 to 7
- block_window: int32 [4096], P(('lat', 'lon')), may hold values from 0 to 2
- send_cols: int32 [128, 2048], P(('lat', 'lon')), may hold values from 0 to 2047
Outputs:
- increment: float32 [4, 16, 64, 4096], P(None, None, 'lat', 'lon')
- residual: float32 [4, 16, 64, 4096], P(None, None, 'lat', 'lon')
The draws below stay inside these ranges and needn't reach their ends.
Inputs may be any that keep to these rules, and one draw needn't show every extreme that they name: `obs_slot`: an index into the 2048 slots that the observation's own device receives: slot s * 16 + q comes from device s. `send_cols`: entry r * 16 + q of device s's row is a local cell of device s, row-major over 8 x 256, sent to slot q of device r. `block_count`: rows of a block at or past its count are padding and observe nothing.
All inputs are finite; a program needn't handle non-finite values.
Results may differ from the reference program's by a relative error of at most 0.00025.
Values sent between devices are 32-bit elements; how exact they have to be, the bound alone decides.
A program may use at most 128 MiB of HBM per device.

```python
import math
import jax
import jax.numpy as jnp
from jax import lax

VARS = 4
LEV = 16
TYPES = 8
KPTS = 4
WIN = 3
STEP_WIN = 2
ITERS = 2
BLOCK_ROWS = 128
CLAT = 8
CLON = 256
RECV = 2048
CHANNELS = 64
NLAT = 64
NLON = 4096
SLOTS = 16
NOBS_DEV = 4096
NOBS = 524288
NBLK = 4096
N_LAT = 8
N_LON = 16


def place_ends(result, own_key, smallest, largest):
    longest = result.shape.index(max(result.shape))
    spots = []
    for shift in (0, 1):
        where = [jax.random.randint(jax.random.fold_in(own_key, axis), (), 0, length) for axis, length in enumerate(result.shape)]
        where[longest] = (where[longest] + shift) % result.shape[longest]
        spots.append(tuple(where))
    return result.at[spots[0]].set(smallest).at[spots[1]].set(largest)


def level_of(own_key, extent, pieces, smallest, top_value):
    def one(dim, parts):
        steps = jax.random.uniform(jax.random.fold_in(jax.random.fold_in(own_key, 6), dim), (parts,), jnp.float32, smallest / len(pieces), top_value / len(pieces))
        return jnp.repeat(jnp.exp(steps), extent[dim] // parts).reshape((-1,) + (1,) * (len(extent) - dim - 1))

    loudness = one(*pieces[0])
    for cut in pieces[1:]:
        loudness = loudness * one(*cut)
    return loudness


def normal_values(stream_key, shape, spread, most, split=(), held_as=jnp.bfloat16):
    entries = jax.random.normal(stream_key, shape, jnp.float32) * spread
    if len(split) > 0:
        entries = level_of(stream_key, shape, split, -0.22, 0.18) * entries
    return jnp.clip(entries, min=-most, max=most).astype(held_as)


def setup_inputs(seed: int = 0) -> dict:
    seeds = jax.random.split(jax.random.key(seed), 12)
    zonal_wind = jnp.clip(jax.random.uniform(seeds[0], (LEV, NLAT, NLON), jnp.float32, -0.45, 0.45) * level_of(seeds[0], (LEV, NLAT, NLON), ((1, 8), (2, 16)), -0.4, 0.0), -0.45, 0.45)
    merid_wind = jnp.clip(jax.random.uniform(seeds[1], (LEV, NLAT, NLON), jnp.float32, -0.45, 0.45) * level_of(seeds[1], (LEV, NLAT, NLON), ((1, 8), (2, 16)), -0.4, 0.0), -0.45, 0.45)
    operator_rows = normal_values(seeds[2], (TYPES, CHANNELS), (CHANNELS // 4) ** -0.5, 1.5, (), jnp.float32)
    innovation = normal_values(seeds[3], (NOBS,), 1.0, 6.0, ((0, 128),), jnp.float32)
    error_weight = jnp.clip(jnp.exp(math.log(4.0) - 2.7725887 * jax.random.uniform(seeds[4], (NOBS,), jnp.float32) ** level_of(seeds[4], (NOBS,), ((0, 128),), -0.2, 0.2)), 0.25, 4.0)
    interp_weight = jnp.clip(0.05 + 0.95 * jax.random.uniform(seeds[5], (KPTS, NOBS), jnp.float32) ** level_of(seeds[5], (KPTS, NOBS), ((1, 128),), -0.2, 0.2), 0.05, 1.0)
    obs_slot = place_ends(jax.random.randint(seeds[6], (KPTS, NOBS), 0, RECV), jax.random.fold_in(seeds[6], 1), 0, RECV - 1).astype(jnp.int32)
    block_count = place_ends(jax.random.randint(seeds[7], (NBLK,), 1, BLOCK_ROWS + 1), jax.random.fold_in(seeds[7], 1), 1, BLOCK_ROWS).astype(jnp.int32)
    block_type = place_ends(jax.random.randint(seeds[8], (NBLK,), 0, TYPES), jax.random.fold_in(seeds[8], 1), 0, TYPES - 1).astype(jnp.int32)
    block_window = place_ends(jax.random.randint(seeds[9], (NBLK,), 0, WIN), jax.random.fold_in(seeds[9], 1), 0, WIN - 1).astype(jnp.int32)
    send_cols = place_ends(jax.random.randint(seeds[10], (N_LAT * N_LON, RECV), 0, CLAT * CLON), jax.random.fold_in(seeds[10], 1), 0, (CLAT * CLON) - 1).astype(jnp.int32)
    return dict(zonal_wind=zonal_wind, merid_wind=merid_wind, operator_rows=operator_rows, innovation=innovation, error_weight=error_weight, interp_weight=interp_weight, obs_slot=obs_slot, block_count=block_count, block_type=block_type, block_window=block_window, send_cols=send_cols)


HIGH = lax.Precision.HIGHEST


def from_below(field):
    padded = jnp.pad(field, ((0, 0), (0, 0), (1, 0), (0, 0)))
    return padded[:, :, :-1]


def from_above(field):
    padded = jnp.pad(field, ((0, 0), (0, 0), (0, 1), (0, 0)))
    return padded[:, :, 1:]


def reference(zonal_wind, merid_wind, operator_rows, innovation, error_weight, interp_weight, obs_slot, block_count, block_type, block_window, send_cols):
    keep_rate = 1.0 - jnp.abs(zonal_wind) - jnp.abs(merid_wind)
    from_west = jnp.maximum(zonal_wind, 0.0)
    from_east = jnp.minimum(zonal_wind, 0.0)
    from_south = jnp.maximum(merid_wind, 0.0)
    from_north = jnp.minimum(merid_wind, 0.0)
    devices = N_LAT * N_LON
    ncell = NLAT * NLON
    channels = VARS * LEV
    source = jnp.arange(devices, dtype=jnp.int32)[:, None]
    row_global = (source // N_LON) * CLAT + send_cols // CLON
    col_global = (source % N_LON) * CLON + send_cols % CLON
    global_cell = (row_global * NLON + col_global).reshape(devices, devices, SLOTS)
    global_cell = jnp.transpose(global_cell, (1, 0, 2)).reshape(devices * RECV)
    owner = (jnp.arange(NOBS, dtype=jnp.int32) // NOBS_DEV)[None, :]
    cell = global_cell[owner * RECV + obs_slot]
    live = (jnp.arange(BLOCK_ROWS, dtype=jnp.int32)[None, :] < block_count[:, None]).reshape(NOBS)
    weight_live = error_weight * live.astype(jnp.float32)
    row_type = jnp.broadcast_to(block_type[:, None], (NBLK, BLOCK_ROWS)).reshape(NOBS)
    row_window = jnp.broadcast_to(block_window[:, None], (NBLK, BLOCK_ROWS)).reshape(NOBS)
    flat_index = ((row_window * TYPES + row_type)[None, :] * ncell + cell).astype(jnp.int32)

    def tangent_step(field):
        west = jnp.roll(field, 1, axis=3)
        east = jnp.roll(field, -1, axis=3)
        return keep_rate * field + from_west * west - from_east * east + from_south * from_below(field) - from_north * from_above(field)

    def adjoint_step(field):
        return keep_rate * field + jnp.roll(from_west * field, -1, axis=3) - jnp.roll(from_east * field, 1, axis=3) + from_above(from_south * field) - from_below(from_north * field)

    def forward_model(field):
        states = [field]
        for _ in range(WIN - 1):
            for _ in range(STEP_WIN):
                field = tangent_step(field)
            states.append(field)
        return states

    def observe(states):
        projected = jnp.stack([jnp.dot(operator_rows, state.reshape(channels, ncell), precision=HIGH) for state in states])
        picked = projected.reshape(-1)[flat_index]
        return jnp.sum(interp_weight * picked, axis=0)

    def adjoint_model(weighted):
        terms = (interp_weight * weighted[None, :]).reshape(-1)
        summed = jax.ops.segment_sum(terms, flat_index.reshape(-1), num_segments=WIN * TYPES * ncell).reshape(WIN, TYPES, ncell)
        forcing = [jnp.dot(operator_rows.T, summed[window], precision=HIGH).reshape(VARS, LEV, NLAT, NLON) for window in range(WIN)]
        field = forcing[WIN - 1]
        for window in range(WIN - 2, -1, -1):
            for _ in range(STEP_WIN):
                field = adjoint_step(field)
            field = field + forcing[window]
        return field

    def hessian(direction):
        return direction + adjoint_model(weight_live * observe(forward_model(direction)))

    right = adjoint_model(weight_live * innovation)
    increment = jnp.zeros_like(right)
    residual = right
    direction = right
    norm_now = jnp.sum(residual * residual)
    for _ in range(ITERS):
        image = hessian(direction)
        alpha = norm_now / jnp.sum(direction * image)
        increment = increment + alpha * direction
        residual = residual - alpha * image
        norm_next = jnp.sum(residual * residual)
        direction = residual + (norm_next / norm_now) * direction
        norm_now = norm_next
    return increment, residual
```

```python
import functools

import jax
import jax.numpy as jnp
from jax import lax
from jax.experimental import pallas as pl
from jax.experimental.pallas import tpu as pltpu
from jax.sharding import PartitionSpec as P

MESH = pl.DeviceIdType.MESH
F32 = jnp.float32
BF16 = jnp.bfloat16

TYPES = 8
WIN = 3
WT = WIN * TYPES
KPTS = 4
SLOTS = 16
ROWS = 128
N_LAT = 8
N_LON = 16
NDEV = N_LAT * N_LON
NBLK = 32
LEV = 16
CH = 64
LAT = 8
LON = 256
EXT = 16
LANES = 384
NT = (((1,), (1,)), ((), ()))


def split(value):
    high = value.astype(BF16).astype(F32)
    return high, value - high


def mm(left, right):
    return jnp.dot(left, right, preferred_element_type=F32)


def mm_nt(left, right):
    return lax.dot_general(left, right, NT, preferred_element_type=F32)


def place(number):
    return {"lat": number // N_LON, "lon": lax.rem(number, N_LON)}


def pack_rows(rows):
    packed = None
    for r, row in enumerate(rows):
        lane = lax.broadcasted_iota(jnp.int32, (row.shape[0], 128), 1)
        ends = jnp.where(lane < 64, row[:, :128], row[:, 128:])
        moved = pltpu.roll(ends, 4 + 16 * r, axis=1)
        packed = moved if packed is None else jnp.where((lane >> 4) == r, moved, packed)
    return packed


def kernel(
    zonal, merid, op2, opt4, innov, weight, interp, slots, cols, meta_v, count_s, type_s, window_s,
    x_out, r_out,
    winds, field, res, dirn, inc, kp,
    onehot, cweight, live, zrow, yrow, rblk, tsplit,
    colhot, proj, ssum, sext, stage, lgather, lscatter, sacc,
    send_f, send_b, recv_f, recv_b, wown,
    pack_w, pack_x, pack_s, ns_w, ns_x, ns_s, hp_w, hp_x, hp_s, rrv, part,
    a2a_send, a2a_recv, hw_send, hw_recv, hx_send, hx_recv, hs_send, hs_recv,
):
    lat = lax.axis_index("lat")
    lon = lax.axis_index("lon")
    me = lat * N_LON + lon
    barrier = pltpu.get_barrier_semaphore()

    def greet(i, carry):
        pl.semaphore_signal(
            barrier, inc=1, device_id=place(lax.rem(me + i, NDEV)), device_id_type=MESH
        )
        return carry

    lax.fori_loop(1, NDEV, greet, 0)

    north = lax.rem(lat + 1, N_LAT)
    south = lax.rem(lat + N_LAT - 1, N_LAT)
    east = lax.rem(lon + 1, N_LON)
    west = lax.rem(lon + N_LON - 1, N_LON)
    valid_s = jnp.where(lat > 0, 1.0, 0.0).astype(F32)
    valid_n = jnp.where(lat < N_LAT - 1, 1.0, 0.0).astype(F32)

    def halo(low, high, pack, ns, hp, send, recv):
        copies = [
            (high, ns.at[0], north, lon),
            (low, ns.at[1], south, lon),
            (pack, hp.at[0], lat, east),
            (pack, hp.at[1], lat, west),
            (pack, hp.at[2], north, east),
            (pack, hp.at[3], north, west),
            (pack, hp.at[4], south, east),
            (pack, hp.at[5], south, west),
        ]
        return [
            pltpu.make_async_remote_copy(
                src, dst, send.at[i], recv.at[i], device_id={"lat": a, "lon": o}, device_id_type=MESH
            )
            for i, (src, dst, a, o) in enumerate(copies)
        ]

    def halo_w():
        return halo(wown.at[pl.ds(0, 4)], wown.at[pl.ds(4, 4)], pack_w, ns_w, hp_w, hw_send, hw_recv)

    def halo_x():
        return halo(res.at[pl.ds(0, 4)], res.at[pl.ds(4, 4)], pack_x, ns_x, hp_x, hx_send, hx_recv)

    def halo_s():
        return halo(ssum.at[pl.ds(0, 4)], ssum.at[pl.ds(4, 4)], pack_s, ns_s, hp_s, hs_send, hs_recv)

    def sides(hp, base, rows):
        lane = lax.broadcasted_iota(jnp.int32, hp.shape[1:], 1)
        both = jnp.where((lane & 15) < 4, hp[base], hp[base + 1])
        return [pltpu.roll(both, (256 - 16 * r - 4) % 128, axis=1) for r in rows]

    def a2a_start(src, dst, k):
        def go(i, carry):
            to = lax.rem(me + i, NDEV)
            pltpu.make_async_remote_copy(
                src.at[to], dst.at[me], a2a_send.at[k], a2a_recv.at[k],
                device_id=place(to), device_id_type=MESH,
            ).start()
            return carry

        lax.fori_loop(1, NDEV, go, 0)
        dst[me] = src[me]

    def a2a_wait(src, dst, k):
        got = dst.at[pl.ds(0, NDEV - 1)]
        pltpu.make_async_copy(got, got, a2a_recv.at[k]).wait()
        gone = src.at[pl.ds(0, NDEV - 1)]
        pltpu.make_async_copy(gone, gone, a2a_send.at[k]).wait()

    for r in range(LAT):
        wown[r, :LEV, :] = zonal[:, r, :]
        wown[r, LEV:, :] = merid[:, r, :]
    pack_w[...] = pack_rows([wown[r] for r in range(LAT)])

    def tables(b, carry):
        at = pl.ds(pl.multiple_of(b * ROWS, ROWS), ROWS)
        slot = slots[:, at]
        wgt = interp[:, at]
        sender = slot >> 4
        inner = slot & 15
        sub = lax.broadcasted_iota(jnp.int32, (NDEV, ROWS), 0)
        sub16 = lax.broadcasted_iota(jnp.int32, (SLOTS, ROWS), 0)
        for k in range(KPTS):
            lanes = slice(k * ROWS, (k + 1) * ROWS)
            onehot[b, :, lanes] = jnp.where(sub == sender[k : k + 1], 1.0, 0.0).astype(BF16)
            cweight[b, :, lanes] = jnp.where(sub16 == inner[k : k + 1], wgt[k : k + 1], 0.0)
        lane = lax.broadcasted_iota(jnp.int32, (1, ROWS), 1)
        wl = jnp.where(lane < count_s[b], weight[b], 0.0)
        live[b] = wl
        zrow[b] = wl * innov[b]
        yrow[b] = jnp.zeros((1, ROWS), F32)
        return carry

    lax.fori_loop(0, NBLK, tables, 0)
    for n in range(8):
        low = cols[:, n * 256 : (n + 1) * 256] & 127
        sub = lax.broadcasted_iota(jnp.int32, (128, 256), 0)
        colhot[n] = jnp.where(sub == low, 1.0, 0.0).astype(BF16)
    lane32 = lax.broadcasted_iota(jnp.int32, (CH, 32), 1)
    opt_h, opt_l = split(opt4[...])
    opt = jnp.where((lane32 & 8) == 0, opt_h, opt_l).astype(BF16)
    op_h, op_l = split(op2[...])
    opp = jnp.concatenate([op_h, op_l], axis=0).astype(BF16)
    ids = meta_v[1:2, :] * TYPES + meta_v[0:1, :]
    member = jnp.where(lax.broadcasted_iota(jnp.int32, (32, NBLK), 0) == ids, 1.0, 0.0).astype(BF16)
    for r in range(LAT):
        dirn[r] = jnp.zeros((CH, LON), F32)
        inc[r] = jnp.zeros((CH, LON), F32)
    rrv[...] = jnp.ones((1, 128), F32)
    part[...] = jnp.zeros((1, 128), F32)

    pl.semaphore_wait(barrier, NDEV - 1)
    for copy in halo_w():
        copy.start()

    def build_winds():
        for copy in halo_w():
            copy.wait()
        tiles = [None] * EXT
        own = sides(hp_w, 0, range(8))
        low = sides(hp_w, 2, range(4, 8))
        high = sides(hp_w, 4, range(0, 4))
        for e in range(EXT):
            if e < 4:
                main, side, ok = ns_w[0, e], low[e], valid_s
            elif e < 12:
                main, side, ok = wown[e - 4], own[e - 4], None
            else:
                main, side, ok = ns_w[1, e - 12], high[e - 12], valid_n
            both = jnp.concatenate([main, side], axis=1)
            u = both[:LEV]
            v = both[LEV:]
            values = (
                1.0 - jnp.abs(u) - jnp.abs(v),
                jnp.maximum(u, 0.0),
                jnp.maximum(-u, 0.0),
                jnp.maximum(v, 0.0),
                jnp.maximum(-v, 0.0),
            )
            for i, value in enumerate(values):
                winds[i, e] = value if ok is None else value * ok

    def advance(dst, src, lo, hi, adjoint, emit):
        def body(e, carry):
            for var in range(4):
                at = slice(var * LEV, (var + 1) * LEV)
                x = field[src, e, at, :]
                below = field[src, e - 1, at, :]
                above = field[src, e + 1, at, :]
                if adjoint:
                    out = (
                        winds[0, e] * x
                        + pltpu.roll(winds[1, e] * x, LANES - 1, axis=1)
                        + pltpu.roll(winds[2, e] * x, 1, axis=1)
                        + winds[3, e + 1] * above
                        + winds[4, e - 1] * below
                    )
                else:
                    out = (
                        winds[0, e] * x
                        + winds[1, e] * pltpu.roll(x, 1, axis=1)
                        + winds[2, e] * pltpu.roll(x, LANES - 1, axis=1)
                        + winds[3, e] * below
                        + winds[4, e] * above
                    )
                emit(dst, e, at, out)
            return carry

        lax.fori_loop(lo, hi, body, 0)

    def put(dst, e, at, out):
        field[dst, e, at, :] = out

    def project(window, source):
        def body(r, carry):
            high, low = split(source(r))
            both = jnp.concatenate([high, low], axis=0).astype(BF16)
            out = mm(opp, both)
            proj[r, window * TYPES : (window + 1) * TYPES, :] = out[:8] + out[8:]
            return carry

        lax.fori_loop(0, LAT, body, 0)

    def message(dst, row):
        for w in range(WIN):
            dst[:, w, :] = stage[w * 128 : (w + 1) * 128, :].T
        dst[:, 3, :] = jnp.broadcast_to(row, (NDEV, 128))

    def total(recv):
        lanes = jnp.sum(recv[:, 3, :], axis=0, keepdims=True)
        return jnp.broadcast_to(jnp.sum(lanes, axis=1, keepdims=True), (1, 128))

    def wide(row):
        return jnp.concatenate([row, row], axis=1)

    def forward(it):
        pack_x[...] = pack_rows([res[r] for r in range(LAT)])
        for copy in halo_x():
            copy.start()
        project(0, lambda r: res[r])
        for copy in halo_x():
            copy.wait()
        own = sides(hp_x, 0, range(8))
        for r in range(LAT):
            field[0, r + 4, :, :256] = res[r]
            field[0, r + 4, :, 256:] = own[r]
        low = sides(hp_x, 2, range(4, 8))
        high = sides(hp_x, 4, range(0, 4))
        for e in range(4):
            field[0, e, :, :256] = ns_x[0, e] * valid_s
            field[0, e, :, 256:] = low[e] * valid_s
            field[0, e + 12, :, :256] = ns_x[1, e] * valid_n
            field[0, e + 12, :, 256:] = high[e] * valid_n
        advance(1, 0, 1, 15, False, put)
        advance(0, 1, 2, 14, False, put)
        project(1, lambda r: field[0, r + 4, :, :256])
        advance(1, 0, 3, 13, False, put)
        advance(0, 1, 4, 12, False, put)
        project(2, lambda r: field[0, r + 4, :, :256])
        for r in range(LAT):
            value = proj[r]
            pair = jnp.concatenate([value[:, :128], value[:, 128:]], axis=0)
            high, low = split(pair)
            lgather[r * 48 : (r + 1) * 48, :128] = high.astype(BF16)
            lgather[r * 48 : (r + 1) * 48, 128:] = low.astype(BF16)
        for n in range(8):
            hot = colhot[n]
            found = mm(lgather[...], jnp.concatenate([hot, hot], axis=0))
            band = jnp.broadcast_to(cols[:, n * 256 : (n + 1) * 256] >> 7, (WT, 256))
            got = found[:WT]
            for h in range(1, 16):
                got = jnp.where(band == h, found[h * WT : (h + 1) * WT], got)
            for half in range(2):
                for w in range(WIN):
                    stage[pl.ds(w * 128 + 2 * n + half, 8, stride=16), :] = got[
                        w * 8 : (w + 1) * 8, half * 128 : (half + 1) * 128
                    ]
        message(send_f, part[...])
        a2a_start(send_f, recv_f, 0)
        a2a_wait(send_f, recv_f, 0)
        norm = total(recv_f)
        beta = jnp.where(it == 1, jnp.zeros_like(norm), norm / rrv[...])
        rrv[...] = norm
        for w in range(WIN):
            table = recv_f[:, w, :].T
            high, low = split(table)
            for t in range(TYPES):
                at = slice(t * 16, (t + 1) * 16)
                tsplit[w * TYPES + t] = jnp.concatenate([high[at], low[at]], axis=0).astype(BF16)

        def look(b, acc):
            which = window_s[b] * TYPES + type_s[b]
            got = mm(tsplit[which], onehot[b])
            both = (got[:16] + got[16:]) * cweight[b]
            summed = (both[:, :128] + both[:, 128:256]) + (both[:, 256:384] + both[:, 384:])
            y = jnp.sum(summed, axis=0, keepdims=True) + beta * yrow[b]
            yrow[b] = y
            z = live[b] * y
            zrow[b] = z
            return acc + z * y

        quad = lax.fori_loop(0, NBLK, look, jnp.zeros((1, ROWS), F32), unroll=4)

        def turn(r, acc):
            p = res[r] + wide(beta) * dirn[r]
            dirn[r] = p
            return acc + jnp.sum((p * p).reshape(8, 8, LON), axis=0)

        pp = lax.fori_loop(0, LAT, turn, jnp.zeros((8, LON), F32))
        pp = jnp.sum(pp, axis=0, keepdims=True)
        part[...] = quad + pp[:, :128] + pp[:, 128:]

    def outer(it, carry):
        @pl.when(it > 0)
        def _():
            forward(it)

        def spread(b, c):
            z = zrow[b]
            value = cweight[b] * jnp.concatenate([z, z, z, z], axis=1)
            high, low = split(value)
            both = jnp.concatenate([high, low], axis=0).astype(BF16)
            out = mm_nt(both, onehot[b])
            rblk[b] = out[:16] + out[16:]
            return c

        lax.fori_loop(0, NBLK, spread, 0, unroll=4)
        for q in range(SLOTS):
            high, low = split(rblk[:, q, :])
            out = mm(member, high.astype(BF16)) + mm(member, low.astype(BF16))
            for w in range(WIN):
                stage[pl.ds(w * 128 + q, 8, stride=16), :] = out[w * 8 : (w + 1) * 8]
        message(send_b, part[...])
        a2a_start(send_b, recv_b, 1)

        @pl.when(it == 0)
        def _():
            build_winds()

        a2a_wait(send_b, recv_b, 1)
        for w in range(WIN):
            stage[w * 128 : (w + 1) * 128, :] = recv_b[:, w, :].T
        alpha = rrv[...] / total(recv_b)
        for n in range(8):
            halves = []
            for half in range(2):
                halves.append(
                    jnp.concatenate(
                        [stage[pl.ds(w * 128 + 2 * n + half, 8, stride=16), :] for w in range(WIN)],
                        axis=0,
                    )
                )
            high, low = split(jnp.concatenate(halves, axis=1))
            band = jnp.broadcast_to(cols[:, n * 256 : (n + 1) * 256] >> 7, (WT, 256))
            for r in range(LAT):
                for i, value in enumerate((high, low)):
                    pair = jnp.concatenate(
                        [
                            jnp.where(band == 2 * r, value, 0.0),
                            jnp.where(band == 2 * r + 1, value, 0.0),
                        ],
                        axis=0,
                    ).astype(BF16)
                    lscatter[r * 48 : (r + 1) * 48, i * 256 : (i + 1) * 256] = pair
            hot = colhot[n]
            out = mm_nt(lscatter[...], jnp.concatenate([hot, hot], axis=1))
            if n == 0:
                sacc[...] = out
            else:
                sacc[...] += out
        for r in range(LAT):
            ssum[r, :, :128] = sacc[r * 48 : r * 48 + WT, :]
            ssum[r, :, 128:] = sacc[r * 48 + WT : (r + 1) * 48, :]
        pack_s[...] = pack_rows([ssum[r] for r in range(LAT)])
        for copy in halo_s():
            copy.start()
        for copy in halo_s():
            copy.wait()
        own = sides(hp_s, 0, range(8))
        low = sides(hp_s, 2, range(4, 8))
        high = sides(hp_s, 4, range(0, 4))
        for r in range(LAT):
            sext[r + 4, :, :256] = ssum[r]
            sext[r + 4, :, 256:] = own[r]
        for e in range(4):
            sext[e, :, :256] = ns_s[0, e]
            sext[e, :, 256:] = low[e]
            sext[e + 12, :, :256] = ns_s[1, e]
            sext[e + 12, :, 256:] = high[e]

        def forcing(e, window):
            high, low = split(sext[e, window * TYPES : (window + 1) * TYPES, :])
            return mm(opt, jnp.concatenate([high, high, low, low], axis=0).astype(BF16))

        def last(e, c):
            field[0, e] = forcing(e, 2)
            return c

        def middle(e, c):
            field[0, e] += forcing(e, 1)
            return c

        lax.fori_loop(0, EXT, last, 0, unroll=2)
        advance(1, 0, 1, 15, True, put)
        advance(0, 1, 2, 14, True, put)
        lax.fori_loop(2, 14, middle, 0, unroll=2)
        advance(1, 0, 3, 13, True, put)
        advance(0, 1, 4, 12, True, put)

        def result(r):
            return field[0, r + 4, :, :256] + forcing(r + 4, 0)[:, :256]

        @pl.when(it == 0)
        def _():
            def body(r, acc):
                value = result(r)
                res[r] = value
                return acc + jnp.sum((value * value).reshape(8, 8, LON), axis=0)

            acc = lax.fori_loop(0, LAT, body, jnp.zeros((8, LON), F32))
            acc = jnp.sum(acc, axis=0, keepdims=True)
            part[...] = acc[:, :128] + acc[:, 128:]

        @pl.when(it > 0)
        def _():
            scale = wide(alpha)

            def body(r, acc):
                p = dirn[r]
                q = p + result(r)
                x = inc[r] + scale * p
                value = res[r] - scale * q
                inc[r] = x
                res[r] = value
                return acc + jnp.sum((value * value).reshape(8, 8, LON), axis=0)

            acc = lax.fori_loop(0, LAT, body, jnp.zeros((8, LON), F32))
            acc = jnp.sum(acc, axis=0, keepdims=True)
            part[...] = acc[:, :128] + acc[:, 128:]

        return carry

    lax.fori_loop(0, 3, outer, 0)
    x_out[...] = inc[...]
    r_out[...] = res[...]


def shards(
    zonal_wind, merid_wind, operator_rows, innovation, error_weight, interp_weight, obs_slot,
    block_count, block_type, block_window, send_cols,
):
    op2 = jnp.tile(operator_rows, (1, 2))
    opt4 = jnp.tile(operator_rows.T, (1, 4))
    cols = send_cols.reshape(NDEV, SLOTS).T.reshape(1, NDEV * SLOTS)
    meta = jnp.stack([block_type, block_window])
    vm = pl.BlockSpec(memory_space=pltpu.VMEM)
    sm = pl.BlockSpec(memory_space=pltpu.SMEM)
    V = pltpu.VMEM
    dma = pltpu.SemaphoreType.DMA
    x, r = pl.pallas_call(
        kernel,
        out_shape=[jax.ShapeDtypeStruct((LAT, CH, LON), F32)] * 2,
        in_specs=[vm] * 10 + [sm] * 3,
        out_specs=[vm] * 2,
        scratch_shapes=[
            V((5, EXT, LEV, LANES), F32),
            V((2, EXT, CH, LANES), F32),
            V((LAT, CH, LON), F32),
            V((LAT, CH, LON), F32),
            V((LAT, CH, LON), F32),
            V((8, 128), F32),
            V((NBLK, NDEV, KPTS * ROWS), BF16),
            V((NBLK, SLOTS, KPTS * ROWS), F32),
            V((NBLK, 1, ROWS), F32),
            V((NBLK, 1, ROWS), F32),
            V((NBLK, 1, ROWS), F32),
            V((NBLK, SLOTS, NDEV), F32),
            V((WT, 32, NDEV), BF16),
            V((8, 128, 256), BF16),
            V((LAT, WT, LON), F32),
            V((LAT, WT, LON), F32),
            V((EXT, WT, LANES), F32),
            V((WIN * 128, 128), F32),
            V((16 * WT, 256), BF16),
            V((16 * WT, 512), BF16),
            V((16 * WT, 128), F32),
            V((NDEV, 4, 128), F32),
            V((NDEV, 4, 128), F32),
            V((NDEV, 4, 128), F32),
            V((NDEV, 4, 128), F32),
            V((LAT, 2 * LEV, LON), F32),
            V((2 * LEV, 128), F32),
            V((CH, 128), F32),
            V((WT, 128), F32),
            V((2, 4, 2 * LEV, LON), F32),
            V((2, 4, CH, LON), F32),
            V((2, 4, WT, LON), F32),
            V((6, 2 * LEV, 128), F32),
            V((6, CH, 128), F32),
            V((6, WT, 128), F32),
            V((1, 128), F32),
            V((1, 128), F32),
            dma((2,)),
            dma((2,)),
            dma((8,)),
            dma((8,)),
            dma((8,)),
            dma((8,)),
            dma((8,)),
            dma((8,)),
        ],
        compiler_params=pltpu.CompilerParams(
            collective_id=0, has_side_effects=True, vmem_limit_bytes=60 << 20
        ),
        name="cg",
    )(
        zonal_wind, merid_wind, op2, opt4,
        innovation.reshape(NBLK, 1, ROWS), error_weight.reshape(NBLK, 1, ROWS),
        interp_weight, obs_slot, cols, meta, block_count, block_type, block_window,
    )
    shape = (4, LEV, LAT, LON)
    return x.transpose(1, 0, 2).reshape(shape), r.transpose(1, 0, 2).reshape(shape)


def solution(mesh):
    both = ("lat", "lon")
    in_specs = (
        P(None, "lat", "lon"),
        P(None, "lat", "lon"),
        P(),
        P(both),
        P(both),
        P(None, both),
        P(None, both),
        P(both),
        P(both),
        P(both),
        P(both, None),
    )
    out_specs = (P(None, None, "lat", "lon"), P(None, None, "lat", "lon"))
    return jax.shard_map(shards, mesh=mesh, in_specs=in_specs, out_specs=out_specs, check_vma=False)
```

```python
import functools

import jax
import jax.numpy as jnp
from jax import lax
from jax.experimental import pallas as pl
from jax.experimental.pallas import tpu as pltpu
from jax.sharding import PartitionSpec as P

MESH = pl.DeviceIdType.MESH
F32 = jnp.float32
BF16 = jnp.bfloat16

TYPES = 8
WIN = 3
WT = WIN * TYPES
KPTS = 4
SLOTS = 16
ROWS = 128
N_LAT = 8
N_LON = 16
NDEV = N_LAT * N_LON
NBLK = 32
LEV = 16
CH = 64
LAT = 8
LON = 256
EXT = 16
LANES = 384
NT = (((1,), (1,)), ((), ()))


def split(value):
    high = value.astype(BF16).astype(F32)
    return high, value - high


def mm(left, right):
    return jnp.dot(left, right, preferred_element_type=F32)


def mm_nt(left, right):
    return lax.dot_general(left, right, NT, preferred_element_type=F32)


def pack_rows(rows):
    packed = None
    for r, row in enumerate(rows):
        lane = lax.broadcasted_iota(jnp.int32, (row.shape[0], 128), 1)
        ends = jnp.where(lane < 64, row[:, :128], row[:, 128:])
        moved = pltpu.roll(ends, 4 + 16 * r, axis=1)
        packed = moved if packed is None else jnp.where((lane >> 4) == r, moved, packed)
    return packed


def kernel(
    zonal, merid, rows_in, innov, weight, interp, slots, cols, type_v, window_v,
    count_s, type_s, window_s,
    x_out, r_out,
    winds, field, res, dirn, inc, force0, force1, square,
    onehot, cweight, live, zrow, yrow, rblk, tsplit,
    colhot, proj, ssum, sext, stage, lgather, lscatter, sacc,
    send_f, send_b, recv_f, recv_b, wown,
    pack_w, pack_x, pack_s, ns_w, ns_x, ns_s, hp_w, hp_x, hp_s, rrv, part,
    a2a_send, a2a_recv, hw_send, hw_recv, hx_send, hx_recv, hs_send, hs_recv,
):
    lat = lax.axis_index("lat")
    lon = lax.axis_index("lon")
    me = lat * N_LON + lon
    barrier = pltpu.get_barrier_semaphore()

    lons = [lax.rem(lon + j, N_LON) for j in range(N_LON)]

    def everyone(act):
        def far(i, carry):
            a = lax.rem(lat + i, N_LAT)
            for o in lons:
                act(a, o)
            return carry

        lax.fori_loop(1, N_LAT, far, 0)
        for o in lons[1:]:
            act(lat, o)

    def greet(a, o):
        pl.semaphore_signal(
            barrier, inc=1, device_id={"lat": a, "lon": o}, device_id_type=MESH
        )

    everyone(greet)

    north = lax.rem(lat + 1, N_LAT)
    south = lax.rem(lat + N_LAT - 1, N_LAT)
    east = lax.rem(lon + 1, N_LON)
    west = lax.rem(lon + N_LON - 1, N_LON)
    valid_s = jnp.where(lat > 0, 1.0, 0.0).astype(F32)
    valid_n = jnp.where(lat < N_LAT - 1, 1.0, 0.0).astype(F32)

    def halo(low, high, pack, ns, hp, send, recv):
        copies = [
            (high, ns.at[0], north, lon),
            (low, ns.at[1], south, lon),
            (pack, hp.at[0], lat, east),
            (pack, hp.at[1], lat, west),
            (pack, hp.at[2], north, east),
            (pack, hp.at[3], north, west),
            (pack, hp.at[4], south, east),
            (pack, hp.at[5], south, west),
        ]
        return [
            pltpu.make_async_remote_copy(
                src, dst, send.at[i], recv.at[i], device_id={"lat": a, "lon": o}, device_id_type=MESH
            )
            for i, (src, dst, a, o) in enumerate(copies)
        ]

    def halo_w():
        return halo(wown.at[pl.ds(0, 4)], wown.at[pl.ds(4, 4)], pack_w, ns_w, hp_w, hw_send, hw_recv)

    def halo_x():
        return halo(res.at[pl.ds(0, 4)], res.at[pl.ds(4, 4)], pack_x, ns_x, hp_x, hx_send, hx_recv)

    def halo_s():
        return halo(ssum.at[pl.ds(0, 4)], ssum.at[pl.ds(4, 4)], pack_s, ns_s, hp_s, hs_send, hs_recv)

    def sides(hp, base, rows):
        lane = lax.broadcasted_iota(jnp.int32, hp.shape[1:], 1)
        both = jnp.where((lane & 15) < 4, hp[base], hp[base + 1])
        return [pltpu.roll(both, (256 - 16 * r - 4) % 128, axis=1) for r in rows]

    def a2a_start(src, dst, k):
        def go(a, o):
            pltpu.make_async_remote_copy(
                src.at[a * N_LON + o], dst.at[me], a2a_send.at[k], a2a_recv.at[k],
                device_id={"lat": a, "lon": o}, device_id_type=MESH,
            ).start()

        everyone(go)
        dst[me] = src[me]

    def a2a_wait(src, dst, k):
        got = dst.at[pl.ds(0, NDEV - 1)]
        pltpu.make_async_copy(got, got, a2a_recv.at[k]).wait()
        gone = src.at[pl.ds(0, NDEV - 1)]
        pltpu.make_async_copy(gone, gone, a2a_send.at[k]).wait()

    for r in range(LAT):
        wown[r, :LEV, :] = zonal[:, r, :]
        wown[r, LEV:, :] = merid[:, r, :]
    pack_w[...] = pack_rows([wown[r] for r in range(LAT)])

    def tables(b, carry):
        at = pl.ds(pl.multiple_of(b * ROWS, ROWS), ROWS)
        slot = slots[:, at]
        wgt = interp[:, at]
        sender = slot >> 4
        inner = slot & 15
        sub = lax.broadcasted_iota(jnp.int32, (NDEV, ROWS), 0)
        sub16 = lax.broadcasted_iota(jnp.int32, (SLOTS, ROWS), 0)
        for k in range(KPTS):
            lanes = slice(k * ROWS, (k + 1) * ROWS)
            onehot[b, :, lanes] = jnp.where(sub == sender[k : k + 1], 1.0, 0.0).astype(BF16)
            cweight[b, :, lanes] = jnp.where(sub16 == inner[k : k + 1], wgt[k : k + 1], 0.0)
        lane = lax.broadcasted_iota(jnp.int32, (1, ROWS), 1)
        wl = jnp.where(lane < count_s[b], weight[b], 0.0)
        live[b] = wl
        zrow[b] = wl * innov[b]
        yrow[b] = jnp.zeros((1, ROWS), F32)
        return carry

    lax.fori_loop(0, NBLK, tables, 0, unroll=2)
    for n in range(8):
        low = cols[:, n * 256 : (n + 1) * 256] & 255
        sub = lax.broadcasted_iota(jnp.int32, (LON, 256), 0)
        colhot[n] = jnp.where(sub == low, 1.0, 0.0).astype(BF16)
    lane32 = lax.broadcasted_iota(jnp.int32, (CH, 32), 1)
    square[...] = jnp.zeros_like(square)
    for i in range(4):
        square[i * TYPES : (i + 1) * TYPES, :CH] = rows_in[...]
    opt_h, opt_l = split(square[...].T[:CH, :32])
    opt = jnp.where((lane32 & 8) == 0, opt_h, opt_l).astype(BF16)
    op1 = square[:TYPES, :]
    op_h, op_l = split(op1 + pltpu.roll(op1, CH, axis=1))
    opp = jnp.concatenate([op_h, op_l], axis=0).astype(BF16)
    ids = window_v[...] * TYPES + type_v[...]
    member = jnp.where(lax.broadcasted_iota(jnp.int32, (32, NBLK), 0) == ids, 1.0, 0.0).astype(BF16)
    for r in range(LAT):
        dirn[r] = jnp.zeros((CH, LON), F32)
        inc[r] = jnp.zeros((CH, LON), F32)
    rrv[...] = jnp.ones((1, 128), F32)
    part[...] = jnp.zeros((1, 128), F32)

    pl.semaphore_wait(barrier, NDEV - 1)
    for copy in halo_w():
        copy.start()

    def build_winds():
        for copy in halo_w():
            copy.wait()
        tiles = [None] * EXT
        own = sides(hp_w, 0, range(8))
        low = sides(hp_w, 2, range(4, 8))
        high = sides(hp_w, 4, range(0, 4))
        for e in range(EXT):
            if e < 4:
                main, side, ok = ns_w[0, e], low[e], valid_s
            elif e < 12:
                main, side, ok = wown[e - 4], own[e - 4], None
            else:
                main, side, ok = ns_w[1, e - 12], high[e - 12], valid_n
            both = jnp.concatenate([main, side], axis=1)
            u = both[:LEV]
            v = both[LEV:]
            values = (
                1.0 - jnp.abs(u) - jnp.abs(v),
                jnp.maximum(u, 0.0),
                jnp.maximum(-u, 0.0),
                jnp.maximum(v, 0.0),
                jnp.maximum(-v, 0.0),
            )
            for i, value in enumerate(values):
                winds[i, e] = value if ok is None else value * ok

    def advance(dst, src, lo, hi, adjoint, unroll, extra=None):
        def body(e, carry):
            for var in range(4):
                at = slice(var * LEV, (var + 1) * LEV)
                x = field[src, e, at, :]
                below = field[src, e - 1, at, :]
                above = field[src, e + 1, at, :]
                if adjoint:
                    out = (
                        winds[0, e] * x
                        + pltpu.roll(winds[1, e] * x, LANES - 1, axis=1)
                        + pltpu.roll(winds[2, e] * x, 1, axis=1)
                        + winds[3, e + 1] * above
                        + winds[4, e - 1] * below
                    )
                else:
                    out = (
                        winds[0, e] * x
                        + winds[1, e] * pltpu.roll(x, 1, axis=1)
                        + winds[2, e] * pltpu.roll(x, LANES - 1, axis=1)
                        + winds[3, e] * below
                        + winds[4, e] * above
                    )
                field[dst, e, at, :] = out if extra is None else out + extra[e, at, :]
            return carry

        lax.fori_loop(lo, hi, body, 0, unroll=unroll)

    def project(window, source):
        def body(r, carry):
            high, low = split(source(r))
            both = jnp.concatenate([high, low], axis=0).astype(BF16)
            out = mm(opp, both)
            proj[r, window * TYPES : (window + 1) * TYPES, :] = out[:8] + out[8:]
            return carry

        lax.fori_loop(0, LAT, body, 0, unroll=4)

    def message(dst, row):
        for w in range(WIN):
            dst[:, w, :] = stage[w * 128 : (w + 1) * 128, :].T
        dst[:, 3, :] = jnp.broadcast_to(row, (NDEV, 128))

    def total(recv):
        lanes = jnp.sum(recv[:, 3, :], axis=0, keepdims=True)
        return jnp.broadcast_to(jnp.sum(lanes, axis=1, keepdims=True), (1, 128))

    def wide(row):
        return jnp.concatenate([row, row], axis=1)

    def forward(it):
        pack_x[...] = pack_rows([res[r] for r in range(LAT)])
        for copy in halo_x():
            copy.start()
        project(0, lambda r: res[r])
        copies = halo_x()
        for copy in copies[2:4]:
            copy.wait()
        own = sides(hp_x, 0, range(8))
        for r in range(LAT):
            field[0, r + 4, :, :256] = res[r]
            field[0, r + 4, :, 256:] = own[r]
        advance(1, 0, 5, 11, False, 3)
        for copy in copies[:2] + copies[4:]:
            copy.wait()
        low = sides(hp_x, 2, range(4, 8))
        high = sides(hp_x, 4, range(0, 4))
        for e in range(4):
            field[0, e, :, :256] = ns_x[0, e] * valid_s
            field[0, e, :, 256:] = low[e] * valid_s
            field[0, e + 12, :, :256] = ns_x[1, e] * valid_n
            field[0, e + 12, :, 256:] = high[e] * valid_n
        advance(1, 0, 1, 5, False, 4)
        advance(1, 0, 11, 15, False, 4)
        advance(0, 1, 2, 14, False, 6)
        project(1, lambda r: field[0, r + 4, :, :256])
        advance(1, 0, 3, 13, False, 5)
        advance(0, 1, 4, 12, False, 4)
        project(2, lambda r: field[0, r + 4, :, :256])
        for r in range(LAT):
            lgather[r * 48 : (r + 1) * 48, :] = jnp.concatenate(split(proj[r]), axis=0).astype(BF16)
        for n in range(8):
            found = mm(lgather[...], colhot[n])
            band = jnp.broadcast_to(cols[:, n * 256 : (n + 1) * 256] >> 8, (WT, 256))
            got = found[:WT] + found[WT : 2 * WT]
            for r in range(1, LAT):
                at = r * 2 * WT
                got = jnp.where(band == r, found[at : at + WT] + found[at + WT : at + 2 * WT], got)
            for half in range(2):
                for w in range(WIN):
                    stage[pl.ds(w * 128 + 2 * n + half, 8, stride=16), :] = got[
                        w * 8 : (w + 1) * 8, half * 128 : (half + 1) * 128
                    ]
        message(send_f, part[...])
        a2a_start(send_f, recv_f, 0)
        a2a_wait(send_f, recv_f, 0)
        norm = total(recv_f)
        beta = jnp.where(it == 1, jnp.zeros_like(norm), norm / rrv[...])
        rrv[...] = norm
        for w in range(WIN):
            table = recv_f[:, w, :].T
            high, low = split(table)
            for t in range(TYPES):
                at = slice(t * 16, (t + 1) * 16)
                tsplit[w * TYPES + t] = jnp.concatenate([high[at], low[at]], axis=0).astype(BF16)

        def look(b, acc):
            which = window_s[b] * TYPES + type_s[b]
            got = mm(tsplit[which], onehot[b])
            both = (got[:16] + got[16:]) * cweight[b]
            summed = (both[:, :128] + both[:, 128:256]) + (both[:, 256:384] + both[:, 384:])
            y = jnp.sum(summed, axis=0, keepdims=True) + beta * yrow[b]
            yrow[b] = y
            z = live[b] * y
            zrow[b] = z
            return acc + z * y

        quad = lax.fori_loop(0, NBLK, look, jnp.zeros((1, ROWS), F32), unroll=8)

        def turn(r, acc):
            p = res[r] + wide(beta) * dirn[r]
            dirn[r] = p
            return acc + jnp.sum((p * p).reshape(8, 8, LON), axis=0)

        pp = lax.fori_loop(0, LAT, turn, jnp.zeros((8, LON), F32))
        pp = jnp.sum(pp, axis=0, keepdims=True)
        part[...] = quad + pp[:, :128] + pp[:, 128:]

    def outer(it, carry):
        @pl.when(it > 0)
        def _():
            forward(it)

        def spread(b, c):
            z = zrow[b]
            value = cweight[b] * jnp.concatenate([z, z, z, z], axis=1)
            high, low = split(value)
            both = jnp.concatenate([high, low], axis=0).astype(BF16)
            out = mm_nt(both, onehot[b])
            rblk[b] = out[:16] + out[16:]
            return c

        lax.fori_loop(0, NBLK, spread, 0, unroll=8)
        for q in range(SLOTS):
            high, low = split(rblk[:, q, :])
            out = mm(member, high.astype(BF16)) + mm(member, low.astype(BF16))
            for w in range(WIN):
                stage[pl.ds(w * 128 + q, 8, stride=16), :] = out[w * 8 : (w + 1) * 8]
        message(send_b, part[...])
        a2a_start(send_b, recv_b, 1)

        @pl.when(it == 0)
        def _():
            build_winds()

        a2a_wait(send_b, recv_b, 1)
        for w in range(WIN):
            stage[w * 128 : (w + 1) * 128, :] = recv_b[:, w, :].T
        alpha = rrv[...] / total(recv_b)
        for n in range(8):
            halves = []
            for half in range(2):
                halves.append(
                    jnp.concatenate(
                        [stage[pl.ds(w * 128 + 2 * n + half, 8, stride=16), :] for w in range(WIN)],
                        axis=0,
                    )
                )
            high, low = split(jnp.concatenate(halves, axis=1))
            band = jnp.broadcast_to(cols[:, n * 256 : (n + 1) * 256] >> 8, (WT, 256))
            for r in range(LAT):
                here = band == r
                lscatter[r * 48 : (r + 1) * 48, :] = jnp.concatenate(
                    [jnp.where(here, high, 0.0), jnp.where(here, low, 0.0)], axis=0
                ).astype(BF16)
            out = mm_nt(lscatter[...], colhot[n])
            if n == 0:
                sacc[...] = out
            else:
                sacc[...] += out
        for r in range(LAT):
            ssum[r] = sacc[r * 48 : r * 48 + WT, :] + sacc[r * 48 + WT : (r + 1) * 48, :]
        pack_s[...] = pack_rows([ssum[r] for r in range(LAT)])
        copies = halo_s()
        for copy in copies:
            copy.start()

        def forcing(value):
            high, low = split(value)
            return mm(opt, jnp.concatenate([high, high, low, low], axis=0).astype(BF16))

        def nearest(r, c):
            force0[r] = forcing(ssum[r, :TYPES, :])
            return c

        def middle(e, c):
            force1[e] = forcing(sext[e, TYPES : 2 * TYPES, :])
            return c

        def last(e, c):
            field[0, e] = forcing(sext[e, 2 * TYPES :, :])
            return c

        lax.fori_loop(0, LAT, nearest, 0, unroll=4)
        for copy in copies[2:4]:
            copy.wait()
        own = sides(hp_s, 0, range(8))
        for r in range(LAT):
            sext[r + 4, :, :256] = ssum[r]
            sext[r + 4, :, 256:] = own[r]
        lax.fori_loop(4, 12, last, 0, unroll=4)
        lax.fori_loop(4, 12, middle, 0, unroll=4)
        advance(1, 0, 5, 11, True, 3)
        for copy in copies[:2] + copies[4:]:
            copy.wait()
        low = sides(hp_s, 2, range(4, 8))
        high = sides(hp_s, 4, range(0, 4))
        for e in range(4):
            sext[e, :, :256] = ns_s[0, e]
            sext[e, :, 256:] = low[e]
            sext[e + 12, :, :256] = ns_s[1, e]
            sext[e + 12, :, 256:] = high[e]
        lax.fori_loop(0, 4, last, 0, unroll=4)
        lax.fori_loop(12, 16, last, 0, unroll=4)
        lax.fori_loop(2, 4, middle, 0, unroll=2)
        lax.fori_loop(12, 14, middle, 0, unroll=2)
        advance(1, 0, 1, 5, True, 4)
        advance(1, 0, 11, 15, True, 4)
        advance(0, 1, 2, 14, True, 6, force1)
        advance(1, 0, 3, 13, True, 5)
        advance(0, 1, 4, 12, True, 4)

        def result(r):
            return field[0, r + 4, :, :256] + force0[r]

        @pl.when(it == 0)
        def _():
            def body(r, acc):
                value = result(r)
                res[r] = value
                return acc + jnp.sum((value * value).reshape(8, 8, LON), axis=0)

            acc = lax.fori_loop(0, LAT, body, jnp.zeros((8, LON), F32))
            acc = jnp.sum(acc, axis=0, keepdims=True)
            part[...] = acc[:, :128] + acc[:, 128:]

        @pl.when(it > 0)
        def _():
            scale = wide(alpha)

            def body(r, acc):
                p = dirn[r]
                q = p + result(r)
                x = inc[r] + scale * p
                value = res[r] - scale * q
                inc[r] = x
                res[r] = value
                return acc + jnp.sum((value * value).reshape(8, 8, LON), axis=0)

            acc = lax.fori_loop(0, LAT, body, jnp.zeros((8, LON), F32))
            acc = jnp.sum(acc, axis=0, keepdims=True)
            part[...] = acc[:, :128] + acc[:, 128:]

        return carry

    lax.fori_loop(0, 3, outer, 0)
    x_out[...] = inc[...]
    r_out[...] = res[...]


def shards(
    zonal_wind, merid_wind, operator_rows, innovation, error_weight, interp_weight, obs_slot,
    block_count, block_type, block_window, send_cols,
):
    cols = send_cols.reshape(NDEV, SLOTS).T.reshape(1, NDEV * SLOTS)
    vm = pl.BlockSpec(memory_space=pltpu.VMEM)
    sm = pl.BlockSpec(memory_space=pltpu.SMEM)
    V = pltpu.VMEM
    dma = pltpu.SemaphoreType.DMA
    x, r = pl.pallas_call(
        kernel,
        out_shape=[jax.ShapeDtypeStruct((LAT, CH, LON), F32)] * 2,
        in_specs=[vm] * 10 + [sm] * 3,
        out_specs=[vm] * 2,
        scratch_shapes=[
            V((5, EXT, LEV, LANES), F32),
            V((2, EXT, CH, LANES), F32),
            V((LAT, CH, LON), F32),
            V((LAT, CH, LON), F32),
            V((LAT, CH, LON), F32),
            V((LAT, CH, LON), F32),
            V((EXT, CH, LANES), F32),
            V((128, 128), F32),
            V((NBLK, NDEV, KPTS * ROWS), BF16),
            V((NBLK, SLOTS, KPTS * ROWS), F32),
            V((NBLK, 1, ROWS), F32),
            V((NBLK, 1, ROWS), F32),
            V((NBLK, 1, ROWS), F32),
            V((NBLK, SLOTS, NDEV), F32),
            V((WT, 32, NDEV), BF16),
            V((8, LON, 256), BF16),
            V((LAT, WT, LON), F32),
            V((LAT, WT, LON), F32),
            V((EXT, WT, LANES), F32),
            V((WIN * 128, 128), F32),
            V((16 * WT, 256), BF16),
            V((16 * WT, 256), BF16),
            V((16 * WT, 256), F32),
            V((NDEV, 4, 128), F32),
            V((NDEV, 4, 128), F32),
            V((NDEV, 4, 128), F32),
            V((NDEV, 4, 128), F32),
            V((LAT, 2 * LEV, LON), F32),
            V((2 * LEV, 128), F32),
            V((CH, 128), F32),
            V((WT, 128), F32),
            V((2, 4, 2 * LEV, LON), F32),
            V((2, 4, CH, LON), F32),
            V((2, 4, WT, LON), F32),
            V((6, 2 * LEV, 128), F32),
            V((6, CH, 128), F32),
            V((6, WT, 128), F32),
            V((1, 128), F32),
            V((1, 128), F32),
            dma((2,)),
            dma((2,)),
            dma((8,)),
            dma((8,)),
            dma((8,)),
            dma((8,)),
            dma((8,)),
            dma((8,)),
        ],
        compiler_params=pltpu.CompilerParams(
            collective_id=0, has_side_effects=True, vmem_limit_bytes=60 << 20
        ),
        name="cg",
    )(
        zonal_wind, merid_wind, operator_rows,
        innovation.reshape(NBLK, 1, ROWS), error_weight.reshape(NBLK, 1, ROWS),
        interp_weight, obs_slot, cols, block_type.reshape(1, NBLK), block_window.reshape(1, NBLK),
        block_count, block_type, block_window,
    )
    shape = (4, LEV, LAT, LON)
    return x.transpose(1, 0, 2).reshape(shape), r.transpose(1, 0, 2).reshape(shape)


def solution(mesh):
    both = ("lat", "lon")
    in_specs = (
        P(None, "lat", "lon"),
        P(None, "lat", "lon"),
        P(),
        P(both),
        P(both),
        P(None, both),
        P(None, both),
        P(both),
        P(both),
        P(both),
        P(both, None),
    )
    out_specs = (P(None, None, "lat", "lon"), P(None, None, "lat", "lon"))
    return jax.shard_map(shards, mesh=mesh, in_specs=in_specs, out_specs=out_specs, check_vma=False)
```

```python
import functools

import jax
import jax.numpy as jnp
from jax import lax
from jax.experimental import pallas as pl
from jax.experimental.pallas import tpu as pltpu
from jax.sharding import PartitionSpec as P

MESH = pl.DeviceIdType.MESH
F32 = jnp.float32
BF16 = jnp.bfloat16

TYPES = 8
WIN = 3
WT = WIN * TYPES
KPTS = 4
SLOTS = 16
ROWS = 128
N_LAT = 8
N_LON = 16
NDEV = N_LAT * N_LON
NBLK = 32
LEV = 16
CH = 64
LAT = 8
LON = 256
EXT = 24
MID = 16
LANES = 384
NT = (((1,), (1,)), ((), ()))


def split(value):
    high = value.astype(BF16).astype(F32)
    return high, value - high


def mm(left, right):
    return jnp.dot(left, right, preferred_element_type=F32)


def mm_nt(left, right):
    return lax.dot_general(left, right, NT, preferred_element_type=F32)


def pack_rows(rows):
    packed = None
    for r, row in enumerate(rows):
        lane = lax.broadcasted_iota(jnp.int32, (row.shape[0], 128), 1)
        ends = jnp.where(lane < 64, row[:, :128], row[:, 128:])
        moved = pltpu.roll(ends, (8 + 16 * r) % 128, axis=1)
        packed = moved if packed is None else jnp.where((lane >> 4) == r, moved, packed)
    return packed


def offsets():
    steps = [
        (dx, dc, dy, dz)
        for dx in range(4) for dc in range(2) for dy in range(4) for dz in range(4)
    ][1:]
    return sorted(steps, key=lambda t: -sum(min(d, 4 - d) for d in (t[0], t[2], t[3])))


def kernel(
    zonal, merid, rows_in, innov, weight, interp, slots, cols, type_v, window_v,
    count_s, type_s, window_s,
    x_out, r_out,
    winds, field, res, dirn, inc, force0, force1, square, colq,
    onehot, cweight, live, zrow, yrow, rblk, tsplit,
    colhot, proj, ssum, sside, stage, lgather, lscatter, sacc,
    send_f, send_b, recv_f, recv_b, wown,
    pack_w, pack_s, ns_w, ns_s, hp_w, hp_s, rrv, part, betav,
    a2a_send, a2a_recv, hw_send, hw_recv, hs_send, hs_recv,
):
    lat = lax.axis_index("lat")
    lon = lax.axis_index("lon")
    me = lat * N_LON + lon
    barrier = pltpu.get_barrier_semaphore()

    x, core = lat // 2, lax.rem(lat, 2)
    y, z = lon // 4, lax.rem(lon, 4)
    lats = {
        (dx, dc): lax.rem(x + dx, 4) * 2 + lax.rem(core + dc, 2)
        for dx in range(4) for dc in range(2)
    }
    lons = {
        (dy, dz): lax.rem(y + dy, 4) * 4 + lax.rem(z + dz, 4)
        for dy in range(4) for dz in range(4)
    }

    def everyone(act):
        for dx, dc, dy, dz in offsets():
            act(lats[dx, dc], lons[dy, dz])

    def plain(a, o):
        return a * N_LON + o

    def swapped(a, o):
        return lax.rem(o, 8) * 16 + a * 2 + o // 8

    def greet(a, o):
        pl.semaphore_signal(
            barrier, inc=1, device_id={"lat": a, "lon": o}, device_id_type=MESH
        )

    everyone(greet)

    north = lax.rem(lat + 1, N_LAT)
    south = lax.rem(lat + N_LAT - 1, N_LAT)
    east = lax.rem(lon + 1, N_LON)
    west = lax.rem(lon + N_LON - 1, N_LON)
    valid_s = jnp.where(lat > 0, 1.0, 0.0).astype(F32)
    valid_n = jnp.where(lat < N_LAT - 1, 1.0, 0.0).astype(F32)

    def to(src, dst, a, o, send, recv):
        return pltpu.make_async_remote_copy(
            src, dst, send, recv, device_id={"lat": a, "lon": o}, device_id_type=MESH
        )

    def edges(pack, hp, send, recv):
        targets = [
            (north, east), (north, west), (south, east), (south, west), (lat, east), (lat, west)
        ]
        return [
            to(pack, hp.at[i], a, o, send.at[i], recv.at[i]) for i, (a, o) in enumerate(targets)
        ]

    def halo_w():
        return edges(pack_w, hp_w, hw_send, hw_recv) + [
            to(wown, ns_w.at[0], north, lon, hw_send.at[6], hw_recv.at[6]),
            to(wown, ns_w.at[1], south, lon, hw_send.at[7], hw_recv.at[7]),
        ]

    def halo_s(deep):
        copies = edges(pack_s, hp_s, hs_send, hs_recv)
        k = 6
        for w, count in ((2, 8 if deep else 4), (1, 6 if deep else 2), (0, 4 if deep else 0)):
            if count == 0:
                continue
            high = pl.ds(w * LAT + LAT - count, count)
            low = pl.ds(w * LAT, count)
            copies.append(to(ssum.at[high], ns_s.at[0, high], north, lon, hs_send.at[k], hs_recv.at[k]))
            copies.append(
                to(ssum.at[low], ns_s.at[1, low], south, lon, hs_send.at[k + 1], hs_recv.at[k + 1])
            )
            k += 2
        return copies

    def sides(hp, base):
        lane = lax.broadcasted_iota(jnp.int32, hp.shape[1:], 1)
        both = jnp.where((lane & 15) < 8, hp[base], hp[base + 1])
        return [pltpu.roll(both, (256 - 16 * r - 8) % 128, axis=1) for r in range(LAT)]

    def a2a_start(src, dst, k, row_of, mine):
        def go(a, o):
            to(
                src.at[row_of(a, o)], dst.at[mine], a, o, a2a_send.at[k], a2a_recv.at[k]
            ).start()

        everyone(go)
        dst[mine] = src[row_of(lat, lon)]

    def a2a_wait(src, dst, k):
        got = dst.at[pl.ds(0, NDEV - 1)]
        pltpu.make_async_copy(got, got, a2a_recv.at[k]).wait()
        gone = src.at[pl.ds(0, NDEV - 1)]
        pltpu.make_async_copy(gone, gone, a2a_send.at[k]).wait()

    for r in range(LAT):
        wown[r, :LEV, :] = zonal[:, r, :]
        wown[r, LEV:, :] = merid[:, r, :]
    pack_w[...] = pack_rows([wown[r] for r in range(LAT)])

    def tables(b, carry):
        at = pl.ds(pl.multiple_of(b * ROWS, ROWS), ROWS)
        slot = slots[:, at]
        wgt = interp[:, at]
        sender = slot >> 4
        inner = slot & 15
        sub = lax.broadcasted_iota(jnp.int32, (NDEV, ROWS), 0)
        sub16 = lax.broadcasted_iota(jnp.int32, (SLOTS, ROWS), 0)
        for k in range(KPTS):
            lanes = slice(k * ROWS, (k + 1) * ROWS)
            onehot[b, :, lanes] = jnp.where(sub == sender[k : k + 1], 1.0, 0.0).astype(BF16)
            cweight[b, :, lanes] = jnp.where(sub16 == inner[k : k + 1], wgt[k : k + 1], 0.0)
        lane = lax.broadcasted_iota(jnp.int32, (1, ROWS), 1)
        wl = jnp.where(lane < count_s[b], weight[b], 0.0)
        live[b] = wl
        zrow[b] = wl * innov[b]
        yrow[b] = jnp.zeros((1, ROWS), F32)
        return carry

    lax.fori_loop(0, NBLK, tables, 0, unroll=2)
    raw = jnp.concatenate([cols[:, a * 128 : (a + 1) * 128] for a in range(16)], axis=0).astype(F32)
    sub16 = lax.broadcasted_iota(jnp.int32, (16, 128), 0)
    lane16 = lax.broadcasted_iota(jnp.int32, (16, 128), 1) & 15
    slanted = pltpu.roll(raw, 0, axis=1, stride=1, stride_axis=0)
    for q in range(SLOTS):
        moved = pltpu.roll(slanted, (128 - q) % 128, axis=1)
        kept = jnp.where(lane16 == sub16, moved, 0.0)
        colq[q : q + 1, :] = jnp.sum(kept, axis=0, keepdims=True).astype(jnp.int32)

    def columns(n):
        return jnp.concatenate([colq[2 * n : 2 * n + 1, :], colq[2 * n + 1 : 2 * n + 2, :]], axis=1)

    for n in range(8):
        low = columns(n) & 255
        sub = lax.broadcasted_iota(jnp.int32, (LON, 256), 0)
        colhot[n] = jnp.where(sub == low, 1.0, 0.0).astype(BF16)
    lane32 = lax.broadcasted_iota(jnp.int32, (CH, 32), 1)
    square[...] = jnp.zeros_like(square)
    for i in range(4):
        square[i * TYPES : (i + 1) * TYPES, :CH] = rows_in[...]
    opt_h, opt_l = split(square[...].T[:CH, :32])
    opt = jnp.where((lane32 & 8) == 0, opt_h, opt_l).astype(BF16)
    op1 = square[:TYPES, :]
    op_h, op_l = split(op1 + pltpu.roll(op1, CH, axis=1))
    opp = jnp.concatenate([op_h, op_l], axis=0).astype(BF16)
    ids = window_v[...] * TYPES + type_v[...]
    member = jnp.where(lax.broadcasted_iota(jnp.int32, (32, NBLK), 0) == ids, 1.0, 0.0).astype(BF16)
    def clear(r, carry):
        dirn[r] = jnp.zeros((CH, LANES), F32)
        dirn[r + LAT] = jnp.zeros((CH, LANES), F32)
        inc[r] = jnp.zeros((CH, LON), F32)
        return carry

    lax.fori_loop(0, LAT, clear, 0)
    rrv[...] = jnp.ones((1, 128), F32)
    part[...] = jnp.zeros((1, 128), F32)

    pl.semaphore_wait(barrier, NDEV - 1)
    for copy in halo_w():
        copy.start()

    def build_winds():
        for copy in halo_w():
            copy.wait()
        side = sides(hp_w, 0) + sides(hp_w, 4) + sides(hp_w, 2)
        for g in range(EXT):
            if g < 8:
                main, ok = ns_w[0, g], valid_s
            elif g < 16:
                main, ok = wown[g - 8], None
            else:
                main, ok = ns_w[1, g - 16], valid_n
            side_g = side[g]
            both = jnp.concatenate([main, side_g], axis=1)
            u = both[:LEV]
            v = both[LEV:]
            values = (
                1.0 - jnp.abs(u) - jnp.abs(v),
                jnp.maximum(u, 0.0),
                jnp.maximum(-u, 0.0),
                jnp.maximum(v, 0.0),
                jnp.maximum(-v, 0.0),
            )
            for i, value in enumerate(values):
                winds[i, g] = value if ok is None else value * ok

    def advance(dst, src, shift, lo, hi, adjoint, unroll, extra=None):
        def body(g, carry):
            for var in range(4):
                at = slice(var * LEV, (var + 1) * LEV)
                mid = src[g - shift, at, :]
                below = src[g - shift - 1, at, :]
                above = src[g - shift + 1, at, :]
                if adjoint:
                    out = (
                        winds[0, g] * mid
                        + pltpu.roll(winds[1, g] * mid, LANES - 1, axis=1)
                        + pltpu.roll(winds[2, g] * mid, 1, axis=1)
                        + winds[3, g + 1] * above
                        + winds[4, g - 1] * below
                    )
                else:
                    out = (
                        winds[0, g] * mid
                        + winds[1, g] * pltpu.roll(mid, 1, axis=1)
                        + winds[2, g] * pltpu.roll(mid, LANES - 1, axis=1)
                        + winds[3, g] * below
                        + winds[4, g] * above
                    )
                dst[g, at, :] = out if extra is None else out + extra[g, at, :]
            return carry

        lax.fori_loop(lo, hi, body, 0, unroll=unroll)

    def project(window, source):
        def body(r, carry):
            high, low = split(source(r))
            both = jnp.concatenate([high, low], axis=0).astype(BF16)
            out = mm(opp, both)
            proj[r, window * TYPES : (window + 1) * TYPES, :] = out[:8] + out[8:]
            return carry

        lax.fori_loop(0, LAT, body, 0, unroll=4)

    def message(dst, row):
        for w in range(WIN):
            dst[:, w, :] = stage[w * 128 : (w + 1) * 128, :].T
        dst[:, 3, :] = jnp.broadcast_to(row, (NDEV, 128))

    def total(recv):
        lanes = jnp.sum(recv[:, 3, :], axis=0, keepdims=True)
        return jnp.broadcast_to(jnp.sum(lanes, axis=1, keepdims=True), (1, 128))

    def full(row):
        return jnp.concatenate([row, row, row], axis=1)

    def own_squares(value):
        own = value[:, :LON]
        return jnp.sum((own * own).reshape(8, 8, LON), axis=0)

    def forward(it):
        ping, pong = field.at[0], field.at[1]
        project(0, lambda r: res[r + 4, :, :LON])
        advance(pong, res, 4, 5, 19, False, 7)
        advance(ping, pong, 0, 6, 18, False, 6)
        project(1, lambda r: ping[r + 8, :, :LON])
        advance(pong, ping, 0, 7, 17, False, 5)
        advance(ping, pong, 0, 8, 16, False, 4)
        project(2, lambda r: ping[r + 8, :, :LON])
        for r in range(LAT):
            lgather[r * 48 : (r + 1) * 48, :] = jnp.concatenate(split(proj[r]), axis=0).astype(BF16)
        for n in range(8):
            found = mm(lgather[...], colhot[n])
            band = jnp.broadcast_to(columns(n) >> 8, (WT, 256))
            got = found[:WT] + found[WT : 2 * WT]
            for r in range(1, LAT):
                at = r * 2 * WT
                got = jnp.where(band == r, found[at : at + WT] + found[at + WT : at + 2 * WT], got)
            for half in range(2):
                for w in range(WIN):
                    stage[pl.ds(w * 128 + 2 * n + half, 8, stride=16), :] = got[
                        w * 8 : (w + 1) * 8, half * 128 : (half + 1) * 128
                    ]
        message(send_f, part[...])
        a2a_start(send_f, recv_f, 0, swapped, me)
        a2a_wait(send_f, recv_f, 0)
        norm = total(recv_f)
        beta = jnp.where(it == 1, jnp.zeros_like(norm), norm / rrv[...])
        rrv[...] = norm
        for w in range(WIN):
            table = recv_f[:, w, :].T
            high, low = split(table)
            for t in range(TYPES):
                at = slice(t * 16, (t + 1) * 16)
                tsplit[w * TYPES + t] = jnp.concatenate([high[at], low[at]], axis=0).astype(BF16)

        def look(b, acc):
            which = window_s[b] * TYPES + type_s[b]
            got = mm(tsplit[which], onehot[b])
            both = (got[:16] + got[16:]) * cweight[b]
            summed = (both[:, :128] + both[:, 128:256]) + (both[:, 256:384] + both[:, 384:])
            y = jnp.sum(summed, axis=0, keepdims=True) + beta * yrow[b]
            yrow[b] = y
            z = live[b] * y
            zrow[b] = z
            return acc + z * y

        quad = lax.fori_loop(0, NBLK, look, jnp.zeros((1, ROWS), F32), unroll=8)

        def turn(r, acc):
            p = res[r + 4] + full(beta) * dirn[r + 4]
            dirn[r + 4] = p
            return acc + own_squares(p)

        pp = lax.fori_loop(0, LAT, turn, jnp.zeros((8, LON), F32), unroll=2)
        pp = jnp.sum(pp, axis=0, keepdims=True)
        part[...] = quad + pp[:, :128] + pp[:, 128:]
        betav[...] = beta

    def forcing(value):
        high, low = split(value)
        return mm(opt, jnp.concatenate([high, high, low, low], axis=0).astype(BF16))

    def adjoint(it, alpha, deep):
        copies = halo_s(deep)
        for copy in copies:
            copy.start()
        ping, pong = field.at[0], field.at[1]
        into = {2: ping, 1: force1, 0: force0}
        near = {2: 8 if deep else 4, 1: 6 if deep else 2, 0: 4 if deep else 0}

        def own(r, c):
            for w in range(WIN):
                into[w][r + 8, :, :LON] = forcing(ssum[w * LAT + r])
            return c

        def own_side(r, c):
            for w in range(WIN):
                into[w][r + 8, :, LON:] = forcing(sside[r + 8, w * TYPES : (w + 1) * TYPES, :])
            return c

        def outside(w):
            def body(i, c):
                for k, g, r in ((0, 7 - i, 7 - i), (1, 16 + i, i)):
                    into[w][g, :, :LON] = forcing(ns_s[k, w * LAT + r])
                    into[w][g, :, LON:] = forcing(sside[g, w * TYPES : (w + 1) * TYPES, :])
                return c

            if near[w]:
                lax.fori_loop(0, near[w], body, 0, unroll=2)

        lax.fori_loop(0, LAT, own, 0, unroll=2)
        for copy in copies[4:6]:
            copy.wait()
        for r, value in enumerate(sides(hp_s, 4)):
            sside[r + 8] = value
        lax.fori_loop(0, LAT, own_side, 0, unroll=4)
        advance(pong, ping, 0, 9, 15, True, 3)
        for copy in copies[:4]:
            copy.wait()
        for r, value in enumerate(sides(hp_s, 0)):
            sside[r] = value
        for r, value in enumerate(sides(hp_s, 2)):
            sside[r + 16] = value
        for copy in copies[6:]:
            copy.wait()
        for w in (2, 1, 0):
            outside(w)
        if deep:
            advance(pong, ping, 0, 1, 9, True, 4)
            advance(pong, ping, 0, 15, 23, True, 4)
            advance(ping, pong, 0, 2, 22, True, 5, force1)
            advance(pong, ping, 0, 3, 21, True, 6)
            advance(ping, pong, 0, 4, 20, True, 4, force0)
        else:
            advance(pong, ping, 0, 5, 9, True, 4)
            advance(pong, ping, 0, 15, 19, True, 4)
            advance(ping, pong, 0, 6, 18, True, 6, force1)
            advance(pong, ping, 0, 7, 17, True, 5)
            advance(ping, pong, 0, 8, 16, True, 4, force0)
        zero = jnp.zeros((8, LON), F32)

        def done(acc):
            acc = jnp.sum(acc, axis=0, keepdims=True)
            part[...] = acc[:, :128] + acc[:, 128:]

        scale = full(alpha)
        if deep:

            @pl.when(it == 0)
            def _():
                def rim(i, c):
                    e = i + LAT * (i // 4)
                    ok = jnp.where(i < 4, valid_s, valid_n)
                    res[e] = ping[e + 4] * ok
                    return c

                def body(r, acc):
                    value = ping[r + 8]
                    res[r + 4] = value
                    return acc + own_squares(value)

                lax.fori_loop(0, 8, rim, 0)
                done(lax.fori_loop(0, LAT, body, zero, unroll=2))

            @pl.when(it > 0)
            def _():
                def rim(i, c):
                    e = i + LAT * (i // 4)
                    ok = jnp.where(i < 4, valid_s, valid_n)
                    res[e] -= scale * (dirn[e] + ping[e + 4]) * ok
                    return c

                def body(r, acc):
                    p = dirn[r + 4]
                    inc[r] += scale[:, :LON] * p[:, :LON]
                    value = res[r + 4] - scale * (p + ping[r + 8])
                    res[r + 4] = value
                    return acc + own_squares(value)

                lax.fori_loop(0, 8, rim, 0)
                done(lax.fori_loop(0, LAT, body, zero, unroll=2))
        else:
            narrow = scale[:, :LON]

            def body(r, c):
                p = dirn[r + 4, :, :LON]
                x_out[r] = inc[r] + narrow * p
                r_out[r] = res[r + 4, :, :LON] - narrow * (p + ping[r + 8, :, :LON])
                return c

            lax.fori_loop(0, LAT, body, 0, unroll=2)

    def outer(it, carry):
        @pl.when(it > 0)
        def _():
            forward(it)

        def spread(b, c):
            z = zrow[b]
            value = cweight[b] * jnp.concatenate([z, z, z, z], axis=1)
            high, low = split(value)
            both = jnp.concatenate([high, low], axis=0).astype(BF16)
            out = mm_nt(both, onehot[b])
            rblk[b] = out[:16] + out[16:]
            return c

        lax.fori_loop(0, NBLK, spread, 0, unroll=8)
        for q in range(SLOTS):
            high, low = split(rblk[:, q, :])
            out = mm(member, high.astype(BF16)) + mm(member, low.astype(BF16))
            for w in range(WIN):
                stage[pl.ds(w * 128 + q, 8, stride=16), :] = out[w * 8 : (w + 1) * 8]
        message(send_b, part[...])
        a2a_start(send_b, recv_b, 1, plain, swapped(lat, lon))

        @pl.when(it == 0)
        def _():
            build_winds()

        @pl.when(it == 1)
        def _():
            def beyond(i, c):
                e = i + LAT * (i // 4)
                dirn[e] = res[e] + full(betav[...]) * dirn[e]
                return c

            lax.fori_loop(0, 8, beyond, 0)

        a2a_wait(send_b, recv_b, 1)
        for w in range(WIN):
            stage[w * 128 : (w + 1) * 128, :] = recv_b[:, w, :].T
        alpha = rrv[...] / total(recv_b)
        for n in range(8):
            halves = []
            for half in range(2):
                halves.append(
                    jnp.concatenate(
                        [stage[pl.ds(w * 128 + 2 * n + half, 8, stride=16), :] for w in range(WIN)],
                        axis=0,
                    )
                )
            high, low = split(jnp.concatenate(halves, axis=1))
            band = jnp.broadcast_to(columns(n) >> 8, (WT, 256))
            for r in range(LAT):
                here = band == r
                lscatter[r * 48 : (r + 1) * 48, :] = jnp.concatenate(
                    [jnp.where(here, high, 0.0), jnp.where(here, low, 0.0)], axis=0
                ).astype(BF16)
            out = mm_nt(lscatter[...], colhot[n])
            if n == 0:
                sacc[...] = out
            else:
                sacc[...] += out
        for r in range(LAT):
            value = sacc[r * 48 : r * 48 + WT, :] + sacc[r * 48 + WT : (r + 1) * 48, :]
            for w in range(WIN):
                ssum[w * LAT + r] = value[w * TYPES : (w + 1) * TYPES]
        pack_s[...] = pack_rows(
            [jnp.concatenate([ssum[w * LAT + r] for w in range(WIN)], axis=0) for r in range(LAT)]
        )
        @pl.when(it < 2)
        def _():
            adjoint(it, alpha, True)

        @pl.when(it == 2)
        def _():
            adjoint(it, alpha, False)

        return carry

    lax.fori_loop(0, 3, outer, 0)


def shards(
    zonal_wind, merid_wind, operator_rows, innovation, error_weight, interp_weight, obs_slot,
    block_count, block_type, block_window, send_cols,
):
    vm = pl.BlockSpec(memory_space=pltpu.VMEM)
    sm = pl.BlockSpec(memory_space=pltpu.SMEM)
    V = pltpu.VMEM
    dma = pltpu.SemaphoreType.DMA
    x, r = pl.pallas_call(
        kernel,
        out_shape=[jax.ShapeDtypeStruct((LAT, CH, LON), F32)] * 2,
        in_specs=[vm] * 10 + [sm] * 3,
        out_specs=[vm] * 2,
        scratch_shapes=[
            V((5, EXT, LEV, LANES), F32),
            V((2, EXT, CH, LANES), F32),
            V((MID, CH, LANES), F32),
            V((MID, CH, LANES), F32),
            V((LAT, CH, LON), F32),
            V((EXT, CH, LANES), F32),
            V((EXT, CH, LANES), F32),
            V((128, 128), F32),
            V((SLOTS, 128), jnp.int32),
            V((NBLK, NDEV, KPTS * ROWS), BF16),
            V((NBLK, SLOTS, KPTS * ROWS), F32),
            V((NBLK, 1, ROWS), F32),
            V((NBLK, 1, ROWS), F32),
            V((NBLK, 1, ROWS), F32),
            V((NBLK, SLOTS, NDEV), F32),
            V((WT, 32, NDEV), BF16),
            V((8, LON, 256), BF16),
            V((LAT, WT, LON), F32),
            V((WIN * LAT, TYPES, LON), F32),
            V((EXT, WT, 128), F32),
            V((WIN * 128, 128), F32),
            V((16 * WT, 256), BF16),
            V((16 * WT, 256), BF16),
            V((16 * WT, 256), F32),
            V((NDEV, 4, 128), F32),
            V((NDEV, 4, 128), F32),
            V((NDEV, 4, 128), F32),
            V((NDEV, 4, 128), F32),
            V((LAT, 2 * LEV, LON), F32),
            V((2 * LEV, 128), F32),
            V((WT, 128), F32),
            V((2, LAT, 2 * LEV, LON), F32),
            V((2, WIN * LAT, TYPES, LON), F32),
            V((6, 2 * LEV, 128), F32),
            V((6, WT, 128), F32),
            V((1, 128), F32),
            V((1, 128), F32),
            V((1, 128), F32),
            dma((2,)),
            dma((2,)),
            dma((8,)),
            dma((8,)),
            dma((12,)),
            dma((12,)),
        ],
        compiler_params=pltpu.CompilerParams(
            collective_id=0, has_side_effects=True, vmem_limit_bytes=60 << 20
        ),
        name="cg",
    )(
        zonal_wind, merid_wind, operator_rows,
        innovation.reshape(NBLK, 1, ROWS), error_weight.reshape(NBLK, 1, ROWS),
        interp_weight, obs_slot, send_cols, block_type.reshape(1, NBLK), block_window.reshape(1, NBLK),
        block_count, block_type, block_window,
    )
    shape = (4, LEV, LAT, LON)
    return x.transpose(1, 0, 2).reshape(shape), r.transpose(1, 0, 2).reshape(shape)


def solution(mesh):
    both = ("lat", "lon")
    in_specs = (
        P(None, "lat", "lon"),
        P(None, "lat", "lon"),
        P(),
        P(both),
        P(both),
        P(None, both),
        P(None, both),
        P(both),
        P(both),
        P(both),
        P(both, None),
    )
    out_specs = (P(None, None, "lat", "lon"), P(None, None, "lat", "lon"))
    return jax.shard_map(shards, mesh=mesh, in_specs=in_specs, out_specs=out_specs, check_vma=False)
```

```python
import functools

import jax
import jax.numpy as jnp
from jax import lax
from jax.experimental import pallas as pl
from jax.experimental.pallas import tpu as pltpu
from jax.sharding import PartitionSpec as P

MESH = pl.DeviceIdType.MESH
F32 = jnp.float32
BF16 = jnp.bfloat16

TYPES = 8
WIN = 3
WT = WIN * TYPES
KPTS = 4
SLOTS = 16
ROWS = 128
N_LAT = 8
N_LON = 16
NDEV = N_LAT * N_LON
NBLK = 32
LEV = 16
CH = 64
LAT = 8
LON = 256
EXT = 24
MID = 16
LANES = 384
NT = (((1,), (1,)), ((), ()))


def split(value):
    high = value.astype(BF16).astype(F32)
    return high, value - high


def mm(left, right):
    return jnp.dot(left, right, preferred_element_type=F32)


def mm_nt(left, right):
    return lax.dot_general(left, right, NT, preferred_element_type=F32)


def pack_rows(rows):
    packed = None
    for r, row in enumerate(rows):
        lane = lax.broadcasted_iota(jnp.int32, (row.shape[0], 128), 1)
        ends = jnp.where(lane < 64, row[:, :128], row[:, 128:])
        moved = pltpu.roll(ends, (8 + 16 * r) % 128, axis=1)
        packed = moved if packed is None else jnp.where((lane >> 4) == r, moved, packed)
    return packed


def offsets():
    steps = [
        (dx, dc, dy, dz)
        for dx in range(4) for dc in range(2) for dy in range(4) for dz in range(4)
    ][1:]
    return sorted(steps, key=lambda t: -sum(min(d, 4 - d) for d in (t[0], t[2], t[3])))


def kernel(
    zonal_h, merid_h, interp_h, slots_h, rows_in, innov, weight, cols, type_v, window_v,
    count_s, type_s, window_s,
    x_out, r_out,
    zonal, merid, interp, slots, in_sem, winds, field, res, dirn, inc, force0, force1, square, colq,
    onehot, cweight, live, zrow, yrow, rblk, tsplit,
    colhot, proj, ssum, sside, stage, lgather, lscatter, sacc,
    send_f, send_b, recv_f, recv_b, wown,
    pack_w, pack_s, ns_w, ns_s, hp_w, hp_s, rrv, part, betav,
    a2a_send, a2a_recv, hw_send, hw_recv, hs_send, hs_recv,
):
    loads = [
        pltpu.make_async_copy(src, dst, in_sem.at[i])
        for i, (src, dst) in enumerate(
            ((zonal_h, zonal), (merid_h, merid), (interp_h, interp), (slots_h, slots))
        )
    ]
    for load in loads:
        load.start()
    lat = lax.axis_index("lat")
    lon = lax.axis_index("lon")
    me = lat * N_LON + lon
    barrier = pltpu.get_barrier_semaphore()

    x, core = lat // 2, lax.rem(lat, 2)
    y, z = lon // 4, lax.rem(lon, 4)
    lats = {
        (dx, dc): lax.rem(x + dx, 4) * 2 + lax.rem(core + dc, 2)
        for dx in range(4) for dc in range(2)
    }
    lons = {
        (dy, dz): lax.rem(y + dy, 4) * 4 + lax.rem(z + dz, 4)
        for dy in range(4) for dz in range(4)
    }

    def everyone(act):
        for dx, dc, dy, dz in offsets():
            act(lats[dx, dc], lons[dy, dz])

    def plain(a, o):
        return a * N_LON + o

    def swapped(a, o):
        return lax.rem(o, 8) * 16 + a * 2 + o // 8

    def greet(a, o):
        pl.semaphore_signal(
            barrier, inc=1, device_id={"lat": a, "lon": o}, device_id_type=MESH
        )

    everyone(greet)

    north = lax.rem(lat + 1, N_LAT)
    south = lax.rem(lat + N_LAT - 1, N_LAT)
    east = lax.rem(lon + 1, N_LON)
    west = lax.rem(lon + N_LON - 1, N_LON)
    valid_s = jnp.where(lat > 0, 1.0, 0.0).astype(F32)
    valid_n = jnp.where(lat < N_LAT - 1, 1.0, 0.0).astype(F32)

    def to(src, dst, a, o, send, recv):
        return pltpu.make_async_remote_copy(
            src, dst, send, recv, device_id={"lat": a, "lon": o}, device_id_type=MESH
        )

    def edges(pack, hp, send, recv):
        targets = [
            (north, east), (north, west), (south, east), (south, west), (lat, east), (lat, west)
        ]
        return [
            to(pack, hp.at[i], a, o, send.at[i], recv.at[i]) for i, (a, o) in enumerate(targets)
        ]

    def halo_w():
        return edges(pack_w, hp_w, hw_send, hw_recv) + [
            to(wown, ns_w.at[0], north, lon, hw_send.at[6], hw_recv.at[6]),
            to(wown, ns_w.at[1], south, lon, hw_send.at[7], hw_recv.at[7]),
        ]

    def halo_s(deep):
        copies = edges(pack_s, hp_s, hs_send, hs_recv)
        k = 6
        for w, count in ((2, 8 if deep else 4), (1, 6 if deep else 2), (0, 4 if deep else 0)):
            if count == 0:
                continue
            high = pl.ds(w * LAT + LAT - count, count)
            low = pl.ds(w * LAT, count)
            copies.append(to(ssum.at[high], ns_s.at[0, high], north, lon, hs_send.at[k], hs_recv.at[k]))
            copies.append(
                to(ssum.at[low], ns_s.at[1, low], south, lon, hs_send.at[k + 1], hs_recv.at[k + 1])
            )
            k += 2
        return copies

    def sides(hp, base):
        lane = lax.broadcasted_iota(jnp.int32, hp.shape[1:], 1)
        both = jnp.where((lane & 15) < 8, hp[base], hp[base + 1])
        return [pltpu.roll(both, (256 - 16 * r - 8) % 128, axis=1) for r in range(LAT)]

    def a2a_start(src, dst, k, row_of, mine):
        def go(a, o):
            to(
                src.at[row_of(a, o)], dst.at[mine], a, o, a2a_send.at[k], a2a_recv.at[k]
            ).start()

        everyone(go)
        dst[mine] = src[row_of(lat, lon)]

    def a2a_wait(src, dst, k):
        got = dst.at[pl.ds(0, NDEV - 1)]
        pltpu.make_async_copy(got, got, a2a_recv.at[k]).wait()
        gone = src.at[pl.ds(0, NDEV - 1)]
        pltpu.make_async_copy(gone, gone, a2a_send.at[k]).wait()

    for load in loads:
        load.wait()
    for r in range(LAT):
        wown[r, :LEV, :] = zonal[:, r, :]
        wown[r, LEV:, :] = merid[:, r, :]
    pack_w[...] = pack_rows([wown[r] for r in range(LAT)])

    def tables(b, carry):
        at = pl.ds(pl.multiple_of(b * ROWS, ROWS), ROWS)
        slot = slots[:, at]
        wgt = interp[:, at]
        sender = slot >> 4
        inner = slot & 15
        sub = lax.broadcasted_iota(jnp.int32, (NDEV, ROWS), 0)
        sub16 = lax.broadcasted_iota(jnp.int32, (SLOTS, ROWS), 0)
        for k in range(KPTS):
            lanes = slice(k * ROWS, (k + 1) * ROWS)
            onehot[b, :, lanes] = jnp.where(sub == sender[k : k + 1], 1.0, 0.0).astype(BF16)
            cweight[b, :, lanes] = jnp.where(sub16 == inner[k : k + 1], wgt[k : k + 1], 0.0)
        lane = lax.broadcasted_iota(jnp.int32, (1, ROWS), 1)
        wl = jnp.where(lane < count_s[b], weight[b], 0.0)
        live[b] = wl
        zrow[b] = wl * innov[b]
        yrow[b] = jnp.zeros((1, ROWS), F32)
        return carry

    lax.fori_loop(0, NBLK, tables, 0, unroll=2)
    raw = jnp.concatenate([cols[:, a * 128 : (a + 1) * 128] for a in range(16)], axis=0).astype(F32)
    sub16 = lax.broadcasted_iota(jnp.int32, (16, 128), 0)
    lane16 = lax.broadcasted_iota(jnp.int32, (16, 128), 1) & 15
    slanted = pltpu.roll(raw, 0, axis=1, stride=1, stride_axis=0)
    for q in range(SLOTS):
        moved = pltpu.roll(slanted, (128 - q) % 128, axis=1)
        kept = jnp.where(lane16 == sub16, moved, 0.0)
        colq[q : q + 1, :] = jnp.sum(kept, axis=0, keepdims=True).astype(jnp.int32)

    def columns(n):
        return jnp.concatenate([colq[2 * n : 2 * n + 1, :], colq[2 * n + 1 : 2 * n + 2, :]], axis=1)

    for n in range(8):
        low = columns(n) & 255
        sub = lax.broadcasted_iota(jnp.int32, (LON, 256), 0)
        colhot[n] = jnp.where(sub == low, 1.0, 0.0).astype(BF16)
    lane32 = lax.broadcasted_iota(jnp.int32, (CH, 32), 1)
    square[...] = jnp.zeros_like(square)
    for i in range(4):
        square[i * TYPES : (i + 1) * TYPES, :CH] = rows_in[...]
    opt_h, opt_l = split(square[...].T[:CH, :32])
    opt = jnp.where((lane32 & 8) == 0, opt_h, opt_l).astype(BF16)
    op1 = square[:TYPES, :]
    op_h, op_l = split(op1 + pltpu.roll(op1, CH, axis=1))
    opp = jnp.concatenate([op_h, op_l], axis=0).astype(BF16)
    ids = window_v[...] * TYPES + type_v[...]
    member = jnp.where(lax.broadcasted_iota(jnp.int32, (32, NBLK), 0) == ids, 1.0, 0.0).astype(BF16)
    def clear(r, carry):
        dirn[r] = jnp.zeros((CH, LANES), F32)
        dirn[r + LAT] = jnp.zeros((CH, LANES), F32)
        inc[r] = jnp.zeros((CH, LON), F32)
        return carry

    lax.fori_loop(0, LAT, clear, 0)
    rrv[...] = jnp.ones((1, 128), F32)
    part[...] = jnp.zeros((1, 128), F32)

    pl.semaphore_wait(barrier, NDEV - 1)
    for copy in halo_w():
        copy.start()

    def build_winds():
        for copy in halo_w():
            copy.wait()
        side = sides(hp_w, 0) + sides(hp_w, 4) + sides(hp_w, 2)
        for g in range(EXT):
            if g < 8:
                main, ok = ns_w[0, g], valid_s
            elif g < 16:
                main, ok = wown[g - 8], None
            else:
                main, ok = ns_w[1, g - 16], valid_n
            side_g = side[g]
            both = jnp.concatenate([main, side_g], axis=1)
            u = both[:LEV]
            v = both[LEV:]
            values = (
                1.0 - jnp.abs(u) - jnp.abs(v),
                jnp.maximum(u, 0.0),
                jnp.maximum(-u, 0.0),
                jnp.maximum(v, 0.0),
                jnp.maximum(-v, 0.0),
            )
            for i, value in enumerate(values):
                winds[i, g] = value if ok is None else value * ok

    def advance(dst, src, shift, lo, hi, adjoint, unroll, extra=None):
        def body(g, carry):
            for var in range(4):
                at = slice(var * LEV, (var + 1) * LEV)
                mid = src[g - shift, at, :]
                below = src[g - shift - 1, at, :]
                above = src[g - shift + 1, at, :]
                if adjoint:
                    out = (
                        winds[0, g] * mid
                        + pltpu.roll(winds[1, g] * mid, LANES - 1, axis=1)
                        + pltpu.roll(winds[2, g] * mid, 1, axis=1)
                        + winds[3, g + 1] * above
                        + winds[4, g - 1] * below
                    )
                else:
                    out = (
                        winds[0, g] * mid
                        + winds[1, g] * pltpu.roll(mid, 1, axis=1)
                        + winds[2, g] * pltpu.roll(mid, LANES - 1, axis=1)
                        + winds[3, g] * below
                        + winds[4, g] * above
                    )
                dst[g, at, :] = out if extra is None else out + extra[g, at, :]
            return carry

        lax.fori_loop(lo, hi, body, 0, unroll=unroll)

    def project(window, source):
        def body(r, carry):
            high, low = split(source(r))
            both = jnp.concatenate([high, low], axis=0).astype(BF16)
            out = mm(opp, both)
            proj[r, window * TYPES : (window + 1) * TYPES, :] = out[:8] + out[8:]
            return carry

        lax.fori_loop(0, LAT, body, 0, unroll=8)

    def message(dst, row):
        for w in range(WIN):
            dst[:, w, :] = stage[w * 128 : (w + 1) * 128, :].T
        dst[:, 3, :] = jnp.broadcast_to(row, (NDEV, 128))

    def total(recv):
        lanes = jnp.sum(recv[:, 3, :], axis=0, keepdims=True)
        return jnp.broadcast_to(jnp.sum(lanes, axis=1, keepdims=True), (1, 128))

    def full(row):
        return jnp.concatenate([row, row, row], axis=1)

    def own_squares(value):
        own = value[:, :LON]
        return jnp.sum((own * own).reshape(8, 8, LON), axis=0)

    def forward(it):
        ping, pong = field.at[0], field.at[1]
        project(0, lambda r: res[r + 4, :, :LON])
        advance(pong, res, 4, 5, 19, False, 14)
        advance(ping, pong, 0, 6, 18, False, 12)
        project(1, lambda r: ping[r + 8, :, :LON])
        advance(pong, ping, 0, 7, 17, False, 10)
        advance(ping, pong, 0, 8, 16, False, 8)
        project(2, lambda r: ping[r + 8, :, :LON])
        for r in range(LAT):
            lgather[r * 48 : (r + 1) * 48, :] = jnp.concatenate(split(proj[r]), axis=0).astype(BF16)
        for n in range(8):
            found = mm(lgather[...], colhot[n])
            band = jnp.broadcast_to(columns(n) >> 8, (WT, 256))
            got = found[:WT] + found[WT : 2 * WT]
            for r in range(1, LAT):
                at = r * 2 * WT
                got = jnp.where(band == r, found[at : at + WT] + found[at + WT : at + 2 * WT], got)
            for half in range(2):
                for w in range(WIN):
                    stage[pl.ds(w * 128 + 2 * n + half, 8, stride=16), :] = got[
                        w * 8 : (w + 1) * 8, half * 128 : (half + 1) * 128
                    ]
        message(send_f, part[...])
        a2a_start(send_f, recv_f, 0, swapped, me)
        a2a_wait(send_f, recv_f, 0)
        norm = total(recv_f)
        beta = jnp.where(it == 1, jnp.zeros_like(norm), norm / rrv[...])
        rrv[...] = norm
        for w in range(WIN):
            table = recv_f[:, w, :].T
            high, low = split(table)
            for t in range(TYPES):
                at = slice(t * 16, (t + 1) * 16)
                tsplit[w * TYPES + t] = jnp.concatenate([high[at], low[at]], axis=0).astype(BF16)

        def look(b, acc):
            which = window_s[b] * TYPES + type_s[b]
            got = mm(tsplit[which], onehot[b])
            both = (got[:16] + got[16:]) * cweight[b]
            summed = (both[:, :128] + both[:, 128:256]) + (both[:, 256:384] + both[:, 384:])
            y = jnp.sum(summed, axis=0, keepdims=True) + beta * yrow[b]
            yrow[b] = y
            z = live[b] * y
            zrow[b] = z
            return acc + z * y

        quad = lax.fori_loop(0, NBLK, look, jnp.zeros((1, ROWS), F32), unroll=8)

        def turn(r, acc):
            p = res[r + 4] + full(beta) * dirn[r + 4]
            dirn[r + 4] = p
            return acc + own_squares(p)

        pp = lax.fori_loop(0, LAT, turn, jnp.zeros((8, LON), F32), unroll=2)
        pp = jnp.sum(pp, axis=0, keepdims=True)
        part[...] = quad + pp[:, :128] + pp[:, 128:]
        betav[...] = beta

    def forcing(value):
        high, low = split(value)
        return mm(opt, jnp.concatenate([high, high, low, low], axis=0).astype(BF16))

    def adjoint(it, alpha, deep):
        copies = halo_s(deep)
        for copy in copies:
            copy.start()
        ping, pong = field.at[0], field.at[1]
        into = {2: ping, 1: force1, 0: force0}
        near = {2: 8 if deep else 4, 1: 6 if deep else 2, 0: 4 if deep else 0}

        def own(r, c):
            for w in range(WIN):
                into[w][r + 8, :, :LON] = forcing(ssum[w * LAT + r])
            return c

        def own_side(r, c):
            for w in range(WIN):
                into[w][r + 8, :, LON:] = forcing(sside[r + 8, w * TYPES : (w + 1) * TYPES, :])
            return c

        def outside(w):
            count = near[w]
            if count == 0:
                return

            def body(i, c):
                for k, g, r in ((0, i + 8 - count, i + 8 - count), (1, 16 + i, i)):
                    into[w][g, :, :LON] = forcing(ns_s[k, w * LAT + r])
                    into[w][g, :, LON:] = forcing(sside[g, w * TYPES : (w + 1) * TYPES, :])
                return c

            lax.fori_loop(0, count, body, 0, unroll=4 if count % 4 == 0 else count // 2)

        def landed(w):
            if near[w]:
                at = 6 + 2 * (2 - w)
                for copy in copies[at : at + 2]:
                    copy.wait()

        lax.fori_loop(0, LAT, own, 0, unroll=4)
        for copy in copies[4:6]:
            copy.wait()
        for r, value in enumerate(sides(hp_s, 4)):
            sside[r + 8] = value
        lax.fori_loop(0, LAT, own_side, 0, unroll=8)
        advance(pong, ping, 0, 9, 15, True, 6)
        for copy in copies[:4]:
            copy.wait()
        for r, value in enumerate(sides(hp_s, 0)):
            sside[r] = value
        for r, value in enumerate(sides(hp_s, 2)):
            sside[r + 16] = value
        landed(2)
        outside(2)
        lo, hi = (1, 23) if deep else (5, 19)
        advance(pong, ping, 0, lo, 9, True, 9 - lo)
        advance(pong, ping, 0, 15, hi, True, hi - 15)
        landed(1)
        outside(1)
        lo, hi = lo + 1, hi - 1
        advance(ping, pong, 0, lo, hi, True, (hi - lo) // 2 if deep else hi - lo, force1)
        lo, hi = lo + 1, hi - 1
        advance(pong, ping, 0, lo, hi, True, (hi - lo) // 2 if deep else hi - lo)
        landed(0)
        outside(0)
        lo, hi = lo + 1, hi - 1
        advance(ping, pong, 0, lo, hi, True, 8, force0)
        zero = jnp.zeros((8, LON), F32)

        def done(acc):
            acc = jnp.sum(acc, axis=0, keepdims=True)
            part[...] = acc[:, :128] + acc[:, 128:]

        scale = full(alpha)
        if deep:

            @pl.when(it == 0)
            def _():
                def rim(i, c):
                    e = i + LAT * (i // 4)
                    ok = jnp.where(i < 4, valid_s, valid_n)
                    res[e] = ping[e + 4] * ok
                    return c

                def body(r, acc):
                    value = ping[r + 8]
                    res[r + 4] = value
                    return acc + own_squares(value)

                lax.fori_loop(0, 8, rim, 0)
                done(lax.fori_loop(0, LAT, body, zero, unroll=2))

            @pl.when(it > 0)
            def _():
                def rim(i, c):
                    e = i + LAT * (i // 4)
                    ok = jnp.where(i < 4, valid_s, valid_n)
                    res[e] -= scale * (dirn[e] + ping[e + 4]) * ok
                    return c

                def body(r, acc):
                    p = dirn[r + 4]
                    inc[r] += scale[:, :LON] * p[:, :LON]
                    value = res[r + 4] - scale * (p + ping[r + 8])
                    res[r + 4] = value
                    return acc + own_squares(value)

                lax.fori_loop(0, 8, rim, 0)
                done(lax.fori_loop(0, LAT, body, zero, unroll=2))
        else:
            narrow = scale[:, :LON]

            def body(r, c):
                p = dirn[r + 4, :, :LON]
                x_out[r] = inc[r] + narrow * p
                r_out[r] = res[r + 4, :, :LON] - narrow * (p + ping[r + 8, :, :LON])
                return c

            lax.fori_loop(0, LAT, body, 0, unroll=2)

    def outer(it, carry):
        @pl.when(it > 0)
        def _():
            forward(it)

        def spread(b, c):
            z = zrow[b]
            value = cweight[b] * jnp.concatenate([z, z, z, z], axis=1)
            high, low = split(value)
            both = jnp.concatenate([high, low], axis=0).astype(BF16)
            out = mm_nt(both, onehot[b])
            rblk[b] = out[:16] + out[16:]
            return c

        lax.fori_loop(0, NBLK, spread, 0, unroll=8)
        for q in range(SLOTS):
            high, low = split(rblk[:, q, :])
            out = mm(member, high.astype(BF16)) + mm(member, low.astype(BF16))
            for w in range(WIN):
                stage[pl.ds(w * 128 + q, 8, stride=16), :] = out[w * 8 : (w + 1) * 8]
        message(send_b, part[...])
        a2a_start(send_b, recv_b, 1, plain, swapped(lat, lon))

        @pl.when(it == 0)
        def _():
            build_winds()

        @pl.when(it == 1)
        def _():
            def beyond(i, c):
                e = i + LAT * (i // 4)
                dirn[e] = res[e] + full(betav[...]) * dirn[e]
                return c

            lax.fori_loop(0, 8, beyond, 0)

        a2a_wait(send_b, recv_b, 1)
        for w in range(WIN):
            stage[w * 128 : (w + 1) * 128, :] = recv_b[:, w, :].T
        alpha = rrv[...] / total(recv_b)
        for n in range(8):
            halves = []
            for half in range(2):
                halves.append(
                    jnp.concatenate(
                        [stage[pl.ds(w * 128 + 2 * n + half, 8, stride=16), :] for w in range(WIN)],
                        axis=0,
                    )
                )
            high, low = split(jnp.concatenate(halves, axis=1))
            band = jnp.broadcast_to(columns(n) >> 8, (WT, 256))
            for r in range(LAT):
                here = band == r
                lscatter[r * 48 : (r + 1) * 48, :] = jnp.concatenate(
                    [jnp.where(here, high, 0.0), jnp.where(here, low, 0.0)], axis=0
                ).astype(BF16)
            out = mm_nt(lscatter[...], colhot[n])
            if n == 0:
                sacc[...] = out
            else:
                sacc[...] += out
        for r in range(LAT):
            value = sacc[r * 48 : r * 48 + WT, :] + sacc[r * 48 + WT : (r + 1) * 48, :]
            for w in range(WIN):
                ssum[w * LAT + r] = value[w * TYPES : (w + 1) * TYPES]
        pack_s[...] = pack_rows(
            [jnp.concatenate([ssum[w * LAT + r] for w in range(WIN)], axis=0) for r in range(LAT)]
        )
        @pl.when(it < 2)
        def _():
            adjoint(it, alpha, True)

        @pl.when(it == 2)
        def _():
            adjoint(it, alpha, False)

        return carry

    lax.fori_loop(0, 3, outer, 0)


def flip(x_in, r_in, x_out, r_out):
    for r in range(LAT):
        x_out[:, r, :] = x_in[r]
        r_out[:, r, :] = r_in[r]


def shards(
    zonal_wind, merid_wind, operator_rows, innovation, error_weight, interp_weight, obs_slot,
    block_count, block_type, block_window, send_cols,
):
    vm = pl.BlockSpec(memory_space=pltpu.VMEM)
    sm = pl.BlockSpec(memory_space=pltpu.SMEM)
    V = pltpu.VMEM
    dma = pltpu.SemaphoreType.DMA
    x, r = pl.pallas_call(
        kernel,
        out_shape=[jax.ShapeDtypeStruct((LAT, CH, LON), F32)] * 2,
        in_specs=[pl.BlockSpec(memory_space=pl.ANY)] * 4 + [vm] * 6 + [sm] * 3,
        out_specs=[vm] * 2,
        scratch_shapes=[
            V((LEV, LAT, LON), F32),
            V((LEV, LAT, LON), F32),
            V((KPTS, NBLK * ROWS), F32),
            V((KPTS, NBLK * ROWS), jnp.int32),
            dma((4,)),
            V((5, EXT, LEV, LANES), F32),
            V((2, EXT, CH, LANES), F32),
            V((MID, CH, LANES), F32),
            V((MID, CH, LANES), F32),
            V((LAT, CH, LON), F32),
            V((EXT, CH, LANES), F32),
            V((EXT, CH, LANES), F32),
            V((128, 128), F32),
            V((SLOTS, 128), jnp.int32),
            V((NBLK, NDEV, KPTS * ROWS), BF16),
            V((NBLK, SLOTS, KPTS * ROWS), F32),
            V((NBLK, 1, ROWS), F32),
            V((NBLK, 1, ROWS), F32),
            V((NBLK, 1, ROWS), F32),
            V((NBLK, SLOTS, NDEV), F32),
            V((WT, 32, NDEV), BF16),
            V((8, LON, 256), BF16),
            V((LAT, WT, LON), F32),
            V((WIN * LAT, TYPES, LON), F32),
            V((EXT, WT, 128), F32),
            V((WIN * 128, 128), F32),
            V((16 * WT, 256), BF16),
            V((16 * WT, 256), BF16),
            V((16 * WT, 256), F32),
            V((NDEV, 4, 128), F32),
            V((NDEV, 4, 128), F32),
            V((NDEV, 4, 128), F32),
            V((NDEV, 4, 128), F32),
            V((LAT, 2 * LEV, LON), F32),
            V((2 * LEV, 128), F32),
            V((WT, 128), F32),
            V((2, LAT, 2 * LEV, LON), F32),
            V((2, WIN * LAT, TYPES, LON), F32),
            V((6, 2 * LEV, 128), F32),
            V((6, WT, 128), F32),
            V((1, 128), F32),
            V((1, 128), F32),
            V((1, 128), F32),
            dma((2,)),
            dma((2,)),
            dma((8,)),
            dma((8,)),
            dma((12,)),
            dma((12,)),
        ],
        compiler_params=pltpu.CompilerParams(
            collective_id=0, has_side_effects=True, vmem_limit_bytes=60 << 20
        ),
        name="cg",
    )(
        zonal_wind, merid_wind, interp_weight, obs_slot, operator_rows,
        innovation.reshape(NBLK, 1, ROWS), error_weight.reshape(NBLK, 1, ROWS),
        send_cols, block_type.reshape(1, NBLK), block_window.reshape(1, NBLK),
        block_count, block_type, block_window,
    )
    shape = (4, LEV, LAT, LON)
    x, r = pl.pallas_call(
        flip,
        out_shape=[jax.ShapeDtypeStruct((CH, LAT, LON), F32)] * 2,
        in_specs=[vm] * 2,
        out_specs=[vm] * 2,
        name="flip",
    )(x, r)
    return x.reshape(shape), r.reshape(shape)


def solution(mesh):
    both = ("lat", "lon")
    in_specs = (
        P(None, "lat", "lon"),
        P(None, "lat", "lon"),
        P(),
        P(both),
        P(both),
        P(None, both),
        P(None, both),
        P(both),
        P(both),
        P(both),
        P(both, None),
    )
    out_specs = (P(None, None, "lat", "lon"), P(None, None, "lat", "lon"))
    return jax.shard_map(shards, mesh=mesh, in_specs=in_specs, out_specs=out_specs, check_vma=False)
```

```python
import functools

import jax
import jax.numpy as jnp
from jax import lax
from jax.experimental import pallas as pl
from jax.experimental.pallas import tpu as pltpu
from jax.sharding import PartitionSpec as P

MESH = pl.DeviceIdType.MESH
F32 = jnp.float32
BF16 = jnp.bfloat16

TYPES = 8
WIN = 3
WT = WIN * TYPES
KPTS = 4
SLOTS = 16
ROWS = 128
N_LAT = 8
N_LON = 16
NDEV = N_LAT * N_LON
NBLK = 32
LEV = 16
CH = 64
LAT = 8
LON = 256
EXT = 24
MID = 16
LANES = 384
NT = (((1,), (1,)), ((), ()))


def split(value):
    high = value.astype(BF16).astype(F32)
    return high, value - high


def exact(value):
    high = value.astype(BF16)
    rest = value - high.astype(F32)
    middle = rest.astype(BF16)
    return high, middle, (rest - middle.astype(F32)).astype(BF16)


def mm(left, right):
    return jnp.dot(left, right, preferred_element_type=F32)


def mm_nt(left, right):
    return lax.dot_general(left, right, NT, preferred_element_type=F32)


def pack_rows(rows):
    packed = None
    for r, row in enumerate(rows):
        lane = lax.broadcasted_iota(jnp.int32, (row.shape[0], 128), 1)
        ends = jnp.where(lane < 64, row[:, :128], row[:, 128:])
        moved = pltpu.roll(ends, (8 + 16 * r) % 128, axis=1)
        packed = moved if packed is None else jnp.where((lane >> 4) == r, moved, packed)
    return packed


def pack_typed(rows):
    packed = None
    for r, row in enumerate(rows):
        lane = lax.broadcasted_iota(jnp.int32, (row.shape[0], 128), 1)
        even = pltpu.roll(row[:, :128], (4 + 16 * r) % 128, axis=1)
        odd = pltpu.roll(row[:, 128:], (12 + 16 * r) % 128, axis=1)
        moved = jnp.where((lane & 15) < 8, even, odd)
        packed = moved if packed is None else jnp.where((lane >> 4) == r, moved, packed)
    return packed


def tiles(value):
    return value[:, :128], value[:, 128:256], value[:, 256:]


def west_of(parts):
    even, odd, rim = parts
    first = lax.broadcasted_iota(jnp.int32, even.shape, 1) == 0
    odd = pltpu.roll(odd, 1, axis=1)
    rim = pltpu.roll(rim, 1, axis=1)
    return jnp.where(first, rim, odd), even, jnp.where(first, odd, rim)


def east_of(parts):
    even, odd, rim = parts
    last = lax.broadcasted_iota(jnp.int32, even.shape, 1) == 127
    even = pltpu.roll(even, 127, axis=1)
    rim = pltpu.roll(rim, 127, axis=1)
    return odd, jnp.where(last, rim, even), jnp.where(last, even, rim)


def offsets():
    steps = [
        (dx, dc, dy, dz)
        for dx in range(4) for dc in range(2) for dy in range(4) for dz in range(4)
    ][1:]
    return sorted(steps, key=lambda t: -sum(min(d, 4 - d) for d in (t[0], t[2], t[3])))


def kernel(
    zonal_h, merid_h, interp_h, slots_h, rows_h, innov_h, weight_h, cols_h, typev_h, windowv_h,
    count_h, type_h, window_h,
    x_out, r_out,
    zonal, merid, interp, slots, rows_in, innov, weight, cols, type_v, window_v,
    count_s, type_s, window_s, in_sem, winds, field, res, dirn, inc, force0, force1, square, colq, perm, mend, wnat,
    onehot, cweight, live, zrow, yrow, rblk, tsplit,
    colhot, proj, ssum, sside, stage, lgather, lscatter, sacc,
    send_f, send_b, recv_f, recv_b, wown,
    pack_w, pack_s, ns_w, ns_s, hp_w, hp_s, rrv, part, betav,
    a2a_send, a2a_recv, hw_send, hw_recv, hs_send, hs_recv,
):
    loads = [
        pltpu.make_async_copy(src, dst, in_sem.at[i])
        for i, (src, dst) in enumerate(
            (
                (slots_h, slots), (interp_h, interp), (count_h, count_s), (type_h, type_s),
                (window_h, window_s), (weight_h, weight), (innov_h, innov), (cols_h, cols),
                (rows_h, rows_in), (typev_h, type_v), (windowv_h, window_v), (zonal_h, zonal),
                (merid_h, merid),
            )
        )
    ]
    for load in loads:
        load.start()
    lat = lax.axis_index("lat")
    lon = lax.axis_index("lon")
    me = lat * N_LON + lon
    barrier = pltpu.get_barrier_semaphore()

    x, core = lat // 2, lax.rem(lat, 2)
    y, z = lon // 4, lax.rem(lon, 4)
    lats = {
        (dx, dc): lax.rem(x + dx, 4) * 2 + lax.rem(core + dc, 2)
        for dx in range(4) for dc in range(2)
    }
    lons = {
        (dy, dz): lax.rem(y + dy, 4) * 4 + lax.rem(z + dz, 4)
        for dy in range(4) for dz in range(4)
    }

    def everyone(act):
        for dx, dc, dy, dz in offsets():
            act(lats[dx, dc], lons[dy, dz])

    def plain(a, o):
        return a * N_LON + o

    def swapped(a, o):
        return lax.rem(o, 8) * 16 + a * 2 + o // 8

    def greet(a, o):
        pl.semaphore_signal(
            barrier, inc=1, device_id={"lat": a, "lon": o}, device_id_type=MESH
        )

    everyone(greet)

    north = lax.rem(lat + 1, N_LAT)
    south = lax.rem(lat + N_LAT - 1, N_LAT)
    east = lax.rem(lon + 1, N_LON)
    west = lax.rem(lon + N_LON - 1, N_LON)
    valid_s = jnp.where(lat > 0, 1.0, 0.0).astype(F32)
    valid_n = jnp.where(lat < N_LAT - 1, 1.0, 0.0).astype(F32)

    def to(src, dst, a, o, send, recv):
        return pltpu.make_async_remote_copy(
            src, dst, send, recv, device_id={"lat": a, "lon": o}, device_id_type=MESH
        )

    def edges(pack, hp, send, recv):
        targets = [
            (north, east), (north, west), (south, east), (south, west), (lat, east), (lat, west)
        ]
        return [
            to(pack, hp.at[i], a, o, send.at[i], recv.at[i]) for i, (a, o) in enumerate(targets)
        ]

    def halo_w():
        return edges(pack_w, hp_w, hw_send, hw_recv) + [
            to(wown, ns_w.at[0], north, lon, hw_send.at[6], hw_recv.at[6]),
            to(wown, ns_w.at[1], south, lon, hw_send.at[7], hw_recv.at[7]),
        ]

    def halo_s(deep):
        copies = edges(pack_s, hp_s, hs_send, hs_recv)
        k = 6
        for w, count in ((2, 8 if deep else 4), (1, 6 if deep else 2), (0, 4 if deep else 0)):
            if count == 0:
                continue
            high = pl.ds(w * LAT + LAT - count, count)
            low = pl.ds(w * LAT, count)
            copies.append(to(ssum.at[high], ns_s.at[0, high], north, lon, hs_send.at[k], hs_recv.at[k]))
            copies.append(
                to(ssum.at[low], ns_s.at[1, low], south, lon, hs_send.at[k + 1], hs_recv.at[k + 1])
            )
            k += 2
        return copies

    def sides(hp, base):
        lane = lax.broadcasted_iota(jnp.int32, hp.shape[1:], 1)
        both = jnp.where((lane & 15) < 8, hp[base], hp[base + 1])
        return [pltpu.roll(both, (256 - 16 * r - 8) % 128, axis=1) for r in range(LAT)]

    def a2a_start(src, dst, k, row_of, mine):
        def go(a, o):
            to(
                src.at[pl.ds(row_of(a, o) * 4, 4)], dst.at[pl.ds(mine * 4, 4)], a, o,
                a2a_send.at[k], a2a_recv.at[k],
            ).start()

        everyone(go)
        dst[pl.ds(mine * 4, 4), :] = src[pl.ds(row_of(lat, lon) * 4, 4), :]

    def a2a_wait(src, dst, k):
        got = dst.at[pl.ds(0, 4 * (NDEV - 1))]
        pltpu.make_async_copy(got, got, a2a_recv.at[k]).wait()
        gone = src.at[pl.ds(0, 4 * (NDEV - 1))]
        pltpu.make_async_copy(gone, gone, a2a_send.at[k]).wait()

    for load in loads:
        load.wait()
    for r in range(LAT):
        wnat[r, :LEV, :] = zonal[:, r, :]
        wnat[r, LEV:, :] = merid[:, r, :]
    pack_w[...] = pack_rows([wnat[r] for r in range(LAT)])
    natural = lax.broadcasted_iota(jnp.int32, (LON, LON), 0)
    held = lax.broadcasted_iota(jnp.int32, (LON, LON), 1)
    perm[...] = jnp.where(held == (natural & 1) * 128 + (natural >> 1), 1.0, 0.0).astype(BF16)
    here = lax.broadcasted_iota(jnp.int32, (128, 128), 0)
    there = lax.broadcasted_iota(jnp.int32, (128, 128), 1)
    goal = (here & 112) + ((here >> 2) & 1) * 8 + 2 * (here & 3) + ((here >> 3) & 1)
    mend[...] = jnp.where(there == goal, 1.0, 0.0).astype(BF16)
    for i in range(4):
        high, middle, low = exact(wnat[2 * i : 2 * i + 2].reshape(4 * LEV, LON))
        value = mm(high, perm[...]) + mm(middle, perm[...]) + mm(low, perm[...])
        wown[2 * i : 2 * i + 2] = value.reshape(2, 2 * LEV, LON)

    def tables(b, carry):
        at = pl.ds(pl.multiple_of(b * ROWS, ROWS), ROWS)
        slot = slots[:, at]
        wgt = interp[:, at]
        sender = slot >> 4
        inner = slot & 15
        sub = lax.broadcasted_iota(jnp.int32, (NDEV, ROWS), 0)
        sub16 = lax.broadcasted_iota(jnp.int32, (SLOTS, ROWS), 0)
        for k in range(KPTS):
            lanes = slice(k * ROWS, (k + 1) * ROWS)
            onehot[b, :, lanes] = jnp.where(sub == sender[k : k + 1], 1.0, 0.0).astype(BF16)
            cweight[b, :, lanes] = jnp.where(sub16 == inner[k : k + 1], wgt[k : k + 1], 0.0)
        lane = lax.broadcasted_iota(jnp.int32, (1, ROWS), 1)
        wl = jnp.where(lane < count_s[b], weight[b], 0.0)
        live[b] = wl
        zrow[b] = wl * innov[b]
        yrow[b] = jnp.zeros((1, ROWS), F32)
        return carry

    lax.fori_loop(0, NBLK, tables, 0, unroll=2)
    raw = jnp.concatenate([cols[:, a * 128 : (a + 1) * 128] for a in range(16)], axis=0).astype(F32)
    sub16 = lax.broadcasted_iota(jnp.int32, (16, 128), 0)
    lane16 = lax.broadcasted_iota(jnp.int32, (16, 128), 1) & 15
    slanted = pltpu.roll(raw, 0, axis=1, stride=1, stride_axis=0)
    for q in range(SLOTS):
        moved = pltpu.roll(slanted, (128 - q) % 128, axis=1)
        kept = jnp.where(lane16 == sub16, moved, 0.0)
        colq[q : q + 1, :] = jnp.sum(kept, axis=0, keepdims=True).astype(jnp.int32)

    def columns(n):
        return jnp.concatenate([colq[2 * n : 2 * n + 1, :], colq[2 * n + 1 : 2 * n + 2, :]], axis=1)

    for n in range(8):
        low = (columns(n) & 1) * 128 + ((columns(n) & 255) >> 1)
        sub = lax.broadcasted_iota(jnp.int32, (LON, 256), 0)
        colhot[n] = jnp.where(sub == low, 1.0, 0.0).astype(BF16)
    lane32 = lax.broadcasted_iota(jnp.int32, (CH, 32), 1)
    square[...] = jnp.zeros_like(square)
    for i in range(4):
        square[i * TYPES : (i + 1) * TYPES, :CH] = rows_in[...]
    opt_h, opt_l = split(square[...].T[:CH, :32])
    opt = jnp.where((lane32 & 8) == 0, opt_h, opt_l).astype(BF16)
    op1 = square[:TYPES, :]
    op_h, op_l = split(op1 + pltpu.roll(op1, CH, axis=1))
    opp = jnp.concatenate([op_h, op_l], axis=0).astype(BF16)
    ids = window_v[...] * TYPES + type_v[...]
    member = jnp.where(lax.broadcasted_iota(jnp.int32, (32, NBLK), 0) == ids, 1.0, 0.0).astype(BF16)
    def clear(r, carry):
        dirn[r] = jnp.zeros((CH, LANES), F32)
        dirn[r + LAT] = jnp.zeros((CH, LANES), F32)
        inc[r] = jnp.zeros((CH, LON), F32)
        return carry

    lax.fori_loop(0, LAT, clear, 0)
    rrv[...] = jnp.ones((1, 128), F32)
    part[...] = jnp.zeros((1, 128), F32)

    def build_winds():
        for copy in halo_w():
            copy.wait()
        side = sides(hp_w, 0) + sides(hp_w, 4) + sides(hp_w, 2)
        for g in range(EXT):
            if g < 8:
                main, ok = ns_w[0, g], valid_s
            elif g < 16:
                main, ok = wown[g - 8], None
            else:
                main, ok = ns_w[1, g - 16], valid_n
            side_g = side[g]
            both = jnp.concatenate([main, side_g], axis=1)
            u = both[:LEV]
            v = both[LEV:]
            values = (
                1.0 - jnp.abs(u) - jnp.abs(v),
                jnp.maximum(u, 0.0),
                jnp.maximum(-u, 0.0),
                jnp.maximum(v, 0.0),
                jnp.maximum(-v, 0.0),
            )
            for i, value in enumerate(values):
                winds[i, g] = value if ok is None else value * ok

    def advance(dst, src, shift, lo, hi, adjoint, unroll, extra=None):
        def body(g, carry):
            for var in range(4):
                at = slice(var * LEV, (var + 1) * LEV)
                mid = tiles(src[g - shift, at, :])
                below = tiles(src[g - shift - 1, at, :])
                above = tiles(src[g - shift + 1, at, :])
                keep, from_west, from_east = (tiles(winds[i, g]) for i in range(3))
                if adjoint:
                    left = east_of([w * m for w, m in zip(from_west, mid)])
                    right = west_of([w * m for w, m in zip(from_east, mid)])
                    up, down = tiles(winds[3, g + 1]), tiles(winds[4, g - 1])
                    up = [w * m for w, m in zip(up, above)]
                    down = [w * m for w, m in zip(down, below)]
                else:
                    left = [w * m for w, m in zip(from_west, west_of(mid))]
                    right = [w * m for w, m in zip(from_east, east_of(mid))]
                    up, down = tiles(winds[3, g]), tiles(winds[4, g])
                    up = [w * m for w, m in zip(up, below)]
                    down = [w * m for w, m in zip(down, above)]
                for i in range(3):
                    lanes = slice(i * 128, (i + 1) * 128)
                    out = keep[i] * mid[i] + left[i] + right[i] + up[i] + down[i]
                    dst[g, at, lanes] = out if extra is None else out + extra[g, at, lanes]
            return carry

        lax.fori_loop(lo, hi, body, 0, unroll=unroll)

    def project(window, source):
        def body(r, carry):
            high, low = split(source(r))
            both = jnp.concatenate([high, low], axis=0).astype(BF16)
            out = mm(opp, both)
            proj[r, window * TYPES : (window + 1) * TYPES, :] = out[:8] + out[8:]
            return carry

        lax.fori_loop(0, LAT, body, 0, unroll=8)

    def message(dst, row):
        for w in range(WIN):
            dst[pl.ds(w, NDEV, stride=4), :] = stage[w * 128 : (w + 1) * 128, :].T
        dst[pl.ds(3, NDEV, stride=4), :] = jnp.broadcast_to(row, (NDEV, 128))

    def total(recv):
        lanes = jnp.sum(recv[pl.ds(3, NDEV, stride=4), :], axis=0, keepdims=True)
        return jnp.broadcast_to(jnp.sum(lanes, axis=1, keepdims=True), (1, 128))

    def full(row):
        return jnp.concatenate([row, row, row], axis=1)

    def own_squares(value):
        own = value[:, :LON]
        return jnp.sum((own * own).reshape(8, 8, LON), axis=0)

    def forward(it):
        ping, pong = field.at[0], field.at[1]
        project(0, lambda r: res[r + 4, :, :LON])
        advance(pong, res, 4, 5, 19, False, 14)
        advance(ping, pong, 0, 6, 18, False, 12)
        project(1, lambda r: ping[r + 8, :, :LON])
        advance(pong, ping, 0, 7, 17, False, 10)
        advance(ping, pong, 0, 8, 16, False, 8)
        project(2, lambda r: ping[r + 8, :, :LON])
        for r in range(LAT):
            lgather[r * 48 : (r + 1) * 48, :] = jnp.concatenate(split(proj[r]), axis=0).astype(BF16)
        for n in range(8):
            found = mm(lgather[...], colhot[n])
            band = jnp.broadcast_to(columns(n) >> 8, (WT, 256))
            got = found[:WT] + found[WT : 2 * WT]
            for r in range(1, LAT):
                at = r * 2 * WT
                got = jnp.where(band == r, found[at : at + WT] + found[at + WT : at + 2 * WT], got)
            for half in range(2):
                for w in range(WIN):
                    stage[pl.ds(w * 128 + 2 * n + half, 8, stride=16), :] = got[
                        w * 8 : (w + 1) * 8, half * 128 : (half + 1) * 128
                    ]
        message(send_f, part[...])
        a2a_start(send_f, recv_f, 0, swapped, me)
        a2a_wait(send_f, recv_f, 0)
        norm = total(recv_f)
        beta = jnp.where(it == 1, jnp.zeros_like(norm), norm / rrv[...])
        rrv[...] = norm
        for w in range(WIN):
            table = recv_f[pl.ds(w, NDEV, stride=4), :].T
            high, low = split(table)
            for t in range(TYPES):
                at = slice(t * 16, (t + 1) * 16)
                tsplit[w * TYPES + t] = jnp.concatenate([high[at], low[at]], axis=0).astype(BF16)

        def look(b, acc):
            which = window_s[b] * TYPES + type_s[b]
            got = mm(tsplit[which], onehot[b])
            both = (got[:16] + got[16:]) * cweight[b]
            summed = (both[:, :128] + both[:, 128:256]) + (both[:, 256:384] + both[:, 384:])
            y = jnp.sum(summed, axis=0, keepdims=True) + beta * yrow[b]
            yrow[b] = y
            z = live[b] * y
            zrow[b] = z
            return acc + z * y

        quad = lax.fori_loop(0, NBLK, look, jnp.zeros((1, ROWS), F32), unroll=8)

        def turn(r, acc):
            p = res[r + 4] + full(beta) * dirn[r + 4]
            dirn[r + 4] = p
            return acc + own_squares(p)

        pp = lax.fori_loop(0, LAT, turn, jnp.zeros((8, LON), F32), unroll=2)
        pp = jnp.sum(pp, axis=0, keepdims=True)
        part[...] = quad + pp[:, :128] + pp[:, 128:]
        betav[...] = beta

    def forcing(value):
        high, low = split(value)
        return mm(opt, jnp.concatenate([high, high, low, low], axis=0).astype(BF16))

    def adjoint(it, alpha, deep):
        copies = halo_s(deep)
        for copy in copies:
            copy.start()
        ping, pong = field.at[0], field.at[1]
        into = {2: ping, 1: force1, 0: force0}
        near = {2: 8 if deep else 4, 1: 6 if deep else 2, 0: 4 if deep else 0}

        def own(r, c):
            for w in range(WIN):
                into[w][r + 8, :, :LON] = forcing(ssum[w * LAT + r])
            return c

        def own_side(r, c):
            for w in range(WIN):
                into[w][r + 8, :, LON:] = forcing(sside[r + 8, w * TYPES : (w + 1) * TYPES, :])
            return c

        def outside(w):
            count = near[w]
            if count == 0:
                return

            def body(i, c):
                for k, g, r in ((0, i + 8 - count, i + 8 - count), (1, 16 + i, i)):
                    into[w][g, :, :LON] = forcing(ns_s[k, w * LAT + r])
                    into[w][g, :, LON:] = forcing(sside[g, w * TYPES : (w + 1) * TYPES, :])
                return c

            lax.fori_loop(0, count, body, 0, unroll=4 if count % 4 == 0 else count // 2)

        def landed(w):
            if near[w]:
                at = 6 + 2 * (2 - w)
                for copy in copies[at : at + 2]:
                    copy.wait()

        lax.fori_loop(0, LAT, own, 0, unroll=4)
        for copy in copies[4:6]:
            copy.wait()
        for r, value in enumerate(sides(hp_s, 4)):
            sside[r + 8] = value
        lax.fori_loop(0, LAT, own_side, 0, unroll=8)
        advance(pong, ping, 0, 9, 15, True, 6)
        for copy in copies[:4]:
            copy.wait()
        for r, value in enumerate(sides(hp_s, 0)):
            sside[r] = value
        for r, value in enumerate(sides(hp_s, 2)):
            sside[r + 16] = value
        landed(2)
        outside(2)
        lo, hi = (1, 23) if deep else (5, 19)
        advance(pong, ping, 0, lo, 9, True, 9 - lo)
        advance(pong, ping, 0, 15, hi, True, hi - 15)
        landed(1)
        outside(1)
        lo, hi = lo + 1, hi - 1
        advance(ping, pong, 0, lo, hi, True, (hi - lo) // 2 if deep else hi - lo, force1)
        lo, hi = lo + 1, hi - 1
        advance(pong, ping, 0, lo, hi, True, (hi - lo) // 2 if deep else hi - lo)
        landed(0)
        outside(0)
        lo, hi = lo + 1, hi - 1
        advance(ping, pong, 0, lo, hi, True, 8, force0)
        zero = jnp.zeros((8, LON), F32)

        def done(acc):
            acc = jnp.sum(acc, axis=0, keepdims=True)
            part[...] = acc[:, :128] + acc[:, 128:]

        scale = full(alpha)
        if deep:

            @pl.when(it == 0)
            def _():
                def rim(i, c):
                    e = i + LAT * (i // 4)
                    ok = jnp.where(i < 4, valid_s, valid_n)
                    res[e] = ping[e + 4] * ok
                    return c

                def body(r, acc):
                    value = ping[r + 8]
                    res[r + 4] = value
                    return acc + own_squares(value)

                lax.fori_loop(0, 8, rim, 0)
                done(lax.fori_loop(0, LAT, body, zero, unroll=2))

            @pl.when(it > 0)
            def _():
                def rim(i, c):
                    e = i + LAT * (i // 4)
                    ok = jnp.where(i < 4, valid_s, valid_n)
                    res[e] -= scale * (dirn[e] + ping[e + 4]) * ok
                    return c

                def body(r, acc):
                    p = dirn[r + 4]
                    inc[r] += scale[:, :LON] * p[:, :LON]
                    value = res[r + 4] - scale * (p + ping[r + 8])
                    res[r + 4] = value
                    return acc + own_squares(value)

                lax.fori_loop(0, 8, rim, 0)
                done(lax.fori_loop(0, LAT, body, zero, unroll=2))
        else:
            narrow = scale[:, :LON]

            def body(r, c):
                p = dirn[r + 4, :, :LON]
                value = jnp.concatenate(
                    [
                        inc[r] + narrow * p,
                        res[r + 4, :, :LON] - narrow * (p + ping[r + 8, :, :LON]),
                    ],
                    axis=0,
                )
                high, middle, low = exact(value)
                value = mm_nt(high, perm[...]) + mm_nt(middle, perm[...]) + mm_nt(low, perm[...])
                x_out[r] = value[:CH]
                r_out[r] = value[CH:]
                return c

            lax.fori_loop(0, LAT, body, 0, unroll=2)

    def observe():
        def spread(b, c):
            z = zrow[b]
            value = cweight[b] * jnp.concatenate([z, z, z, z], axis=1)
            high, low = split(value)
            both = jnp.concatenate([high, low], axis=0).astype(BF16)
            out = mm_nt(both, onehot[b])
            rblk[pl.ds(pl.multiple_of(b * SLOTS, SLOTS), SLOTS), :] = out[:16] + out[16:]
            return c

        lax.fori_loop(0, NBLK, spread, 0, unroll=8)
        for q in range(SLOTS):
            high, low = split(rblk[pl.ds(q, NBLK, stride=SLOTS), :])
            out = mm(member, high.astype(BF16)) + mm(member, low.astype(BF16))
            for w in range(WIN):
                stage[pl.ds(w * 128 + q, 8, stride=16), :] = out[w * 8 : (w + 1) * 8]
        message(send_b, part[...])

    observe()
    pl.semaphore_wait(barrier, NDEV - 1)

    def outer(it, carry):
        a2a_start(send_b, recv_b, 1, plain, swapped(lat, lon))

        @pl.when(it == 0)
        def _():
            for copy in halo_w():
                copy.start()
            build_winds()

        @pl.when(it == 1)
        def _():
            def beyond(i, c):
                e = i + LAT * (i // 4)
                dirn[e] = res[e] + full(betav[...]) * dirn[e]
                return c

            lax.fori_loop(0, 8, beyond, 0)

        a2a_wait(send_b, recv_b, 1)
        for w in range(WIN):
            stage[w * 128 : (w + 1) * 128, :] = recv_b[pl.ds(w, NDEV, stride=4), :].T
        alpha = rrv[...] / total(recv_b)
        for n in range(8):
            halves = []
            for half in range(2):
                halves.append(
                    jnp.concatenate(
                        [stage[pl.ds(w * 128 + 2 * n + half, 8, stride=16), :] for w in range(WIN)],
                        axis=0,
                    )
                )
            high, low = split(jnp.concatenate(halves, axis=1))
            band = jnp.broadcast_to(columns(n) >> 8, (WT, 256))
            for r in range(LAT):
                here = band == r
                lscatter[r * 48 : (r + 1) * 48, :] = jnp.concatenate(
                    [jnp.where(here, high, 0.0), jnp.where(here, low, 0.0)], axis=0
                ).astype(BF16)
            out = mm_nt(lscatter[...], colhot[n])
            if n == 0:
                sacc[...] = out
            else:
                sacc[...] += out
        for r in range(LAT):
            value = sacc[r * 48 : r * 48 + WT, :] + sacc[r * 48 + WT : (r + 1) * 48, :]
            for w in range(WIN):
                ssum[w * LAT + r] = value[w * TYPES : (w + 1) * TYPES]
        mixed = pack_typed(
            [jnp.concatenate([ssum[w * LAT + r] for w in range(WIN)], axis=0) for r in range(LAT)]
        )
        mixed = mm(jnp.concatenate(split(mixed), axis=0).astype(BF16), mend[...])
        pack_s[...] = mixed[:WT] + mixed[WT:]
        @pl.when(it < 2)
        def _():
            adjoint(it, alpha, True)
            forward(it + 1)
            observe()

        @pl.when(it == 2)
        def _():
            adjoint(it, alpha, False)

        return carry

    lax.fori_loop(0, 3, outer, 0)


def flip(x_in, r_in, x_out, r_out):
    for r in range(LAT):
        x_out[:, r, :] = x_in[r]
        r_out[:, r, :] = r_in[r]


def shards(
    zonal_wind, merid_wind, operator_rows, innovation, error_weight, interp_weight, obs_slot,
    block_count, block_type, block_window, send_cols,
):
    vm = pl.BlockSpec(memory_space=pltpu.VMEM)
    V = pltpu.VMEM
    dma = pltpu.SemaphoreType.DMA
    x, r = pl.pallas_call(
        kernel,
        out_shape=[jax.ShapeDtypeStruct((LAT, CH, LON), F32)] * 2,
        in_specs=[pl.BlockSpec(memory_space=pl.ANY)] * 13,
        out_specs=[vm] * 2,
        scratch_shapes=[
            V((LEV, LAT, LON), F32),
            V((LEV, LAT, LON), F32),
            V((KPTS, NBLK * ROWS), F32),
            V((KPTS, NBLK * ROWS), jnp.int32),
            V((TYPES, CH), F32),
            V((NBLK, 1, ROWS), F32),
            V((NBLK, 1, ROWS), F32),
            V((1, NDEV * SLOTS), jnp.int32),
            V((1, NBLK), jnp.int32),
            V((1, NBLK), jnp.int32),
            pltpu.SMEM((NBLK,), jnp.int32),
            pltpu.SMEM((NBLK,), jnp.int32),
            pltpu.SMEM((NBLK,), jnp.int32),
            dma((13,)),
            V((5, EXT, LEV, LANES), F32),
            V((2, EXT, CH, LANES), F32),
            V((MID, CH, LANES), F32),
            V((MID, CH, LANES), F32),
            V((LAT, CH, LON), F32),
            V((EXT, CH, LANES), F32),
            V((EXT, CH, LANES), F32),
            V((128, 128), F32),
            V((SLOTS, 128), jnp.int32),
            V((LON, LON), BF16),
            V((128, 128), BF16),
            V((LAT, 2 * LEV, LON), F32),
            V((NBLK, NDEV, KPTS * ROWS), BF16),
            V((NBLK, SLOTS, KPTS * ROWS), F32),
            V((NBLK, 1, ROWS), F32),
            V((NBLK, 1, ROWS), F32),
            V((NBLK, 1, ROWS), F32),
            V((NBLK * SLOTS, NDEV), F32),
            V((WT, 32, NDEV), BF16),
            V((8, LON, 256), BF16),
            V((LAT, WT, LON), F32),
            V((WIN * LAT, TYPES, LON), F32),
            V((EXT, WT, 128), F32),
            V((WIN * 128, 128), F32),
            V((16 * WT, 256), BF16),
            V((16 * WT, 256), BF16),
            V((16 * WT, 256), F32),
            V((NDEV * 4, 128), F32),
            V((NDEV * 4, 128), F32),
            V((NDEV * 4, 128), F32),
            V((NDEV * 4, 128), F32),
            V((LAT, 2 * LEV, LON), F32),
            V((2 * LEV, 128), F32),
            V((WT, 128), F32),
            V((2, LAT, 2 * LEV, LON), F32),
            V((2, WIN * LAT, TYPES, LON), F32),
            V((6, 2 * LEV, 128), F32),
            V((6, WT, 128), F32),
            V((1, 128), F32),
            V((1, 128), F32),
            V((1, 128), F32),
            dma((2,)),
            dma((2,)),
            dma((8,)),
            dma((8,)),
            dma((12,)),
            dma((12,)),
        ],
        compiler_params=pltpu.CompilerParams(
            collective_id=0, has_side_effects=True, vmem_limit_bytes=60 << 20
        ),
        name="cg",
    )(
        zonal_wind, merid_wind, interp_weight, obs_slot, operator_rows,
        innovation.reshape(NBLK, 1, ROWS), error_weight.reshape(NBLK, 1, ROWS),
        send_cols, block_type.reshape(1, NBLK), block_window.reshape(1, NBLK),
        block_count, block_type, block_window,
    )
    shape = (4, LEV, LAT, LON)
    x, r = pl.pallas_call(
        flip,
        out_shape=[jax.ShapeDtypeStruct((CH, LAT, LON), F32)] * 2,
        in_specs=[vm] * 2,
        out_specs=[vm] * 2,
        name="flip",
    )(x, r)
    return x.reshape(shape), r.reshape(shape)


def solution(mesh):
    both = ("lat", "lon")
    in_specs = (
        P(None, "lat", "lon"),
        P(None, "lat", "lon"),
        P(),
        P(both),
        P(both),
        P(None, both),
        P(None, both),
        P(both),
        P(both),
        P(both),
        P(both, None),
    )
    out_specs = (P(None, None, "lat", "lon"), P(None, None, "lat", "lon"))
    return jax.shard_map(shards, mesh=mesh, in_specs=in_specs, out_specs=out_specs, check_vma=False)
```

```python
import functools

import jax
import jax.numpy as jnp
from jax import lax
from jax.experimental import pallas as pl
from jax.experimental.pallas import tpu as pltpu
from jax.sharding import PartitionSpec as P

MESH = pl.DeviceIdType.MESH
F32 = jnp.float32
BF16 = jnp.bfloat16

TYPES = 8
WIN = 3
WT = WIN * TYPES
KPTS = 4
SLOTS = 16
ROWS = 128
N_LAT = 8
N_LON = 16
NDEV = N_LAT * N_LON
NBLK = 32
LEV = 16
CH = 64
LAT = 8
LON = 256
EXT = 24
MID = 16
LANES = 384
NT = (((1,), (1,)), ((), ()))


def split(value):
    high = value.astype(BF16).astype(F32)
    return high, value - high


def exact(value):
    high = value.astype(BF16)
    rest = value - high.astype(F32)
    middle = rest.astype(BF16)
    return high, middle, (rest - middle.astype(F32)).astype(BF16)


def mm(left, right):
    return jnp.dot(left, right, preferred_element_type=F32)


def mm_nt(left, right):
    return lax.dot_general(left, right, NT, preferred_element_type=F32)


def pack_rows(rows):
    packed = None
    for r, row in enumerate(rows):
        lane = lax.broadcasted_iota(jnp.int32, (row.shape[0], 128), 1)
        ends = jnp.where(lane < 64, row[:, :128], row[:, 128:])
        moved = pltpu.roll(ends, (8 + 16 * r) % 128, axis=1)
        packed = moved if packed is None else jnp.where((lane >> 4) == r, moved, packed)
    return packed


def pack_typed(rows):
    packed = None
    for r, row in enumerate(rows):
        lane = lax.broadcasted_iota(jnp.int32, (row.shape[0], 128), 1)
        even = pltpu.roll(row[:, :128], (4 + 16 * r) % 128, axis=1)
        odd = pltpu.roll(row[:, 128:], (12 + 16 * r) % 128, axis=1)
        moved = jnp.where((lane & 15) < 8, even, odd)
        packed = moved if packed is None else jnp.where((lane >> 4) == r, moved, packed)
    return packed


def tiles(value):
    return value[:, :128], value[:, 128:256], value[:, 256:]


def west_of(parts):
    even, odd, rim = parts
    first = lax.broadcasted_iota(jnp.int32, even.shape, 1) == 0
    odd = pltpu.roll(odd, 1, axis=1)
    rim = pltpu.roll(rim, 1, axis=1)
    return jnp.where(first, rim, odd), even, jnp.where(first, odd, rim)


def east_of(parts):
    even, odd, rim = parts
    last = lax.broadcasted_iota(jnp.int32, even.shape, 1) == 127
    even = pltpu.roll(even, 127, axis=1)
    rim = pltpu.roll(rim, 127, axis=1)
    return odd, jnp.where(last, rim, even), jnp.where(last, even, rim)


def offsets():
    steps = [
        (dx, dc, dy, dz)
        for dx in range(4) for dc in range(2) for dy in range(4) for dz in range(4)
    ][1:]
    return sorted(steps, key=lambda t: -sum(min(d, 4 - d) for d in (t[0], t[2], t[3])))


def kernel(
    zonal_h, merid_h, interp_h, slots_h, rows_h, innov_h, weight_h, cols_h, typev_h, windowv_h,
    count_h, type_h, window_h,
    x_out, r_out,
    zonal, merid, interp, slots, rows_in, innov, weight, cols, type_v, window_v,
    count_s, type_s, window_s, in_sem, winds, field, res, dirn, inc, force0, force1, square, colq, perm, mend, wnat,
    onehot, cweight, live, zrow, yrow, rblk, tsplit,
    colhot, proj, ssum, sside, stage, lgather, lscatter, sacc,
    send_f, send_b, recv_f, recv_b, wown,
    pack_w, pack_s, ns_w, ns_s, hp_w, hp_s, rrv, part, rpart, betav, back, x_held, r_held, out_sem,
    a2a_send, a2a_recv, hw_send, hw_recv, hs_send, hs_recv,
):
    loads = [
        pltpu.make_async_copy(src, dst, in_sem.at[i])
        for i, (src, dst) in enumerate(
            (
                (slots_h, slots), (interp_h, interp), (count_h, count_s), (type_h, type_s),
                (window_h, window_s), (weight_h, weight), (innov_h, innov), (cols_h, cols),
                (rows_h, rows_in), (typev_h, type_v), (windowv_h, window_v), (zonal_h, zonal),
                (merid_h, merid),
            )
        )
    ]
    for load in loads:
        load.start()
    lat = lax.axis_index("lat")
    lon = lax.axis_index("lon")
    me = lat * N_LON + lon
    barrier = pltpu.get_barrier_semaphore()

    x, core = lat // 2, lax.rem(lat, 2)
    y, z = lon // 4, lax.rem(lon, 4)
    lats = {
        (dx, dc): lax.rem(x + dx, 4) * 2 + lax.rem(core + dc, 2)
        for dx in range(4) for dc in range(2)
    }
    lons = {
        (dy, dz): lax.rem(y + dy, 4) * 4 + lax.rem(z + dz, 4)
        for dy in range(4) for dz in range(4)
    }

    def everyone(act):
        for dx, dc, dy, dz in offsets():
            act(lats[dx, dc], lons[dy, dz])

    def plain(a, o):
        return a * N_LON + o

    def swapped(a, o):
        return lax.rem(o, 8) * 16 + a * 2 + o // 8

    def greet(a, o):
        pl.semaphore_signal(
            barrier, inc=1, device_id={"lat": a, "lon": o}, device_id_type=MESH
        )

    everyone(greet)

    north = lax.rem(lat + 1, N_LAT)
    south = lax.rem(lat + N_LAT - 1, N_LAT)
    east = lax.rem(lon + 1, N_LON)
    west = lax.rem(lon + N_LON - 1, N_LON)
    valid_s = jnp.where(lat > 0, 1.0, 0.0).astype(F32)
    valid_n = jnp.where(lat < N_LAT - 1, 1.0, 0.0).astype(F32)

    def to(src, dst, a, o, send, recv):
        return pltpu.make_async_remote_copy(
            src, dst, send, recv, device_id={"lat": a, "lon": o}, device_id_type=MESH
        )

    def edges(pack, hp, send, recv):
        targets = [
            (north, east), (north, west), (south, east), (south, west), (lat, east), (lat, west)
        ]
        return [
            to(pack, hp.at[i], a, o, send.at[i], recv.at[i]) for i, (a, o) in enumerate(targets)
        ]

    def halo_w():
        return edges(pack_w, hp_w, hw_send, hw_recv) + [
            to(wown, ns_w.at[0], north, lon, hw_send.at[6], hw_recv.at[6]),
            to(wown, ns_w.at[1], south, lon, hw_send.at[7], hw_recv.at[7]),
        ]

    def halo_s(deep):
        copies = edges(pack_s, hp_s, hs_send, hs_recv)
        k = 6
        for w, count in ((2, 8 if deep else 4), (1, 6 if deep else 2), (0, 4 if deep else 0)):
            if count == 0:
                continue
            high = pl.ds(w * LAT + LAT - count, count)
            low = pl.ds(w * LAT, count)
            copies.append(to(ssum.at[high], ns_s.at[0, high], north, lon, hs_send.at[k], hs_recv.at[k]))
            copies.append(
                to(ssum.at[low], ns_s.at[1, low], south, lon, hs_send.at[k + 1], hs_recv.at[k + 1])
            )
            k += 2
        return copies

    def sides(hp, base):
        lane = lax.broadcasted_iota(jnp.int32, hp.shape[1:], 1)
        both = jnp.where((lane & 15) < 8, hp[base], hp[base + 1])
        return [pltpu.roll(both, (256 - 16 * r - 8) % 128, axis=1) for r in range(LAT)]

    def a2a_start(src, dst, k, row_of, mine, rows):
        def go(a, o):
            to(
                src.at[pl.ds(row_of(a, o) * 4, rows)], dst.at[pl.ds(mine * 4, rows)], a, o,
                a2a_send.at[k], a2a_recv.at[k],
            ).start()

        everyone(go)
        dst[pl.ds(mine * 4, 4), :] = src[pl.ds(row_of(lat, lon) * 4, 4), :]

    def a2a_wait(src, dst, k, rows):
        got = dst.at[pl.ds(0, rows * (NDEV - 1))]
        pltpu.make_async_copy(got, got, a2a_recv.at[k]).wait()
        gone = src.at[pl.ds(0, rows * (NDEV - 1))]
        pltpu.make_async_copy(gone, gone, a2a_send.at[k]).wait()

    for load in loads:
        load.wait()
    for r in range(LAT):
        wnat[r, :LEV, :] = zonal[:, r, :]
        wnat[r, LEV:, :] = merid[:, r, :]
    pack_w[...] = pack_rows([wnat[r] for r in range(LAT)])
    natural = lax.broadcasted_iota(jnp.int32, (LON, LON), 0)
    held = lax.broadcasted_iota(jnp.int32, (LON, LON), 1)
    perm[...] = jnp.where(held == (natural & 1) * 128 + (natural >> 1), 1.0, 0.0).astype(BF16)
    back[...] = jnp.where(held == (natural & 127) * 2 + (natural >> 7), 1.0, 0.0).astype(BF16)
    here = lax.broadcasted_iota(jnp.int32, (128, 128), 0)
    there = lax.broadcasted_iota(jnp.int32, (128, 128), 1)
    goal = (here & 112) + ((here >> 2) & 1) * 8 + 2 * (here & 3) + ((here >> 3) & 1)
    mend[...] = jnp.where(there == goal, 1.0, 0.0).astype(BF16)
    for i in range(4):
        high, middle, low = exact(wnat[2 * i : 2 * i + 2].reshape(4 * LEV, LON))
        value = mm(high, perm[...]) + mm(middle, perm[...]) + mm(low, perm[...])
        wown[2 * i : 2 * i + 2] = value.reshape(2, 2 * LEV, LON)

    def tables(b, carry):
        at = pl.ds(pl.multiple_of(b * ROWS, ROWS), ROWS)
        slot = slots[:, at]
        wgt = interp[:, at]
        sender = slot >> 4
        inner = slot & 15
        sub = lax.broadcasted_iota(jnp.int32, (NDEV, ROWS), 0)
        sub16 = lax.broadcasted_iota(jnp.int32, (SLOTS, ROWS), 0)
        for k in range(KPTS):
            lanes = slice(k * ROWS, (k + 1) * ROWS)
            onehot[b, :, lanes] = jnp.where(sub == sender[k : k + 1], 1.0, 0.0).astype(BF16)
            cweight[b, :, lanes] = jnp.where(sub16 == inner[k : k + 1], wgt[k : k + 1], 0.0)
        lane = lax.broadcasted_iota(jnp.int32, (1, ROWS), 1)
        wl = jnp.where(lane < count_s[b], weight[b], 0.0)
        live[b] = wl
        zrow[b] = wl * innov[b]
        yrow[b] = jnp.zeros((1, ROWS), F32)
        return carry

    lax.fori_loop(0, NBLK, tables, 0, unroll=2)
    raw = jnp.concatenate([cols[:, a * 128 : (a + 1) * 128] for a in range(16)], axis=0).astype(F32)
    sub16 = lax.broadcasted_iota(jnp.int32, (16, 128), 0)
    lane16 = lax.broadcasted_iota(jnp.int32, (16, 128), 1) & 15
    slanted = pltpu.roll(raw, 0, axis=1, stride=1, stride_axis=0)
    for q in range(SLOTS):
        moved = pltpu.roll(slanted, (128 - q) % 128, axis=1)
        kept = jnp.where(lane16 == sub16, moved, 0.0)
        colq[q : q + 1, :] = jnp.sum(kept, axis=0, keepdims=True).astype(jnp.int32)

    def columns(n):
        return jnp.concatenate([colq[2 * n : 2 * n + 1, :], colq[2 * n + 1 : 2 * n + 2, :]], axis=1)

    for n in range(8):
        low = (columns(n) & 1) * 128 + ((columns(n) & 255) >> 1)
        sub = lax.broadcasted_iota(jnp.int32, (LON, 256), 0)
        colhot[n] = jnp.where(sub == low, 1.0, 0.0).astype(BF16)
    lane32 = lax.broadcasted_iota(jnp.int32, (CH, 32), 1)
    square[...] = jnp.zeros_like(square)
    for i in range(4):
        square[i * TYPES : (i + 1) * TYPES, :CH] = rows_in[...]
    opt_h, opt_l = split(square[...].T[:CH, :32])
    opt = jnp.where((lane32 & 8) == 0, opt_h, opt_l).astype(BF16)
    op1 = square[:TYPES, :]
    op_h, op_l = split(op1 + pltpu.roll(op1, CH, axis=1))
    opp = jnp.concatenate([op_h, op_l], axis=0).astype(BF16)
    ids = window_v[...] * TYPES + type_v[...]
    member = jnp.where(lax.broadcasted_iota(jnp.int32, (32, NBLK), 0) == ids, 1.0, 0.0).astype(BF16)
    def clear(r, carry):
        dirn[r] = jnp.zeros((CH, LANES), F32)
        dirn[r + LAT] = jnp.zeros((CH, LANES), F32)
        inc[r] = jnp.zeros((CH, LON), F32)
        return carry

    lax.fori_loop(0, LAT, clear, 0)
    rrv[...] = jnp.ones((1, 128), F32)
    rpart[...] = jnp.zeros((1, 128), F32)
    part[...] = jnp.zeros((1, 128), F32)

    def build_winds():
        for copy in halo_w():
            copy.wait()
        side = sides(hp_w, 0) + sides(hp_w, 4) + sides(hp_w, 2)
        for g in range(EXT):
            if g < 8:
                main, ok = ns_w[0, g], valid_s
            elif g < 16:
                main, ok = wown[g - 8], None
            else:
                main, ok = ns_w[1, g - 16], valid_n
            side_g = side[g]
            both = jnp.concatenate([main, side_g], axis=1)
            u = both[:LEV]
            v = both[LEV:]
            values = (
                1.0 - jnp.abs(u) - jnp.abs(v),
                jnp.maximum(u, 0.0),
                jnp.maximum(-u, 0.0),
                jnp.maximum(v, 0.0),
                jnp.maximum(-v, 0.0),
            )
            for i, value in enumerate(values):
                winds[i, g] = value if ok is None else value * ok

    def advance(dst, src, shift, lo, hi, adjoint, unroll, extra=None):
        def body(g, carry):
            for var in range(4):
                at = slice(var * LEV, (var + 1) * LEV)
                mid = tiles(src[g - shift, at, :])
                below = tiles(src[g - shift - 1, at, :])
                above = tiles(src[g - shift + 1, at, :])
                keep, from_west, from_east = (tiles(winds[i, g]) for i in range(3))
                if adjoint:
                    left = east_of([w * m for w, m in zip(from_west, mid)])
                    right = west_of([w * m for w, m in zip(from_east, mid)])
                    up, down = tiles(winds[3, g + 1]), tiles(winds[4, g - 1])
                    up = [w * m for w, m in zip(up, above)]
                    down = [w * m for w, m in zip(down, below)]
                else:
                    left = [w * m for w, m in zip(from_west, west_of(mid))]
                    right = [w * m for w, m in zip(from_east, east_of(mid))]
                    up, down = tiles(winds[3, g]), tiles(winds[4, g])
                    up = [w * m for w, m in zip(up, below)]
                    down = [w * m for w, m in zip(down, above)]
                for i in range(3):
                    lanes = slice(i * 128, (i + 1) * 128)
                    out = keep[i] * mid[i] + left[i] + right[i] + up[i] + down[i]
                    dst[g, at, lanes] = out if extra is None else out + extra[g, at, lanes]
            return carry

        lax.fori_loop(lo, hi, body, 0, unroll=unroll)

    def project(window, source):
        def body(r, carry):
            high, low = split(source(r))
            both = jnp.concatenate([high, low], axis=0).astype(BF16)
            out = mm(opp, both)
            proj[r, window * TYPES : (window + 1) * TYPES, :] = out[:8] + out[8:]
            return carry

        lax.fori_loop(0, LAT, body, 0, unroll=8)

    def message(dst, row):
        for w in range(WIN):
            dst[pl.ds(w, NDEV, stride=4), :] = stage[w * 128 : (w + 1) * 128, :].T
        dst[pl.ds(3, NDEV, stride=4), :] = jnp.broadcast_to(row, (NDEV, 128))

    def received(recv):
        return jnp.sum(recv[pl.ds(3, NDEV, stride=4), :], axis=0, keepdims=True)

    def spread_sum(lanes):
        return jnp.broadcast_to(jnp.sum(lanes, axis=1, keepdims=True), (1, 128))

    lower = lax.broadcasted_iota(jnp.int32, (1, 128), 1) < 64

    def fold(row):
        return row + pltpu.roll(row, 64, axis=1)

    def full(row):
        return jnp.concatenate([row, row, row], axis=1)

    def own_squares(value):
        own = value[:, :LON]
        return jnp.sum((own * own).reshape(8, 8, LON), axis=0)

    def forward(it):
        ping, pong = field.at[0], field.at[1]
        project(0, lambda r: res[r + 4, :, :LON])
        advance(pong, res, 4, 5, 19, False, 14)
        advance(ping, pong, 0, 6, 18, False, 12)
        project(1, lambda r: ping[r + 8, :, :LON])
        advance(pong, ping, 0, 7, 17, False, 10)
        advance(ping, pong, 0, 8, 16, False, 8)
        project(2, lambda r: ping[r + 8, :, :LON])
        for r in range(LAT):
            lgather[r * 48 : (r + 1) * 48, :] = jnp.concatenate(split(proj[r]), axis=0).astype(BF16)
        for n in range(8):
            found = mm(lgather[...], colhot[n])
            band = jnp.broadcast_to(columns(n) >> 8, (WT, 256))
            got = found[:WT] + found[WT : 2 * WT]
            for r in range(1, LAT):
                at = r * 2 * WT
                got = jnp.where(band == r, found[at : at + WT] + found[at + WT : at + 2 * WT], got)
            for half in range(2):
                for w in range(WIN):
                    stage[pl.ds(w * 128 + 2 * n + half, 8, stride=16), :] = got[
                        w * 8 : (w + 1) * 8, half * 128 : (half + 1) * 128
                    ]
        message(send_f, rpart[...])

        def exchange(rows):
            a2a_start(send_f, recv_f, 0, swapped, me, rows)
            a2a_wait(send_f, recv_f, 0, rows)

        @pl.when(it == 1)
        def _():
            exchange(3)

        @pl.when(it > 1)
        def _():
            exchange(4)

        norm = spread_sum(received(recv_f))
        beta = jnp.where(it == 1, jnp.zeros_like(norm), norm / rrv[...])
        for w in range(WIN):
            table = recv_f[pl.ds(w, NDEV, stride=4), :].T
            high, low = split(table)
            for t in range(TYPES):
                at = slice(t * 16, (t + 1) * 16)
                tsplit[w * TYPES + t] = jnp.concatenate([high[at], low[at]], axis=0).astype(BF16)

        def look(b, acc):
            which = window_s[b] * TYPES + type_s[b]
            got = mm(tsplit[which], onehot[b])
            both = (got[:16] + got[16:]) * cweight[b]
            summed = (both[:, :128] + both[:, 128:256]) + (both[:, 256:384] + both[:, 384:])
            y = jnp.sum(summed, axis=0, keepdims=True) + beta * yrow[b]
            yrow[b] = y
            z = live[b] * y
            zrow[b] = z
            return acc + z * y

        quad = lax.fori_loop(0, NBLK, look, jnp.zeros((1, ROWS), F32), unroll=8)

        def turn(r, acc):
            p = res[r + 4] + full(beta) * dirn[r + 4]
            dirn[r + 4] = p
            return acc + own_squares(p)

        pp = lax.fori_loop(0, LAT, turn, jnp.zeros((8, LON), F32), unroll=2)
        pp = jnp.sum(pp, axis=0, keepdims=True)
        part[...] = quad + pp[:, :128] + pp[:, 128:]
        betav[...] = beta

    def row_copy(i):
        held_rows, out = (x_held, x_out) if i < LAT else (r_held, r_out)
        return pltpu.make_async_copy(held_rows.at[i % LAT], out.at[:, i % LAT, :], out_sem.at[i])

    left = inc

    def restore(dst, out, base, group, row):
        rows = range(4 * group, 4 * group + 4)
        high, middle, low = exact(jnp.concatenate([row(r) for r in rows], axis=0))
        value = mm(high, back[...]) + mm(middle, back[...]) + mm(low, back[...])
        for i, r in enumerate(rows):
            dst[r] = value[i * CH : (i + 1) * CH]
            row_copy(base + r).start()

    def forcing(value):
        high, low = split(value)
        return mm(opt, jnp.concatenate([high, high, low, low], axis=0).astype(BF16))

    def adjoint(it, alpha, deep):
        copies = halo_s(deep)
        for copy in copies:
            copy.start()
        ping, pong = field.at[0], field.at[1]
        into = {2: ping, 1: force1, 0: force0}
        near = {2: 8 if deep else 4, 1: 6 if deep else 2, 0: 4 if deep else 0}

        def own(r, c):
            for w in range(WIN):
                into[w][r + 8, :, :LON] = forcing(ssum[w * LAT + r])
            return c

        def own_side(r, c):
            for w in range(WIN):
                into[w][r + 8, :, LON:] = forcing(sside[r + 8, w * TYPES : (w + 1) * TYPES, :])
            return c

        def outside(w):
            count = near[w]
            if count == 0:
                return

            def body(i, c):
                for k, g, r in ((0, i + 8 - count, i + 8 - count), (1, 16 + i, i)):
                    into[w][g, :, :LON] = forcing(ns_s[k, w * LAT + r])
                    into[w][g, :, LON:] = forcing(sside[g, w * TYPES : (w + 1) * TYPES, :])
                return c

            lax.fori_loop(0, count, body, 0, unroll=4 if count % 4 == 0 else count // 2)

        def landed(w):
            if near[w]:
                at = 6 + 2 * (2 - w)
                for copy in copies[at : at + 2]:
                    copy.wait()

        if not deep:
            narrow = full(alpha)[:, :LON]
            for group in range(2):
                restore(x_held, x_out, 0, group, lambda r: inc[r] + narrow * dirn[r + 4, :, :LON])
            for r in range(LAT):
                left[r] = res[r + 4, :, :LON] - narrow * dirn[r + 4, :, :LON]
        lax.fori_loop(0, LAT, own, 0, unroll=4)
        for copy in copies[4:6]:
            copy.wait()
        for r, value in enumerate(sides(hp_s, 4)):
            sside[r + 8] = value
        lax.fori_loop(0, LAT, own_side, 0, unroll=8)
        advance(pong, ping, 0, 9, 15, True, 6)
        for copy in copies[:4]:
            copy.wait()
        for r, value in enumerate(sides(hp_s, 0)):
            sside[r] = value
        for r, value in enumerate(sides(hp_s, 2)):
            sside[r + 16] = value
        landed(2)
        outside(2)
        lo, hi = (1, 23) if deep else (5, 19)
        advance(pong, ping, 0, lo, 9, True, 9 - lo)
        advance(pong, ping, 0, 15, hi, True, hi - 15)
        landed(1)
        outside(1)
        lo, hi = lo + 1, hi - 1
        advance(ping, pong, 0, lo, hi, True, (hi - lo) // 2 if deep else hi - lo, force1)
        lo, hi = lo + 1, hi - 1
        advance(pong, ping, 0, lo, hi, True, (hi - lo) // 2 if deep else hi - lo)
        landed(0)
        outside(0)
        lo, hi = lo + 1, hi - 1
        advance(ping, pong, 0, lo, hi, True, 8, force0)
        zero = jnp.zeros((8, LON), F32)

        def done(acc):
            acc = jnp.sum(acc, axis=0, keepdims=True)
            rpart[...] = acc[:, :128] + acc[:, 128:]

        scale = full(alpha)
        if deep:

            @pl.when(it == 0)
            def _():
                def rim(i, c):
                    e = i + LAT * (i // 4)
                    ok = jnp.where(i < 4, valid_s, valid_n)
                    res[e] = ping[e + 4] * ok
                    return c

                def body(r, acc):
                    value = ping[r + 8]
                    res[r + 4] = value
                    return acc + own_squares(value)

                lax.fori_loop(0, 8, rim, 0)
                done(lax.fori_loop(0, LAT, body, zero, unroll=2))

            @pl.when(it > 0)
            def _():
                def rim(i, c):
                    e = i + LAT * (i // 4)
                    ok = jnp.where(i < 4, valid_s, valid_n)
                    res[e] -= scale * (dirn[e] + ping[e + 4]) * ok
                    return c

                def body(r, acc):
                    p = dirn[r + 4]
                    inc[r] += scale[:, :LON] * p[:, :LON]
                    value = res[r + 4] - scale * (p + ping[r + 8])
                    res[r + 4] = value
                    return acc + own_squares(value)

                lax.fori_loop(0, 8, rim, 0)
                done(lax.fori_loop(0, LAT, body, zero, unroll=2))
        else:
            for group in range(2):
                restore(
                    r_held, r_out, LAT, group,
                    lambda r: left[r] - scale[:, :LON] * ping[r + 8, :, :LON],
                )
            for i in range(2 * LAT):
                row_copy(i).wait()

    def observe():
        def spread(b, c):
            z = zrow[b]
            value = cweight[b] * jnp.concatenate([z, z, z, z], axis=1)
            high, low = split(value)
            both = jnp.concatenate([high, low], axis=0).astype(BF16)
            out = mm_nt(both, onehot[b])
            rblk[pl.ds(pl.multiple_of(b * SLOTS, SLOTS), SLOTS), :] = out[:16] + out[16:]
            return c

        lax.fori_loop(0, NBLK, spread, 0, unroll=8)
        for q in range(SLOTS):
            high, low = split(rblk[pl.ds(q, NBLK, stride=SLOTS), :])
            out = mm(member, high.astype(BF16)) + mm(member, low.astype(BF16))
            for w in range(WIN):
                stage[pl.ds(w * 128 + q, 8, stride=16), :] = out[w * 8 : (w + 1) * 8]
        message(send_b, jnp.where(lower, fold(part[...]), fold(rpart[...])))

    observe()
    pl.semaphore_wait(barrier, NDEV - 1)

    def outer(it, carry):
        @pl.when(it == 0)
        def _():
            a2a_start(send_b, recv_b, 1, plain, swapped(lat, lon), 3)

        @pl.when(it > 0)
        def _():
            a2a_start(send_b, recv_b, 1, plain, swapped(lat, lon), 4)


        @pl.when(it == 0)
        def _():
            for copy in halo_w():
                copy.start()
            build_winds()

        @pl.when(it == 1)
        def _():
            def beyond(i, c):
                e = i + LAT * (i // 4)
                dirn[e] = res[e] + full(betav[...]) * dirn[e]
                return c

            lax.fori_loop(0, 8, beyond, 0)

        @pl.when(it == 0)
        def _():
            a2a_wait(send_b, recv_b, 1, 3)

        @pl.when(it > 0)
        def _():
            a2a_wait(send_b, recv_b, 1, 4)

        for w in range(WIN):
            stage[w * 128 : (w + 1) * 128, :] = recv_b[pl.ds(w, NDEV, stride=4), :].T
        sums = received(recv_b)
        norm = spread_sum(jnp.where(lower, 0.0, sums))
        rrv[...] = norm
        alpha = norm / spread_sum(jnp.where(lower, sums, 0.0))
        for n in range(8):
            halves = []
            for half in range(2):
                halves.append(
                    jnp.concatenate(
                        [stage[pl.ds(w * 128 + 2 * n + half, 8, stride=16), :] for w in range(WIN)],
                        axis=0,
                    )
                )
            high, low = split(jnp.concatenate(halves, axis=1))
            band = jnp.broadcast_to(columns(n) >> 8, (WT, 256))
            for r in range(LAT):
                here = band == r
                lscatter[r * 48 : (r + 1) * 48, :] = jnp.concatenate(
                    [jnp.where(here, high, 0.0), jnp.where(here, low, 0.0)], axis=0
                ).astype(BF16)
            out = mm_nt(lscatter[...], colhot[n])
            if n == 0:
                sacc[...] = out
            else:
                sacc[...] += out
        for r in range(LAT):
            value = sacc[r * 48 : r * 48 + WT, :] + sacc[r * 48 + WT : (r + 1) * 48, :]
            for w in range(WIN):
                ssum[w * LAT + r] = value[w * TYPES : (w + 1) * TYPES]
        mixed = pack_typed(
            [jnp.concatenate([ssum[w * LAT + r] for w in range(WIN)], axis=0) for r in range(LAT)]
        )
        mixed = mm(jnp.concatenate(split(mixed), axis=0).astype(BF16), mend[...])
        pack_s[...] = mixed[:WT] + mixed[WT:]
        @pl.when(it < 2)
        def _():
            adjoint(it, alpha, True)
            forward(it + 1)
            observe()

        @pl.when(it == 2)
        def _():
            adjoint(it, alpha, False)

        return carry

    lax.fori_loop(0, 3, outer, 0)


def relay(x_in, r_in, x_out, r_out, held, load, store):
    loads, stores = [], []
    for i in range(8):
        src, dst = (x_in, x_out) if i < 4 else (r_in, r_out)
        at = pl.ds(i % 4 * LEV, LEV)
        loads.append(pltpu.make_async_copy(src.at[at], held.at[i], load.at[i]))
        stores.append(pltpu.make_async_copy(held.at[i], dst.at[at], store.at[i]))
    for copy in loads:
        copy.start()
    for first, second in zip(loads, stores):
        first.wait()
        second.start()
    for copy in stores:
        copy.wait()


def shards(
    zonal_wind, merid_wind, operator_rows, innovation, error_weight, interp_weight, obs_slot,
    block_count, block_type, block_window, send_cols,
):
    V = pltpu.VMEM
    dma = pltpu.SemaphoreType.DMA
    x, r = pl.pallas_call(
        kernel,
        out_shape=[jax.ShapeDtypeStruct((CH, LAT, LON), F32)] * 2,
        in_specs=[pl.BlockSpec(memory_space=pl.ANY)] * 13,
        out_specs=[pl.BlockSpec(memory_space=pl.ANY)] * 2,
        scratch_shapes=[
            V((LEV, LAT, LON), F32),
            V((LEV, LAT, LON), F32),
            V((KPTS, NBLK * ROWS), F32),
            V((KPTS, NBLK * ROWS), jnp.int32),
            V((TYPES, CH), F32),
            V((NBLK, 1, ROWS), F32),
            V((NBLK, 1, ROWS), F32),
            V((1, NDEV * SLOTS), jnp.int32),
            V((1, NBLK), jnp.int32),
            V((1, NBLK), jnp.int32),
            pltpu.SMEM((NBLK,), jnp.int32),
            pltpu.SMEM((NBLK,), jnp.int32),
            pltpu.SMEM((NBLK,), jnp.int32),
            dma((13,)),
            V((5, EXT, LEV, LANES), F32),
            V((2, EXT, CH, LANES), F32),
            V((MID, CH, LANES), F32),
            V((MID, CH, LANES), F32),
            V((LAT, CH, LON), F32),
            V((EXT, CH, LANES), F32),
            V((EXT, CH, LANES), F32),
            V((128, 128), F32),
            V((SLOTS, 128), jnp.int32),
            V((LON, LON), BF16),
            V((128, 128), BF16),
            V((LAT, 2 * LEV, LON), F32),
            V((NBLK, NDEV, KPTS * ROWS), BF16),
            V((NBLK, SLOTS, KPTS * ROWS), F32),
            V((NBLK, 1, ROWS), F32),
            V((NBLK, 1, ROWS), F32),
            V((NBLK, 1, ROWS), F32),
            V((NBLK * SLOTS, NDEV), F32),
            V((WT, 32, NDEV), BF16),
            V((8, LON, 256), BF16),
            V((LAT, WT, LON), F32),
            V((WIN * LAT, TYPES, LON), F32),
            V((EXT, WT, 128), F32),
            V((WIN * 128, 128), F32),
            V((16 * WT, 256), BF16),
            V((16 * WT, 256), BF16),
            V((16 * WT, 256), F32),
            V((NDEV * 4, 128), F32),
            V((NDEV * 4, 128), F32),
            V((NDEV * 4, 128), F32),
            V((NDEV * 4, 128), F32),
            V((LAT, 2 * LEV, LON), F32),
            V((2 * LEV, 128), F32),
            V((WT, 128), F32),
            V((2, LAT, 2 * LEV, LON), F32),
            V((2, WIN * LAT, TYPES, LON), F32),
            V((6, 2 * LEV, 128), F32),
            V((6, WT, 128), F32),
            V((1, 128), F32),
            V((1, 128), F32),
            V((1, 128), F32),
            V((1, 128), F32),
            V((LON, LON), BF16),
            V((LAT, CH, LON), F32),
            V((LAT, CH, LON), F32),
            dma((2 * LAT,)),
            dma((2,)),
            dma((2,)),
            dma((8,)),
            dma((8,)),
            dma((12,)),
            dma((12,)),
        ],
        compiler_params=pltpu.CompilerParams(
            collective_id=0, has_side_effects=True, vmem_limit_bytes=60 << 20
        ),
        name="cg",
    )(
        zonal_wind, merid_wind, interp_weight, obs_slot, operator_rows,
        innovation.reshape(NBLK, 1, ROWS), error_weight.reshape(NBLK, 1, ROWS),
        send_cols, block_type.reshape(1, NBLK), block_window.reshape(1, NBLK),
        block_count, block_type, block_window,
    )
    shape = (4, LEV, LAT, LON)
    hbm = pl.BlockSpec(memory_space=pl.ANY)
    x, r = pl.pallas_call(
        relay,
        out_shape=[jax.ShapeDtypeStruct((CH, LAT, LON), F32)] * 2,
        in_specs=[hbm] * 2,
        out_specs=[hbm] * 2,
        scratch_shapes=[
            pltpu.VMEM((8, LEV, LAT, LON), F32),
            pltpu.SemaphoreType.DMA((8,)),
            pltpu.SemaphoreType.DMA((8,)),
        ],
        compiler_params=pltpu.CompilerParams(vmem_limit_bytes=60 << 20),
        name="relay",
    )(x, r)
    return x.reshape(shape), r.reshape(shape)


def solution(mesh):
    both = ("lat", "lon")
    in_specs = (
        P(None, "lat", "lon"),
        P(None, "lat", "lon"),
        P(),
        P(both),
        P(both),
        P(None, both),
        P(None, both),
        P(both),
        P(both),
        P(both),
        P(both, None),
    )
    out_specs = (P(None, None, "lat", "lon"), P(None, None, "lat", "lon"))
    return jax.shard_map(shards, mesh=mesh, in_specs=in_specs, out_specs=out_specs, check_vma=False)
```

```python
import functools

import jax
import jax.numpy as jnp
from jax import lax
from jax.experimental import pallas as pl
from jax.experimental.pallas import tpu as pltpu
from jax.sharding import PartitionSpec as P

MESH = pl.DeviceIdType.MESH
F32 = jnp.float32
BF16 = jnp.bfloat16

TYPES = 8
WIN = 3
WT = WIN * TYPES
KPTS = 4
SLOTS = 16
ROWS = 128
N_LAT = 8
N_LON = 16
NDEV = N_LAT * N_LON
NBLK = 32
LEV = 16
CH = 64
LAT = 8
LON = 256
EXT = 24
MID = 16
LANES = 384
NT = (((1,), (1,)), ((), ()))


def split(value):
    high = value.astype(BF16).astype(F32)
    return high, value - high


def exact(value):
    high = value.astype(BF16)
    rest = value - high.astype(F32)
    middle = rest.astype(BF16)
    return high, middle, (rest - middle.astype(F32)).astype(BF16)


def mm(left, right):
    return jnp.dot(left, right, preferred_element_type=F32)


def mm_nt(left, right):
    return lax.dot_general(left, right, NT, preferred_element_type=F32)


def pack_rows(rows):
    packed = None
    for r, row in enumerate(rows):
        lane = lax.broadcasted_iota(jnp.int32, (row.shape[0], 128), 1)
        ends = jnp.where(lane < 64, row[:, :128], row[:, 128:])
        moved = pltpu.roll(ends, (8 + 16 * r) % 128, axis=1)
        packed = moved if packed is None else jnp.where((lane >> 4) == r, moved, packed)
    return packed


def pack_typed(rows):
    packed = None
    for r, row in enumerate(rows):
        lane = lax.broadcasted_iota(jnp.int32, (row.shape[0], 128), 1)
        even = pltpu.roll(row[:, :128], (4 + 16 * r) % 128, axis=1)
        odd = pltpu.roll(row[:, 128:], (12 + 16 * r) % 128, axis=1)
        moved = jnp.where((lane & 15) < 8, even, odd)
        packed = moved if packed is None else jnp.where((lane >> 4) == r, moved, packed)
    return packed


def tiles(value):
    return value[:, :128], value[:, 128:256], value[:, 256:]


def west_of(parts):
    even, odd, rim = parts
    first = lax.broadcasted_iota(jnp.int32, even.shape, 1) == 0
    odd = pltpu.roll(odd, 1, axis=1)
    rim = pltpu.roll(rim, 1, axis=1)
    return jnp.where(first, rim, odd), even, jnp.where(first, odd, rim)


def east_of(parts):
    even, odd, rim = parts
    last = lax.broadcasted_iota(jnp.int32, even.shape, 1) == 127
    even = pltpu.roll(even, 127, axis=1)
    rim = pltpu.roll(rim, 127, axis=1)
    return odd, jnp.where(last, rim, even), jnp.where(last, even, rim)


def offsets():
    steps = [
        (dx, dc, dy, dz)
        for dx in range(4) for dc in range(2) for dy in range(4) for dz in range(4)
    ][1:]
    return sorted(steps, key=lambda t: -sum(min(d, 4 - d) for d in (t[0], t[2], t[3])))


def kernel(
    zonal_h, merid_h, interp_h, slots_h, rows_h, innov_h, weight_h, cols_h, typev_h, windowv_h,
    count_h, type_h, window_h,
    x_out, r_out,
    zonal, merid, interp, slots, rows_in, innov, weight, cols, type_v, window_v,
    count_s, type_s, window_s, in_sem, winds, field, res, dirn, inc, force0, force1, square, colq, perm, mend, wnat,
    onehot, cweight, live, zrow, yrow, rblk, tsplit,
    colhot, proj, ssum, sside, stage, lgather, lscatter, sacc,
    send_f, send_b, recv_f, recv_b, wown,
    pack_w, pack_s, ns_w, ns_s, hp_w, hp_s, rrv, part, rpart, betav, back, x_held, r_held, out_sem,
    a2a_send, a2a_recv, hw_send, hw_recv, hs_send, hs_recv,
):
    loads = [
        pltpu.make_async_copy(src, dst, in_sem.at[i])
        for i, (src, dst) in enumerate(
            (
                (slots_h, slots), (interp_h, interp), (count_h, count_s), (type_h, type_s),
                (window_h, window_s), (weight_h, weight), (innov_h, innov), (cols_h, cols),
                (rows_h, rows_in), (typev_h, type_v), (windowv_h, window_v), (zonal_h, zonal),
                (merid_h, merid),
            )
        )
    ]
    for load in loads:
        load.start()
    lat = lax.axis_index("lat")
    lon = lax.axis_index("lon")
    me = lat * N_LON + lon
    barrier = pltpu.get_barrier_semaphore()

    x, core = lat // 2, lax.rem(lat, 2)
    y, z = lon // 4, lax.rem(lon, 4)
    lats = {
        (dx, dc): lax.rem(x + dx, 4) * 2 + lax.rem(core + dc, 2)
        for dx in range(4) for dc in range(2)
    }
    lons = {
        (dy, dz): lax.rem(y + dy, 4) * 4 + lax.rem(z + dz, 4)
        for dy in range(4) for dz in range(4)
    }

    def everyone(act):
        for dx, dc, dy, dz in offsets():
            act(lats[dx, dc], lons[dy, dz])

    def plain(a, o):
        return a * N_LON + o

    def swapped(a, o):
        return lax.rem(o, 8) * 16 + a * 2 + o // 8

    def greet(a, o):
        pl.semaphore_signal(
            barrier, inc=1, device_id={"lat": a, "lon": o}, device_id_type=MESH
        )

    everyone(greet)

    north = lax.rem(lat + 1, N_LAT)
    south = lax.rem(lat + N_LAT - 1, N_LAT)
    east = lax.rem(lon + 1, N_LON)
    west = lax.rem(lon + N_LON - 1, N_LON)
    valid_s = jnp.where(lat > 0, 1.0, 0.0).astype(F32)
    valid_n = jnp.where(lat < N_LAT - 1, 1.0, 0.0).astype(F32)

    def to(src, dst, a, o, send, recv):
        return pltpu.make_async_remote_copy(
            src, dst, send, recv, device_id={"lat": a, "lon": o}, device_id_type=MESH
        )

    def edges(pack, hp, send, recv):
        targets = [
            (north, east), (north, west), (south, east), (south, west), (lat, east), (lat, west)
        ]
        return [
            to(pack, hp.at[i], a, o, send.at[i], recv.at[i]) for i, (a, o) in enumerate(targets)
        ]

    def halo_w():
        return edges(pack_w, hp_w, hw_send, hw_recv) + [
            to(wown, ns_w.at[0], north, lon, hw_send.at[6], hw_recv.at[6]),
            to(wown, ns_w.at[1], south, lon, hw_send.at[7], hw_recv.at[7]),
        ]

    def halo_s(deep):
        copies = edges(pack_s, hp_s, hs_send, hs_recv)
        k = 6
        for w, count in ((2, 8 if deep else 4), (1, 6 if deep else 2), (0, 4 if deep else 0)):
            if count == 0:
                continue
            high = pl.ds(w * LAT + LAT - count, count)
            low = pl.ds(w * LAT, count)
            copies.append(to(ssum.at[high], ns_s.at[0, high], north, lon, hs_send.at[k], hs_recv.at[k]))
            copies.append(
                to(ssum.at[low], ns_s.at[1, low], south, lon, hs_send.at[k + 1], hs_recv.at[k + 1])
            )
            k += 2
        return copies

    def sides(hp, base):
        lane = lax.broadcasted_iota(jnp.int32, hp.shape[1:], 1)
        both = jnp.where((lane & 15) < 8, hp[base], hp[base + 1])
        return [pltpu.roll(both, (256 - 16 * r - 8) % 128, axis=1) for r in range(LAT)]

    def a2a_start(src, dst, k, row_of, mine, rows):
        def go(a, o):
            to(
                src.at[pl.ds(row_of(a, o) * 4, rows)], dst.at[pl.ds(mine * 4, rows)], a, o,
                a2a_send.at[k], a2a_recv.at[k],
            ).start()

        everyone(go)
        dst[pl.ds(mine * 4, 4), :] = src[pl.ds(row_of(lat, lon) * 4, 4), :]

    def a2a_wait(src, dst, k, rows):
        got = dst.at[pl.ds(0, rows * (NDEV - 1))]
        pltpu.make_async_copy(got, got, a2a_recv.at[k]).wait()
        gone = src.at[pl.ds(0, rows * (NDEV - 1))]
        pltpu.make_async_copy(gone, gone, a2a_send.at[k]).wait()

    for load in loads:
        load.wait()
    for r in range(LAT):
        wnat[r, :LEV, :] = zonal[:, r, :]
        wnat[r, LEV:, :] = merid[:, r, :]
    pack_w[...] = pack_rows([wnat[r] for r in range(LAT)])
    natural = lax.broadcasted_iota(jnp.int32, (LON, LON), 0)
    held = lax.broadcasted_iota(jnp.int32, (LON, LON), 1)
    perm[...] = jnp.where(held == (natural & 1) * 128 + (natural >> 1), 1.0, 0.0).astype(BF16)
    back[...] = jnp.where(held == (natural & 127) * 2 + (natural >> 7), 1.0, 0.0).astype(BF16)
    here = lax.broadcasted_iota(jnp.int32, (128, 128), 0)
    there = lax.broadcasted_iota(jnp.int32, (128, 128), 1)
    goal = (here & 112) + ((here >> 2) & 1) * 8 + 2 * (here & 3) + ((here >> 3) & 1)
    mend[...] = jnp.where(there == goal, 1.0, 0.0).astype(BF16)
    for i in range(4):
        high, middle, low = exact(wnat[2 * i : 2 * i + 2].reshape(4 * LEV, LON))
        value = mm(high, perm[...]) + mm(middle, perm[...]) + mm(low, perm[...])
        wown[2 * i : 2 * i + 2] = value.reshape(2, 2 * LEV, LON)

    def tables(b, carry):
        at = pl.ds(pl.multiple_of(b * ROWS, ROWS), ROWS)
        slot = slots[:, at]
        wgt = interp[:, at]
        sender = slot >> 4
        inner = slot & 15
        sub = lax.broadcasted_iota(jnp.int32, (NDEV, ROWS), 0)
        sub16 = lax.broadcasted_iota(jnp.int32, (SLOTS, ROWS), 0)
        for k in range(KPTS):
            lanes = slice(k * ROWS, (k + 1) * ROWS)
            onehot[b, :, lanes] = jnp.where(sub == sender[k : k + 1], 1.0, 0.0).astype(BF16)
            cweight[b, :, lanes] = jnp.where(sub16 == inner[k : k + 1], wgt[k : k + 1], 0.0)
        lane = lax.broadcasted_iota(jnp.int32, (1, ROWS), 1)
        wl = jnp.where(lane < count_s[b], weight[b], 0.0)
        live[b] = wl
        zrow[b] = wl * innov[b]
        yrow[b] = jnp.zeros((1, ROWS), F32)
        return carry

    lax.fori_loop(0, NBLK, tables, 0, unroll=4)
    raw = jnp.concatenate([cols[:, a * 128 : (a + 1) * 128] for a in range(16)], axis=0).astype(F32)
    sub16 = lax.broadcasted_iota(jnp.int32, (16, 128), 0)
    lane16 = lax.broadcasted_iota(jnp.int32, (16, 128), 1) & 15
    slanted = pltpu.roll(raw, 0, axis=1, stride=1, stride_axis=0)
    for q in range(SLOTS):
        moved = pltpu.roll(slanted, (128 - q) % 128, axis=1)
        kept = jnp.where(lane16 == sub16, moved, 0.0)
        colq[q : q + 1, :] = jnp.sum(kept, axis=0, keepdims=True).astype(jnp.int32)

    def columns(n):
        return jnp.concatenate([colq[2 * n : 2 * n + 1, :], colq[2 * n + 1 : 2 * n + 2, :]], axis=1)

    for n in range(8):
        low = (columns(n) & 1) * 128 + ((columns(n) & 255) >> 1)
        sub = lax.broadcasted_iota(jnp.int32, (LON, 256), 0)
        colhot[n] = jnp.where(sub == low, 1.0, 0.0).astype(BF16)
    lane32 = lax.broadcasted_iota(jnp.int32, (CH, 32), 1)
    square[...] = jnp.zeros_like(square)
    for i in range(4):
        square[i * TYPES : (i + 1) * TYPES, :CH] = rows_in[...]
    opt_h, opt_l = split(square[...].T[:CH, :32])
    opt = jnp.where((lane32 & 8) == 0, opt_h, opt_l).astype(BF16)
    op1 = square[:TYPES, :]
    op_h, op_l = split(op1 + pltpu.roll(op1, CH, axis=1))
    opp = jnp.concatenate([op_h, op_l], axis=0).astype(BF16)
    ids = window_v[...] * TYPES + type_v[...]
    member = jnp.where(lax.broadcasted_iota(jnp.int32, (32, NBLK), 0) == ids, 1.0, 0.0).astype(BF16)
    def clear(r, carry):
        dirn[r] = jnp.zeros((CH, LANES), F32)
        dirn[r + LAT] = jnp.zeros((CH, LANES), F32)
        inc[r] = jnp.zeros((CH, LON), F32)
        return carry

    lax.fori_loop(0, LAT, clear, 0)
    rrv[...] = jnp.ones((1, 128), F32)
    rpart[...] = jnp.zeros((1, 128), F32)
    part[...] = jnp.zeros((1, 128), F32)

    def build_winds():
        for copy in halo_w():
            copy.wait()
        side = sides(hp_w, 0) + sides(hp_w, 4) + sides(hp_w, 2)
        for g in range(EXT):
            if g < 8:
                main, ok = ns_w[0, g], valid_s
            elif g < 16:
                main, ok = wown[g - 8], None
            else:
                main, ok = ns_w[1, g - 16], valid_n
            side_g = side[g]
            both = jnp.concatenate([main, side_g], axis=1)
            u = both[:LEV]
            v = both[LEV:]
            values = (
                1.0 - jnp.abs(u) - jnp.abs(v),
                jnp.maximum(u, 0.0),
                jnp.maximum(-u, 0.0),
                jnp.maximum(v, 0.0),
                jnp.maximum(-v, 0.0),
            )
            for i, value in enumerate(values):
                winds[i, g] = value if ok is None else value * ok

    def advance(dst, src, shift, lo, hi, adjoint, unroll, extra=None):
        def body(g, carry):
            for var in range(4):
                at = slice(var * LEV, (var + 1) * LEV)
                mid = tiles(src[g - shift, at, :])
                below = tiles(src[g - shift - 1, at, :])
                above = tiles(src[g - shift + 1, at, :])
                keep, from_west, from_east = (tiles(winds[i, g]) for i in range(3))
                if adjoint:
                    left = east_of([w * m for w, m in zip(from_west, mid)])
                    right = west_of([w * m for w, m in zip(from_east, mid)])
                    up, down = tiles(winds[3, g + 1]), tiles(winds[4, g - 1])
                    up = [w * m for w, m in zip(up, above)]
                    down = [w * m for w, m in zip(down, below)]
                else:
                    left = [w * m for w, m in zip(from_west, west_of(mid))]
                    right = [w * m for w, m in zip(from_east, east_of(mid))]
                    up, down = tiles(winds[3, g]), tiles(winds[4, g])
                    up = [w * m for w, m in zip(up, below)]
                    down = [w * m for w, m in zip(down, above)]
                for i in range(3):
                    lanes = slice(i * 128, (i + 1) * 128)
                    out = keep[i] * mid[i] + left[i] + right[i] + up[i] + down[i]
                    dst[g, at, lanes] = out if extra is None else out + extra[g, at, lanes]
            return carry

        lax.fori_loop(lo, hi, body, 0, unroll=unroll)

    def project(window, source):
        def body(r, carry):
            high, low = split(source(r))
            both = jnp.concatenate([high, low], axis=0).astype(BF16)
            out = mm(opp, both)
            proj[r, window * TYPES : (window + 1) * TYPES, :] = out[:8] + out[8:]
            return carry

        lax.fori_loop(0, LAT, body, 0, unroll=8)

    def message(dst, row):
        for w in range(WIN):
            dst[pl.ds(w, NDEV, stride=4), :] = stage[w * 128 : (w + 1) * 128, :].T
        dst[pl.ds(3, NDEV, stride=4), :] = jnp.broadcast_to(row, (NDEV, 128))

    def received(recv):
        return jnp.sum(recv[pl.ds(3, NDEV, stride=4), :], axis=0, keepdims=True)

    def spread_sum(lanes):
        return jnp.broadcast_to(jnp.sum(lanes, axis=1, keepdims=True), (1, 128))

    lower = lax.broadcasted_iota(jnp.int32, (1, 128), 1) < 64

    def fold(row):
        return row + pltpu.roll(row, 64, axis=1)

    def full(row):
        return jnp.concatenate([row, row, row], axis=1)

    def own_squares(value):
        own = value[:, :LON]
        return jnp.sum((own * own).reshape(8, 8, LON), axis=0)

    def forward(it):
        ping, pong = field.at[0], field.at[1]
        project(0, lambda r: res[r + 4, :, :LON])
        advance(pong, res, 4, 5, 19, False, 14)
        advance(ping, pong, 0, 6, 18, False, 12)
        project(1, lambda r: ping[r + 8, :, :LON])
        advance(pong, ping, 0, 7, 17, False, 10)
        advance(ping, pong, 0, 8, 16, False, 8)
        project(2, lambda r: ping[r + 8, :, :LON])
        for r in range(LAT):
            lgather[r * 48 : (r + 1) * 48, :] = jnp.concatenate(split(proj[r]), axis=0).astype(BF16)
        for n in range(8):
            found = mm(lgather[...], colhot[n])
            band = jnp.broadcast_to(columns(n) >> 8, (WT, 256))
            got = found[:WT] + found[WT : 2 * WT]
            for r in range(1, LAT):
                at = r * 2 * WT
                got = jnp.where(band == r, found[at : at + WT] + found[at + WT : at + 2 * WT], got)
            for half in range(2):
                for w in range(WIN):
                    stage[pl.ds(w * 128 + 2 * n + half, 8, stride=16), :] = got[
                        w * 8 : (w + 1) * 8, half * 128 : (half + 1) * 128
                    ]
        message(send_f, rpart[...])

        def exchange(rows):
            a2a_start(send_f, recv_f, 0, swapped, me, rows)
            a2a_wait(send_f, recv_f, 0, rows)

        @pl.when(it == 1)
        def _():
            exchange(3)

        @pl.when(it > 1)
        def _():
            exchange(4)

        norm = spread_sum(received(recv_f))
        beta = jnp.where(it == 1, jnp.zeros_like(norm), norm / rrv[...])
        for w in range(WIN):
            table = recv_f[pl.ds(w, NDEV, stride=4), :].T
            high, low = split(table)
            for t in range(TYPES):
                at = slice(t * 16, (t + 1) * 16)
                tsplit[w * TYPES + t] = jnp.concatenate([high[at], low[at]], axis=0).astype(BF16)

        def look(b, acc):
            which = window_s[b] * TYPES + type_s[b]
            got = mm(tsplit[which], onehot[b])
            both = (got[:16] + got[16:]) * cweight[b]
            summed = (both[:, :128] + both[:, 128:256]) + (both[:, 256:384] + both[:, 384:])
            y = jnp.sum(summed, axis=0, keepdims=True) + beta * yrow[b]
            yrow[b] = y
            z = live[b] * y
            zrow[b] = z
            return acc + z * y

        quad = lax.fori_loop(0, NBLK, look, jnp.zeros((1, ROWS), F32), unroll=16)

        def turn(r, acc):
            p = res[r + 4] + full(beta) * dirn[r + 4]
            dirn[r + 4] = p
            return acc + own_squares(p)

        pp = lax.fori_loop(0, LAT, turn, jnp.zeros((8, LON), F32), unroll=2)
        pp = jnp.sum(pp, axis=0, keepdims=True)
        part[...] = quad + pp[:, :128] + pp[:, 128:]
        betav[...] = beta

    def row_copy(i):
        held_rows, out = (x_held, x_out) if i < LAT else (r_held, r_out)
        return pltpu.make_async_copy(held_rows.at[i % LAT], out.at[:, i % LAT, :], out_sem.at[i])

    left = inc

    def restore(dst, out, base, group, row):
        rows = range(4 * group, 4 * group + 4)
        high, middle, low = exact(jnp.concatenate([row(r) for r in rows], axis=0))
        value = mm(high, back[...]) + mm(middle, back[...]) + mm(low, back[...])
        for i, r in enumerate(rows):
            dst[r] = value[i * CH : (i + 1) * CH]
            row_copy(base + r).start()

    def forcing(value):
        high, low = split(value)
        return mm(opt, jnp.concatenate([high, high, low, low], axis=0).astype(BF16))

    def adjoint(it, alpha, deep):
        copies = halo_s(deep)
        for copy in copies:
            copy.start()
        ping, pong = field.at[0], field.at[1]
        into = {2: ping, 1: force1, 0: force0}
        near = {2: 8 if deep else 4, 1: 6 if deep else 2, 0: 4 if deep else 0}

        def own(r, c):
            for w in range(WIN):
                into[w][r + 8, :, :LON] = forcing(ssum[w * LAT + r])
            return c

        def own_side(r, c):
            for w in range(WIN):
                into[w][r + 8, :, LON:] = forcing(sside[r + 8, w * TYPES : (w + 1) * TYPES, :])
            return c

        def outside(w):
            count = near[w]
            if count == 0:
                return

            def body(i, c):
                for k, g, r in ((0, i + 8 - count, i + 8 - count), (1, 16 + i, i)):
                    into[w][g, :, :LON] = forcing(ns_s[k, w * LAT + r])
                    into[w][g, :, LON:] = forcing(sside[g, w * TYPES : (w + 1) * TYPES, :])
                return c

            lax.fori_loop(0, count, body, 0, unroll=4 if count % 4 == 0 else count // 2)

        def landed(w):
            if near[w]:
                at = 6 + 2 * (2 - w)
                for copy in copies[at : at + 2]:
                    copy.wait()

        if not deep:
            narrow = full(alpha)[:, :LON]
            for group in range(2):
                restore(x_held, x_out, 0, group, lambda r: inc[r] + narrow * dirn[r + 4, :, :LON])
            for r in range(LAT):
                left[r] = res[r + 4, :, :LON] - narrow * dirn[r + 4, :, :LON]
        lax.fori_loop(0, LAT, own, 0, unroll=4)
        for copy in copies[4:6]:
            copy.wait()
        for r, value in enumerate(sides(hp_s, 4)):
            sside[r + 8] = value
        lax.fori_loop(0, LAT, own_side, 0, unroll=8)
        advance(pong, ping, 0, 9, 15, True, 6)
        for copy in copies[:4]:
            copy.wait()
        for r, value in enumerate(sides(hp_s, 0)):
            sside[r] = value
        for r, value in enumerate(sides(hp_s, 2)):
            sside[r + 16] = value
        landed(2)
        outside(2)
        lo, hi = (1, 23) if deep else (5, 19)
        advance(pong, ping, 0, lo, 9, True, 9 - lo)
        advance(pong, ping, 0, 15, hi, True, hi - 15)
        landed(1)
        outside(1)
        lo, hi = lo + 1, hi - 1
        advance(ping, pong, 0, lo, hi, True, (hi - lo) // 2 if deep else hi - lo, force1)
        lo, hi = lo + 1, hi - 1
        advance(pong, ping, 0, lo, hi, True, hi - lo)
        landed(0)
        outside(0)
        lo, hi = lo + 1, hi - 1
        advance(ping, pong, 0, lo, hi, True, 8, force0)
        zero = jnp.zeros((8, LON), F32)

        def done(acc):
            acc = jnp.sum(acc, axis=0, keepdims=True)
            rpart[...] = acc[:, :128] + acc[:, 128:]

        scale = full(alpha)
        if deep:

            @pl.when(it == 0)
            def _():
                def rim(i, c):
                    e = i + LAT * (i // 4)
                    ok = jnp.where(i < 4, valid_s, valid_n)
                    res[e] = ping[e + 4] * ok
                    return c

                def body(r, acc):
                    value = ping[r + 8]
                    res[r + 4] = value
                    return acc + own_squares(value)

                lax.fori_loop(0, 8, rim, 0)
                done(lax.fori_loop(0, LAT, body, zero, unroll=2))

            @pl.when(it > 0)
            def _():
                def rim(i, c):
                    e = i + LAT * (i // 4)
                    ok = jnp.where(i < 4, valid_s, valid_n)
                    res[e] -= scale * (dirn[e] + ping[e + 4]) * ok
                    return c

                def body(r, acc):
                    p = dirn[r + 4]
                    inc[r] += scale[:, :LON] * p[:, :LON]
                    value = res[r + 4] - scale * (p + ping[r + 8])
                    res[r + 4] = value
                    return acc + own_squares(value)

                lax.fori_loop(0, 8, rim, 0)
                done(lax.fori_loop(0, LAT, body, zero, unroll=2))
        else:
            for group in range(2):
                restore(
                    r_held, r_out, LAT, group,
                    lambda r: left[r] - scale[:, :LON] * ping[r + 8, :, :LON],
                )
            for i in range(2 * LAT):
                row_copy(i).wait()

    def observe():
        def spread(b, c):
            z = zrow[b]
            value = cweight[b] * jnp.concatenate([z, z, z, z], axis=1)
            high, low = split(value)
            both = jnp.concatenate([high, low], axis=0).astype(BF16)
            out = mm_nt(both, onehot[b])
            rblk[pl.ds(pl.multiple_of(b * SLOTS, SLOTS), SLOTS), :] = out[:16] + out[16:]
            return c

        lax.fori_loop(0, NBLK, spread, 0, unroll=16)
        for q in range(SLOTS):
            high, low = split(rblk[pl.ds(q, NBLK, stride=SLOTS), :])
            out = mm(member, high.astype(BF16)) + mm(member, low.astype(BF16))
            for w in range(WIN):
                stage[pl.ds(w * 128 + q, 8, stride=16), :] = out[w * 8 : (w + 1) * 8]
        message(send_b, jnp.where(lower, fold(part[...]), fold(rpart[...])))

    observe()
    pl.semaphore_wait(barrier, NDEV - 1)

    def outer(it, carry):
        @pl.when(it == 0)
        def _():
            a2a_start(send_b, recv_b, 1, plain, swapped(lat, lon), 3)

        @pl.when(it > 0)
        def _():
            a2a_start(send_b, recv_b, 1, plain, swapped(lat, lon), 4)


        @pl.when(it == 0)
        def _():
            for copy in halo_w():
                copy.start()
            build_winds()

        @pl.when(it == 1)
        def _():
            def beyond(i, c):
                e = i + LAT * (i // 4)
                dirn[e] = res[e] + full(betav[...]) * dirn[e]
                return c

            lax.fori_loop(0, 8, beyond, 0)

        @pl.when(it == 0)
        def _():
            a2a_wait(send_b, recv_b, 1, 3)

        @pl.when(it > 0)
        def _():
            a2a_wait(send_b, recv_b, 1, 4)

        for w in range(WIN):
            stage[w * 128 : (w + 1) * 128, :] = recv_b[pl.ds(w, NDEV, stride=4), :].T
        sums = received(recv_b)
        norm = spread_sum(jnp.where(lower, 0.0, sums))
        rrv[...] = norm
        alpha = norm / spread_sum(jnp.where(lower, sums, 0.0))
        for n in range(8):
            halves = []
            for half in range(2):
                halves.append(
                    jnp.concatenate(
                        [stage[pl.ds(w * 128 + 2 * n + half, 8, stride=16), :] for w in range(WIN)],
                        axis=0,
                    )
                )
            high, low = split(jnp.concatenate(halves, axis=1))
            band = jnp.broadcast_to(columns(n) >> 8, (WT, 256))
            for r in range(LAT):
                here = band == r
                lscatter[r * 48 : (r + 1) * 48, :] = jnp.concatenate(
                    [jnp.where(here, high, 0.0), jnp.where(here, low, 0.0)], axis=0
                ).astype(BF16)
            out = mm_nt(lscatter[...], colhot[n])
            if n == 0:
                sacc[...] = out
            else:
                sacc[...] += out
        for r in range(LAT):
            value = sacc[r * 48 : r * 48 + WT, :] + sacc[r * 48 + WT : (r + 1) * 48, :]
            for w in range(WIN):
                ssum[w * LAT + r] = value[w * TYPES : (w + 1) * TYPES]
        mixed = pack_typed(
            [jnp.concatenate([ssum[w * LAT + r] for w in range(WIN)], axis=0) for r in range(LAT)]
        )
        mixed = mm(jnp.concatenate(split(mixed), axis=0).astype(BF16), mend[...])
        pack_s[...] = mixed[:WT] + mixed[WT:]
        @pl.when(it < 2)
        def _():
            adjoint(it, alpha, True)
            forward(it + 1)
            observe()

        @pl.when(it == 2)
        def _():
            adjoint(it, alpha, False)

        return carry

    lax.fori_loop(0, 3, outer, 0)


def relay(x_in, r_in, x_out, r_out, held, load, store):
    loads, stores = [], []
    for i in range(8):
        src, dst = (x_in, x_out) if i < 4 else (r_in, r_out)
        at = pl.ds(i % 4 * LEV, LEV)
        loads.append(pltpu.make_async_copy(src.at[at], held.at[i], load.at[i]))
        stores.append(pltpu.make_async_copy(held.at[i], dst.at[at], store.at[i]))
    for copy in loads:
        copy.start()
    for first, second in zip(loads, stores):
        first.wait()
        second.start()
    for copy in stores:
        copy.wait()


def shards(
    zonal_wind, merid_wind, operator_rows, innovation, error_weight, interp_weight, obs_slot,
    block_count, block_type, block_window, send_cols,
):
    V = pltpu.VMEM
    dma = pltpu.SemaphoreType.DMA
    x, r = pl.pallas_call(
        kernel,
        out_shape=[jax.ShapeDtypeStruct((CH, LAT, LON), F32)] * 2,
        in_specs=[pl.BlockSpec(memory_space=pl.ANY)] * 13,
        out_specs=[pl.BlockSpec(memory_space=pl.ANY)] * 2,
        scratch_shapes=[
            V((LEV, LAT, LON), F32),
            V((LEV, LAT, LON), F32),
            V((KPTS, NBLK * ROWS), F32),
            V((KPTS, NBLK * ROWS), jnp.int32),
            V((TYPES, CH), F32),
            V((NBLK, 1, ROWS), F32),
            V((NBLK, 1, ROWS), F32),
            V((1, NDEV * SLOTS), jnp.int32),
            V((1, NBLK), jnp.int32),
            V((1, NBLK), jnp.int32),
            pltpu.SMEM((NBLK,), jnp.int32),
            pltpu.SMEM((NBLK,), jnp.int32),
            pltpu.SMEM((NBLK,), jnp.int32),
            dma((13,)),
            V((5, EXT, LEV, LANES), F32),
            V((2, EXT, CH, LANES), F32),
            V((MID, CH, LANES), F32),
            V((MID, CH, LANES), F32),
            V((LAT, CH, LON), F32),
            V((EXT, CH, LANES), F32),
            V((EXT, CH, LANES), F32),
            V((128, 128), F32),
            V((SLOTS, 128), jnp.int32),
            V((LON, LON), BF16),
            V((128, 128), BF16),
            V((LAT, 2 * LEV, LON), F32),
            V((NBLK, NDEV, KPTS * ROWS), BF16),
            V((NBLK, SLOTS, KPTS * ROWS), F32),
            V((NBLK, 1, ROWS), F32),
            V((NBLK, 1, ROWS), F32),
            V((NBLK, 1, ROWS), F32),
            V((NBLK * SLOTS, NDEV), F32),
            V((WT, 32, NDEV), BF16),
            V((8, LON, 256), BF16),
            V((LAT, WT, LON), F32),
            V((WIN * LAT, TYPES, LON), F32),
            V((EXT, WT, 128), F32),
            V((WIN * 128, 128), F32),
            V((16 * WT, 256), BF16),
            V((16 * WT, 256), BF16),
            V((16 * WT, 256), F32),
            V((NDEV * 4, 128), F32),
            V((NDEV * 4, 128), F32),
            V((NDEV * 4, 128), F32),
            V((NDEV * 4, 128), F32),
            V((LAT, 2 * LEV, LON), F32),
            V((2 * LEV, 128), F32),
            V((WT, 128), F32),
            V((2, LAT, 2 * LEV, LON), F32),
            V((2, WIN * LAT, TYPES, LON), F32),
            V((6, 2 * LEV, 128), F32),
            V((6, WT, 128), F32),
            V((1, 128), F32),
            V((1, 128), F32),
            V((1, 128), F32),
            V((1, 128), F32),
            V((LON, LON), BF16),
            V((LAT, CH, LON), F32),
            V((LAT, CH, LON), F32),
            dma((2 * LAT,)),
            dma((2,)),
            dma((2,)),
            dma((8,)),
            dma((8,)),
            dma((12,)),
            dma((12,)),
        ],
        compiler_params=pltpu.CompilerParams(
            collective_id=0, has_side_effects=True, vmem_limit_bytes=60 << 20
        ),
        name="cg",
    )(
        zonal_wind, merid_wind, interp_weight, obs_slot, operator_rows,
        innovation.reshape(NBLK, 1, ROWS), error_weight.reshape(NBLK, 1, ROWS),
        send_cols, block_type.reshape(1, NBLK), block_window.reshape(1, NBLK),
        block_count, block_type, block_window,
    )
    shape = (4, LEV, LAT, LON)
    hbm = pl.BlockSpec(memory_space=pl.ANY)
    x, r = pl.pallas_call(
        relay,
        out_shape=[jax.ShapeDtypeStruct((CH, LAT, LON), F32)] * 2,
        in_specs=[hbm] * 2,
        out_specs=[hbm] * 2,
        scratch_shapes=[
            pltpu.VMEM((8, LEV, LAT, LON), F32),
            pltpu.SemaphoreType.DMA((8,)),
            pltpu.SemaphoreType.DMA((8,)),
        ],
        compiler_params=pltpu.CompilerParams(vmem_limit_bytes=60 << 20),
        name="relay",
    )(x, r)
    return x.reshape(shape), r.reshape(shape)


def solution(mesh):
    both = ("lat", "lon")
    in_specs = (
        P(None, "lat", "lon"),
        P(None, "lat", "lon"),
        P(),
        P(both),
        P(both),
        P(None, both),
        P(None, both),
        P(both),
        P(both),
        P(both),
        P(both, None),
    )
    out_specs = (P(None, None, "lat", "lon"), P(None, None, "lat", "lon"))
    return jax.shard_map(shards, mesh=mesh, in_specs=in_specs, out_specs=out_specs, check_vma=False)
```
